32 devices in a mesh: blk: 8 (over z, y), tp: 4 (over x, core).
Axes of the slice: x: 2, y: 2, z: 4, core: 2. Of those that a mesh axis runs over, the one named last changes fastest.
Arguments:
- layer_input: bfloat16 [4096, 2048], P('blk'), may hold values from -6 to 6
- w_query: bfloat16 [2048, 2048], P('blk', 'tp'), may hold values from -0.125 to 0.125
- w_key: bfloat16 [2048, 1024], P('blk', 'tp'), may hold values from -0.125 to 0.125
- w_value: bfloat16 [2048, 1024], P('blk', 'tp'), may hold values from -0.125 to 0.125
- w_output: bfloat16 [2048, 2048], P('tp', 'blk'), may hold values from -1 to 1
- w_gate: bfloat16 [2048, 6144], P('blk', 'tp'), may hold values from -0.125 to 0.125
- w_up: bfloat16 [2048, 6144], P('blk', 'tp'), may hold values from -0.125 to 0.125
- w_down: bfloat16 [6144, 2048], P('tp', 'blk'), may hold values from -0.078125 to 0.078125
- norm_attn: bfloat16 [2048], P('blk'), may hold values from 0.099609375 to 1.8984375
- norm_mlp: bfloat16 [2048], P('blk'), may hold values from 0.099609375 to 1.8984375
- norm_query: bfloat16 [128], replicated, may hold values from 0.099609375 to 1.8984375
- norm_key: bfloat16 [128], replicated, may hold values from 0.099609375 to 1.8984375
- out_grad: bfloat16 [4096, 2048], P('blk'), may hold values from -6 to 6
- doc_lengths: int32 [4], replicated, may hold values from 1 to 2048, 4096 in all
- stretch_order: int32 [16], replicated, may hold values from 0 to 15, each once
Outputs:
- layer_output: bfloat16 [4096, 2048], P('blk')
- input_grad: float32 [4096, 2048], P('blk')
- grad_query: float32 [2048, 2048], P('blk', 'tp')
- grad_key: float32 [2048, 1024], P('blk', 'tp')
- grad_value: float32 [2048, 1024], P('blk', 'tp')
- grad_output: float32 [2048, 2048], P('tp', 'blk')
- grad_gate: float32 [2048, 6144], P('blk', 'tp')
- grad_up: float32 [2048, 6144], P('blk', 'tp')
- grad_down: float32 [6144, 2048], P('tp', 'blk')
- grad_norm_attn: float32 [2048], P('blk')
- grad_norm_mlp: float32 [2048], P('blk')
- grad_norm_query: float32 [128], P('blk')
- grad_norm_key: float32 [128], P('blk')
The draws below stay inside these ranges and needn't reach their ends.
Inputs may be any that keep to these rules, and one draw needn't show every extreme that they name: `doc_lengths`: the 4 lengths sum to 4096; the longest is exactly 2048. Each of the 16 blocks of 256 pack positions appears once; stored row block j holds the positions from stretch_order[j] * 256 on.
All inputs are finite; a program needn't handle non-finite values.
Results may differ from the reference program's by a relative error of at most 0.025.
Values may be sent and summed in bfloat16 or wider, within the bound.
A program may use at most 192 MiB of HBM per device.

```python
import math
from functools import partial
import jax
import jax.numpy as jnp
import numpy as np
from jax import lax

D = 2048
QH = 16
KVH = 8
HD = 128
FF = 6144
TOK_DEV = 512
NDOCS = 4
TOKENS = 4096
STRETCHES = 16
LONGEST = 2048


def level_of(rng, dims, pieces, least, top_value):
    def one(position, parts):
        heights = jax.random.uniform(jax.random.fold_in(jax.random.fold_in(rng, 6), position), (parts,), jnp.float32, least / len(pieces), top_value / len(pieces))
        return jnp.repeat(jnp.exp(heights), dims[position] // parts).reshape((-1,) + (1,) * (len(dims) - position - 1))

    level = one(*pieces[0])
    for cut in pieces[1:]:
        level = level * one(*cut)
    return level


def split_up(amount, total, limit, lean):
    weights = [(1 << 20) // math.isqrt(grade ** lean) + 1 for grade in range(2, amount + 1)]
    rest, counts = total - limit - (amount - 1), [1] * (amount - 1)
    while rest > 0:
        movable = [i for i in range(amount - 1) if counts[i] < limit]
        pool, remaining = sum([weights[i] for i in movable]), rest
        for i in movable:
            addition = min(limit - counts[i], max(1, remaining * weights[i] // pool), rest)
            counts[i] = counts[i] + addition
            rest = rest - addition
    return np.array([limit] + counts)


def uneven(stream_key, number_of, total, reach, slope):
    if number_of == 2:
        one = jax.random.randint(stream_key, (), max(1, total - reach), min(reach, total - 1) + 1)
        return jnp.stack([one, total - one])
    sizes = jnp.asarray(split_up(number_of, total, reach, slope), jnp.int32)
    couples = (number_of - 1) // 2
    source_of, receiver = sizes[1:1 + 2 * couples:2], sizes[2:2 + 2 * couples:2]
    slack = jnp.minimum(source_of - 1, reach - receiver)
    moved = jax.random.randint(jax.random.fold_in(stream_key, 1), (couples,), 0, 1 << 20) % (slack + 1)
    sizes = sizes.at[1:1 + 2 * couples:2].set(source_of - moved).at[2:2 + 2 * couples:2].set(receiver + moved)
    return sizes[jax.random.permutation(jax.random.fold_in(stream_key, 2), number_of)]


def centred(key, extent, spread, limit, cuts=(), held_as=jnp.bfloat16):
    drawn = jax.random.normal(key, extent, jnp.float32) * spread
    if len(cuts) > 0:
        drawn = level_of(key, extent, cuts, -0.22, 0.18) * drawn
    return jnp.clip(drawn, min=-limit, max=limit).astype(held_as)


def setup_inputs(seed: int = 0) -> dict:
    streams_of = jax.random.split(jax.random.key(seed), 16)
    layer_input = centred(streams_of[0], (TOKENS, D), 1.0, 6.0, ((0, 8),))
    w_query = centred(streams_of[1], (D, QH * HD), D ** -0.5, 0.125, ((0, 8), (1, 4)))
    w_key = centred(streams_of[2], (D, KVH * HD), D ** -0.5, 0.125, ((0, 8), (1, 4)))
    w_value = centred(streams_of[3], (D, KVH * HD), D ** -0.5, 0.125, ((0, 8), (1, 4)))
    w_output = centred(streams_of[4], (QH * HD, D), (QH * HD // 64) ** -0.5, 1.0, ((0, 4), (1, 8)))
    w_gate = centred(streams_of[5], (D, FF), D ** -0.5, 0.125, ((0, 8), (1, 4)))
    w_up = centred(streams_of[6], (D, FF), D ** -0.5, 0.125, ((0, 8), (1, 4)))
    w_down = centred(streams_of[7], (FF, D), FF ** -0.5, 0.078125, ((0, 4), (1, 8)))
    norm_attn = jnp.clip(1.0 + 0.18 * jax.random.normal(streams_of[8], (D,), jnp.float32), 0.099609375, 1.8984375).astype(jnp.bfloat16)
    norm_mlp = jnp.clip(1.0 + 0.18 * jax.random.normal(streams_of[9], (D,), jnp.float32), 0.099609375, 1.8984375).astype(jnp.bfloat16)
    norm_query = jnp.clip(1.0 + 0.18 * jax.random.normal(streams_of[10], (HD,), jnp.float32), 0.099609375, 1.8984375).astype(jnp.bfloat16)
    norm_key = jnp.clip(1.0 + 0.18 * jax.random.normal(streams_of[11], (HD,), jnp.float32), 0.099609375, 1.8984375).astype(jnp.bfloat16)
    out_grad = centred(streams_of[12], (TOKENS, D), 1.0, 6.0, ((0, 8),))
    doc_lengths = uneven(streams_of[13], NDOCS, TOKENS, LONGEST, 2).astype(jnp.int32)
    stretch_order = jax.random.permutation(streams_of[14], STRETCHES).astype(jnp.int32)
    return dict(layer_input=layer_input, w_query=w_query, w_key=w_key, w_value=w_value, w_output=w_output, w_gate=w_gate, w_up=w_up, w_down=w_down, norm_attn=norm_attn, norm_mlp=norm_mlp, norm_query=norm_query, norm_key=norm_key, out_grad=out_grad, doc_lengths=doc_lengths, stretch_order=stretch_order)


EPS = 1e-06
ROPE_BASE = 1000000.0
MASKED = -1e+30
HIGH = lax.Precision.HIGHEST

@jax.custom_vjp
def low(v):
    return lax.optimization_barrier(v.astype(jnp.bfloat16)).astype(jnp.float32)

@jax.custom_vjp
def low_back(v):
    return v

def low_keep(v):
    return (low(v), None)

def low_pass(kept, grad):
    return (grad,)

def back_keep(v):
    return (v, None)

def back_low(kept, grad):
    return (low(grad),)
low.defvjp(low_keep, low_pass)
low_back.defvjp(back_keep, back_low)

def rms_scale(values, gain):
    return values * lax.rsqrt(lax.optimization_barrier(jnp.mean(values * values, axis=-1, keepdims=True)) + EPS) * gain

def rotate(values, cosine, sine):
    half = values.shape[-1] // 2
    turned = jnp.concatenate([-values[..., half:], values[..., :half]], axis=-1)
    return values * cosine + turned * sine

def rope_tables(offsets, head_dim):
    half = head_dim // 2
    inverse = ROPE_BASE ** (-2.0 * jnp.arange(half, dtype=jnp.float32) / head_dim)
    angles = offsets.astype(jnp.float32)[:, None] * inverse[None, :]
    angles = jnp.concatenate([angles, angles], axis=-1)
    return (jnp.cos(angles), jnp.sin(angles))

def place_rows(first_row, count, stretch_half, stretch_order, starts):
    rows = (first_row + jnp.arange(count, dtype=jnp.int32)).astype(jnp.int32)
    block_ids = rows // stretch_half
    table_ids = jnp.arange(stretch_order.shape[0], dtype=jnp.int32)
    picked = lax.optimization_barrier(jnp.sum(jnp.where(block_ids[:, None] == table_ids[None, :], stretch_order[None, :], 0), axis=1)).astype(jnp.int32)
    positions = (picked * stretch_half + rows % stretch_half).astype(jnp.int32)
    firsts = lax.optimization_barrier(jnp.max(jnp.where(starts[None, :] <= positions[:, None], starts[None, :], 0), axis=1)).astype(jnp.int32)
    return (positions, firsts)

def layer_forward(inputs, w_query, w_key, w_value, w_output, w_gate, w_up, w_down, gain_attn, gain_mlp, gain_query, gain_key, cosine, sine, positions, firsts):
    tokens = inputs.shape[0]
    group = QH // KVH
    scale = HD ** (-0.5)
    attn_in = low(rms_scale(inputs, gain_attn))
    query_raw = low_back(jnp.dot(attn_in, w_query, precision=HIGH)).reshape(tokens, KVH, group, HD)
    key_raw = low_back(jnp.dot(attn_in, w_key, precision=HIGH)).reshape(tokens, KVH, HD)
    value_all = low_back(low(jnp.dot(attn_in, w_value, precision=HIGH))).reshape(tokens, KVH, HD)
    query_all = low(rotate(rms_scale(query_raw, gain_query), cosine[:, None, None, :], sine[:, None, None, :]))
    key_all = low(rotate(rms_scale(key_raw, gain_key), cosine[:, None, :], sine[:, None, :]))
    block_rows = min(512, tokens)
    blocks = tokens // block_rows

    def attend(block):
        query_block, query_pos, query_first = block
        scores = low_back(jnp.einsum('bkgd,tkd->kgbt', query_block, key_all, precision=HIGH) * scale)
        allowed = (positions[None, :] <= query_pos[:, None]) & (positions[None, :] >= query_first[:, None])
        scores = jnp.where(allowed[None, None], scores, MASKED)
        shifted = jnp.exp(scores - lax.optimization_barrier(jnp.max(scores, axis=-1, keepdims=True)))
        probs = low(shifted / lax.optimization_barrier(jnp.sum(shifted, axis=-1, keepdims=True)))
        return jnp.einsum('kgbt,tkd->bkgd', probs, value_all, precision=HIGH)
    attended = lax.map(jax.checkpoint(attend), (query_all.reshape(blocks, block_rows, KVH, group, HD), positions.reshape(blocks, block_rows), firsts.reshape(blocks, block_rows)))
    attn_out = low_back(low(attended.reshape(tokens, QH * HD)))
    hidden = inputs + low_back(jnp.dot(attn_out, w_output, precision=HIGH))
    mlp_in = low(rms_scale(hidden, gain_mlp))
    gate_pre = low_back(jnp.dot(mlp_in, w_gate, precision=HIGH))
    up_pre = low_back(jnp.dot(mlp_in, w_up, precision=HIGH))
    activated = low(jax.nn.silu(gate_pre) * up_pre)
    return hidden + jnp.dot(activated, w_down, precision=HIGH)

def reference(layer_input, w_query, w_key, w_value, w_output, w_gate, w_up, w_down, norm_attn, norm_mlp, norm_query, norm_key, out_grad, doc_lengths, stretch_order):
    tokens = layer_input.shape[0]
    stretch_half = TOK_DEV // 2
    starts = (jnp.cumsum(doc_lengths) - doc_lengths).astype(jnp.int32)
    positions, firsts = place_rows(0, tokens, stretch_half, stretch_order, starts)
    cosine, sine = rope_tables(positions - firsts, HD)
    primals = tuple((array.astype(jnp.float32) for array in (layer_input, w_query, w_key, w_value, w_output, w_gate, w_up, w_down, norm_attn, norm_mlp, norm_query, norm_key)))
    bound = partial(layer_forward, cosine=cosine, sine=sine, positions=positions, firsts=firsts)
    result, pull = jax.vjp(bound, *primals)
    grads = pull(out_grad.astype(jnp.float32))
    return (result.astype(jnp.bfloat16), grads[0], grads[1], grads[2], grads[3], grads[4], grads[5], grads[6], grads[7], grads[8], grads[9], grads[10], grads[11])
```

```python
from functools import partial

import jax
import jax.numpy as jnp
from jax import lax
from jax.experimental import pallas as pl
from jax.experimental.pallas import tpu as pltpu
from jax.sharding import PartitionSpec as P

EPS = 1e-06
ROPE_BASE = 1000000.0
F32 = jnp.float32
BF16 = jnp.bfloat16


def dot(a, b, dims, out=F32):
    return lax.dot_general(a, b, (dims, ((), ())), preferred_element_type=out)


NN = ((1,), (0,))
NT = ((1,), (1,))
TN = ((0,), (0,))


def ring_order(n):
    return list(range(0, n, 2)) + list(range(n - 1, 0, -2))


def ring_perms(n):
    order = ring_order(n)
    right = [(order[i], order[(i + 1) % n]) for i in range(n)]
    return right, [(b, a) for a, b in right]


def ring_gather(own, n):
    right, left = ring_perms(n)
    half = n // 2
    rows = own.shape[0] // 2
    blocks = [None] * n
    blocks[0] = own
    from_left = from_right = own
    for k in range(1, half):
        from_left = lax.ppermute(from_left, "blk", right)
        from_right = lax.ppermute(from_right, "blk", left)
        blocks[n - k] = from_left
        blocks[k] = from_right
    top = lax.ppermute(from_left[:rows], "blk", right)
    low = lax.ppermute(from_right[rows:], "blk", left)
    blocks[half] = jnp.concatenate([top, low], axis=0)
    return blocks


def ring_scatter(part, n, rows):
    right, left = ring_perms(n)
    half = n // 2
    cut = rows // 2
    far = part(half).astype(BF16)
    to_right = lax.ppermute(far[:cut], "blk", right).astype(F32)
    to_left = lax.ppermute(far[cut:], "blk", left).astype(F32)
    if half == 1:
        return part(0) + jnp.concatenate([to_right, to_left], axis=0)
    for k in range(half - 1, 0, -1):
        send_right, send_left = part(k), part(n - k)
        if k == half - 1:
            send_right = jnp.concatenate([send_right[:cut] + to_right, send_right[cut:]], axis=0)
            send_left = jnp.concatenate([send_left[:cut], send_left[cut:] + to_left], axis=0)
        else:
            send_right = send_right + to_right
            send_left = send_left + to_left
        to_right = lax.ppermute(send_right.astype(BF16), "blk", right).astype(F32)
        to_left = lax.ppermute(send_left.astype(BF16), "blk", left).astype(F32)
    return part(0) + to_right + to_left


CORE_SWAP = [(0, 1), (1, 0), (2, 3), (3, 2)]
X_SWAP = [(0, 2), (1, 3), (2, 0), (3, 1)]


def tp_scatter(value):
    q = value.shape[0] // 4
    value = value.reshape(4, q, value.shape[1])
    send = jnp.stack([value[1], value[3]]).astype(BF16)
    got = lax.ppermute(send, "tp", CORE_SWAP).astype(F32)
    far = (value[2].astype(F32) + got[1]).astype(BF16)
    got_far = lax.ppermute(far, "tp", X_SWAP).astype(F32)
    return value[0].astype(F32) + got[0] + got_far


def tp_gather(own):
    far = lax.ppermute(own, "tp", X_SWAP)
    pair = jnp.stack([own, far])
    other = lax.ppermute(pair, "tp", CORE_SWAP)
    return jnp.concatenate([own, other[0], far, other[1]], axis=0)


def tp_sum(value):
    value = value + lax.ppermute(value, "tp", CORE_SWAP)
    return value + lax.ppermute(value, "tp", X_SWAP)


def arrange_kernel(n, cols_ref, rows_ref, x_ref, g_ref, u_ref, g_out, x_out):
    width = x_ref.shape[1] // n
    x = x_ref[...].astype(F32)
    rs = lax.rsqrt(jnp.mean(x * x, axis=-1, keepdims=True) + EPS)
    for r in range(n):
        at = pl.ds(pl.multiple_of(cols_ref[r] * width, width), width)
        to = pl.ds(r * width, width)
        piece = x_ref[:, at]
        u_ref[:, to] = (piece.astype(F32) * rs).astype(BF16)
        x_out[:, to] = piece
        g_out[:, to] = g_ref[:, at]


def arrange(x, g, cols, rows, n):
    t, d = x.shape
    quarter = t // 4
    if (d // n) % 128:
        def turn(v):
            v = v.reshape(4, quarter, n, d // n)
            return jnp.take(jnp.take(v, rows, axis=0), cols, axis=2).reshape(t, d)

        xr, gr = turn(x), turn(g)
        wide = xr.astype(F32)
        rs = lax.rsqrt(jnp.mean(wide * wide, axis=-1, keepdims=True) + EPS)
        return (wide * rs).astype(BF16), gr, xr
    spec_in = pl.BlockSpec((quarter, d), lambda j, c, r: (r[j], 0))
    spec_out = pl.BlockSpec((quarter, d), lambda j, c, r: (j, 0))
    shape = jax.ShapeDtypeStruct((t, d), BF16)
    return pl.pallas_call(
        partial(arrange_kernel, n),
        grid_spec=pltpu.PrefetchScalarGridSpec(
            num_scalar_prefetch=2,
            grid=(4,),
            in_specs=[spec_in, spec_in],
            out_specs=[spec_out, spec_out, spec_out],
        ),
        out_shape=[shape, shape, shape],
        name="arrange",
    )(cols, rows, x, g)


def restore_kernel(n, cols_ref, rows_ref, x_ref, out_ref):
    width = x_ref.shape[1] // n
    for r in range(n):
        at = pl.ds(pl.multiple_of(cols_ref[r] * width, width), width)
        out_ref[:, at] = x_ref[:, r * width : (r + 1) * width].astype(out_ref.dtype)


def restore(x, cols, rows, n, dtype):
    t, d = x.shape
    quarter = t // 4
    if (d // n) % 128:
        v = x.reshape(4, quarter, n, d // n)
        v = jnp.take(jnp.take(v, rows, axis=0), jnp.argsort(cols), axis=2)
        return v.reshape(t, d).astype(dtype)
    return pl.pallas_call(
        partial(restore_kernel, n),
        grid_spec=pltpu.PrefetchScalarGridSpec(
            num_scalar_prefetch=2,
            grid=(4,),
            in_specs=[pl.BlockSpec((quarter, d), lambda j, c, r: (j, 0))],
            out_specs=pl.BlockSpec((quarter, d), lambda j, c, r: (r[j], 0)),
        ),
        out_shape=jax.ShapeDtypeStruct((t, d), dtype),
        name="restore",
    )(cols, rows, x)


def turned(v, sine):
    return pltpu.roll(v, v.shape[1] // 2, 1) * sine


def qkv_kernel(heads, hd, u_ref, w_ref, cos_ref, sin_ref, gain_ref, raw_ref, q_ref, kv_ref):
    qh, kh = heads
    y = dot(u_ref[...], w_ref[...], NN)
    raw_ref[...] = y[:, : (qh + kh) * hd]
    cosine, sine = cos_ref[...], sin_ref[...]
    for h in range(qh + kh):
        v = y[:, h * hd : (h + 1) * hd]
        rs = lax.rsqrt(jnp.mean(v * v, axis=-1, keepdims=True) + EPS)
        v = v * rs * gain_ref[0 if h < qh else 1]
        v = (v * cosine + turned(v, sine)).astype(BF16)
        if h < qh:
            q_ref[:, h * hd : (h + 1) * hd] = v
        else:
            kv_ref[:, (h - qh) * hd : (h - qh + 1) * hd] = v
    kv_ref[:, kh * hd :] = y[:, (qh + kh) * hd :].astype(BF16)


def qkv_call(u, w, cosine, sine, gains, qh, kh, hd):
    t, d = u.shape
    rows = t // 4
    width = w.shape[1]
    return pl.pallas_call(
        partial(qkv_kernel, (qh, kh), hd),
        grid=(4,),
        in_specs=[
            pl.BlockSpec((rows, d), lambda i: (i, 0)),
            pl.BlockSpec((d, width), lambda i: (0, 0)),
            pl.BlockSpec((rows, hd), lambda i: (i, 0)),
            pl.BlockSpec((rows, hd), lambda i: (i, 0)),
            pl.BlockSpec((2, 1, hd), lambda i: (0, 0, 0)),
        ],
        out_specs=[
            pl.BlockSpec((rows, (qh + kh) * hd), lambda i: (i, 0)),
            pl.BlockSpec((rows, qh * hd), lambda i: (i, 0)),
            pl.BlockSpec((rows, 2 * kh * hd), lambda i: (i, 0)),
        ],
        out_shape=[
            jax.ShapeDtypeStruct((t, (qh + kh) * hd), F32),
            jax.ShapeDtypeStruct((t, qh * hd), BF16),
            jax.ShapeDtypeStruct((t, 2 * kh * hd), BF16),
        ],
        cost_estimate=pl.CostEstimate(
            flops=2 * t * d * width, bytes_accessed=2 * d * (t + width), transcendentals=0
        ),
        name="qkv",
    )(u, w, cosine, sine, gains)


def dqkv_kernel(heads, hd, dq_ref, dkv_ref, raw_ref, cos_ref, sin_ref, gain_ref, out_ref, dgain_ref):
    qh, kh = heads
    cosine, sine = cos_ref[...], sin_ref[...]
    sums = [jnp.zeros((1, hd), F32), jnp.zeros((1, hd), F32)]
    for h in range(qh + kh):
        kind = 0 if h < qh else 1
        if h < qh:
            grad = dq_ref[:, h * hd : (h + 1) * hd].astype(F32)
        else:
            grad = dkv_ref[:, (h - qh) * hd : (h - qh + 1) * hd].astype(F32)
        grad = grad * cosine - turned(grad, sine)
        v = raw_ref[:, h * hd : (h + 1) * hd]
        rs = lax.rsqrt(jnp.mean(v * v, axis=-1, keepdims=True) + EPS)
        unit = v * rs
        sums[kind] = sums[kind] + jnp.sum(grad * unit, axis=0, keepdims=True)
        m = grad * gain_ref[kind]
        back = (m - unit * jnp.mean(m * unit, axis=-1, keepdims=True)) * rs
        out_ref[:, h * hd : (h + 1) * hd] = back.astype(BF16)
    out_ref[:, (qh + kh) * hd :] = dkv_ref[:, kh * hd :].astype(BF16)

    @pl.when(pl.program_id(0) == 0)
    def _():
        dgain_ref[...] = jnp.zeros_like(dgain_ref)

    dgain_ref[0:1, :] += sums[0]
    dgain_ref[1:2, :] += sums[1]


def dqkv_call(dq, dkv, raw, cosine, sine, gains, qh, kh, hd):
    t = dq.shape[0]
    rows = t // 4

    def rowwise(width):
        return pl.BlockSpec((rows, width), lambda i: (i, 0))

    return pl.pallas_call(
        partial(dqkv_kernel, (qh, kh), hd),
        grid=(4,),
        in_specs=[
            rowwise(qh * hd),
            rowwise(2 * kh * hd),
            rowwise((qh + kh) * hd),
            rowwise(hd),
            rowwise(hd),
            pl.BlockSpec((2, 1, hd), lambda i: (0, 0, 0)),
        ],
        out_specs=[rowwise((qh + 2 * kh) * hd), pl.BlockSpec((8, hd), lambda i: (0, 0))],
        out_shape=[
            jax.ShapeDtypeStruct((t, (qh + 2 * kh) * hd), BF16),
            jax.ShapeDtypeStruct((8, hd), F32),
        ],
        name="dqkv",
    )(dq, dkv, raw, cosine, sine, gains)


def tile_masks(base_ref, tile, qpos_ref, qfirst_ref, off_ref, q0, stretch):
    kpos = off_ref[...] + base_ref[tile]
    qpos = qpos_ref[pl.ds(q0, stretch), :]
    qfirst = qfirst_ref[pl.ds(q0, stretch), :]
    return (kpos <= qpos) & (kpos >= qfirst)


def attend_kernel(dims, scale, base_ref, see_ref, q_ref, kv_ref, qpos_ref, qfirst_ref, off_ref, out_ref, lse_ref, acc_ref, sum_ref):
    qh, kh, hd, stretch = dims
    group = qh // kh
    tile = pl.program_id(0)
    last = pl.num_programs(0) - 1

    @pl.when(tile == 0)
    def _():
        acc_ref[...] = jnp.zeros_like(acc_ref)
        sum_ref[...] = jnp.zeros_like(sum_ref)

    for e in range(2):
        q0 = e * stretch

        @pl.when(see_ref[e, tile] > 0)
        def _():
            mask = tile_masks(base_ref, tile, qpos_ref, qfirst_ref, off_ref, q0, stretch)
            for h in range(qh):
                k = kv_ref[:, (h // group) * hd : (h // group + 1) * hd]
                v = kv_ref[:, (kh + h // group) * hd : (kh + h // group + 1) * hd]
                q = q_ref[q0 : q0 + stretch, h * hd : (h + 1) * hd]
                s = dot(q, k, NT) * scale
                p = jnp.where(mask, jnp.exp(s), 0.0)
                sum_ref[h, q0 : q0 + stretch, :] += jnp.sum(p, axis=-1, keepdims=True)
                acc_ref[q0 : q0 + stretch, h * hd : (h + 1) * hd] += dot(p.astype(BF16), v, NN)

    @pl.when(tile == last)
    def _():
        for h in range(qh):
            total = sum_ref[h]
            out_ref[:, h * hd : (h + 1) * hd] = (acc_ref[:, h * hd : (h + 1) * hd] / total).astype(BF16)
            lse_ref[h] = jnp.log(total)


def attend(base, see, q, kv, qpos, qfirst, off, qh, kh, hd, scale):
    t = q.shape[0]
    stretch = t // 2
    tiles = kv.shape[0] // stretch

    def whole(shape):
        return pl.BlockSpec(shape, lambda i, *_: (0,) * len(shape))

    return pl.pallas_call(
        partial(attend_kernel, (qh, kh, hd, stretch), scale),
        grid_spec=pltpu.PrefetchScalarGridSpec(
            num_scalar_prefetch=2,
            grid=(tiles,),
            in_specs=[
                whole((t, qh * hd)),
                pl.BlockSpec((stretch, 2 * kh * hd), lambda i, *_: (i, 0)),
                whole((t, 1)),
                whole((t, 1)),
                whole((1, stretch)),
            ],
            out_specs=[whole((t, qh * hd)), whole((qh, t, 1))],
            scratch_shapes=[pltpu.VMEM((t, qh * hd), F32), pltpu.VMEM((qh, t, 1), F32)],
        ),
        out_shape=[
            jax.ShapeDtypeStruct((t, qh * hd), BF16),
            jax.ShapeDtypeStruct((qh, t, 1), F32),
        ],
        cost_estimate=pl.CostEstimate(
            flops=4 * t * kv.shape[0] * hd * qh, bytes_accessed=2 * kv.size, transcendentals=t * kv.shape[0]
        ),
        name="attend",
    )(base, see, q, kv, qpos, qfirst, off)


def attend_back_kernel(
    dims, scale, base_ref, see_ref, q_ref, kv_ref, do_ref, o_ref, lse_ref, qpos_ref, qfirst_ref, off_ref, dq_ref, dkv_ref, acc_ref, delta_ref
):
    qh, kh, hd, stretch = dims
    group = qh // kh
    tile = pl.program_id(0)
    last = pl.num_programs(0) - 1

    @pl.when(tile == 0)
    def _():
        acc_ref[...] = jnp.zeros_like(acc_ref)
        for h in range(qh):
            at = slice(h * hd, (h + 1) * hd)
            delta_ref[h] = jnp.sum(do_ref[:, at].astype(F32) * o_ref[:, at].astype(F32), axis=-1, keepdims=True)

    sees = [see_ref[0, tile] > 0, see_ref[1, tile] > 0]

    @pl.when(jnp.logical_not(sees[0]))
    def _():
        dkv_ref[...] = jnp.zeros_like(dkv_ref)

    def half(e, add):
        q0 = e * stretch
        mask = tile_masks(base_ref, tile, qpos_ref, qfirst_ref, off_ref, q0, stretch)
        for c in range(kh):
            k = kv_ref[:, c * hd : (c + 1) * hd]
            v = kv_ref[:, (kh + c) * hd : (kh + c + 1) * hd]
            dk = dv = None
            for h in range(c * group, (c + 1) * group):
                at = slice(h * hd, (h + 1) * hd)
                q = q_ref[q0 : q0 + stretch, at]
                do = do_ref[q0 : q0 + stretch, at]
                s = dot(q, k, NT) * scale
                p = jnp.where(mask, jnp.exp(s - lse_ref[h, q0 : q0 + stretch, :]), 0.0)
                dp = dot(do, v, NT)
                ds = (p * (dp - delta_ref[h, q0 : q0 + stretch, :])).astype(BF16)
                acc_ref[q0 : q0 + stretch, at] += dot(ds, k, NN)
                dk_h = dot(ds, q, TN)
                dv_h = dot(p.astype(BF16), do, TN)
                dk = dk_h if dk is None else dk + dk_h
                dv = dv_h if dv is None else dv + dv_h
            ck = slice(c * hd, (c + 1) * hd)
            cv = slice((kh + c) * hd, (kh + c + 1) * hd)
            if add:
                dkv_ref[:, ck] += dk * scale
                dkv_ref[:, cv] += dv
            else:
                dkv_ref[:, ck] = dk * scale
                dkv_ref[:, cv] = dv

    for e in range(2):

        @pl.when(sees[e])
        def _():
            half(e, e == 1)

    @pl.when(tile == last)
    def _():
        dq_ref[...] = acc_ref[...] * scale


def attend_back(base, see, q, kv, do, o, lse, qpos, qfirst, off, qh, kh, hd, scale):
    t = q.shape[0]
    stretch = t // 2
    tiles = kv.shape[0] // stretch

    def whole(shape):
        return pl.BlockSpec(shape, lambda i, *_: (0,) * len(shape))

    tile_spec = pl.BlockSpec((stretch, 2 * kh * hd), lambda i, *_: (i, 0))
    return pl.pallas_call(
        partial(attend_back_kernel, (qh, kh, hd, stretch), scale),
        grid_spec=pltpu.PrefetchScalarGridSpec(
            num_scalar_prefetch=2,
            grid=(tiles,),
            in_specs=[
                whole((t, qh * hd)),
                tile_spec,
                whole((t, qh * hd)),
                whole((t, qh * hd)),
                whole((qh, t, 1)),
                whole((t, 1)),
                whole((t, 1)),
                whole((1, stretch)),
            ],
            out_specs=[whole((t, qh * hd)), tile_spec],
            scratch_shapes=[pltpu.VMEM((t, qh * hd), F32), pltpu.VMEM((qh, t, 1), F32)],
        ),
        out_shape=[
            jax.ShapeDtypeStruct((t, qh * hd), F32),
            jax.ShapeDtypeStruct((kv.shape[0], 2 * kh * hd), F32),
        ],
        cost_estimate=pl.CostEstimate(
            flops=10 * t * kv.shape[0] * hd * qh, bytes_accessed=6 * kv.size, transcendentals=t * kv.shape[0]
        ),
        name="attend_back",
    )(base, see, q, kv, do, o, lse, qpos, qfirst, off)


def unit_rows(values):
    rs = lax.rsqrt(jnp.mean(values * values, axis=-1, keepdims=True) + EPS)
    return values * rs, rs


def norm_back(m, unit, rs):
    return (m - unit * jnp.mean(m * unit, axis=-1, keepdims=True)) * rs


def after(value, *others):
    return lax.optimization_barrier((value,) + others)[0]


def shards(
    n,
    layer_input,
    w_query,
    w_key,
    w_value,
    w_output,
    w_gate,
    w_up,
    w_down,
    norm_attn,
    norm_mlp,
    norm_query,
    norm_key,
    out_grad,
    doc_lengths,
    stretch_order,
):
    t, d = layer_input.shape
    hd = norm_query.shape[0]
    qh, kh = w_query.shape[1] // hd, w_key.shape[1] // hd
    stretch = t // 2
    quarter = t // 4
    width = d // n
    scale = hd ** (-0.5)
    blk, tp = lax.axis_index("blk"), lax.axis_index("tp")

    order = ring_order(n)
    place = jnp.array([order.index(b) for b in range(n)], jnp.int32)
    me = lax.dynamic_index_in_dim(place, blk, keepdims=False)
    cols = jnp.take(jnp.array(order + order, jnp.int32), me + jnp.arange(n, dtype=jnp.int32))
    rows = jnp.arange(4, dtype=jnp.int32) ^ tp.astype(jnp.int32)

    gain_attn = norm_attn.astype(F32)[:, None]
    gain_mlp = norm_mlp.astype(F32)[:, None]
    own_qkv = (jnp.concatenate([w_query, w_key, w_value], axis=1).astype(F32) * gain_attn).astype(BF16)
    own_out = w_output.T
    own_gate = (w_gate.astype(F32) * gain_mlp).astype(BF16)
    own_up = (w_up.astype(F32) * gain_mlp).astype(BF16)
    own_down = w_down.T

    blocks_qkv = ring_gather(own_qkv, n)
    blocks_out = ring_gather(after(own_out, blocks_qkv[1]), n)
    full_qkv = jnp.concatenate(blocks_qkv, axis=0)

    starts = jnp.cumsum(doc_lengths) - doc_lengths
    table = jnp.arange(stretch_order.shape[0], dtype=jnp.int32)

    def stretch_of(ids):
        return jnp.sum(jnp.where(ids[:, None] == table[None, :], stretch_order[None, :], 0), axis=1)

    def first_of(pos):
        return jnp.max(jnp.where(starts[None, :] <= pos[:, None], starts[None, :], 0), axis=1)

    inside = jnp.arange(stretch, dtype=jnp.int32) ^ ((tp % 2) * quarter)
    halves = jnp.arange(2, dtype=jnp.int32) ^ (tp // 2)
    base = stretch_of((cols[:, None] * 2 + halves[None, :]).reshape(-1)) * stretch
    positions = (base[:2, None] + inside[None, :]).reshape(-1)
    firsts = first_of(positions)
    base_first = first_of(base[:2])
    see = ((base[None, :] <= base[:2, None]) & (base[None, :] + (stretch - 1) >= base_first[:, None])).astype(jnp.int32)
    inverse = ROPE_BASE ** (-2.0 * jnp.arange(hd // 2, dtype=F32) / hd)
    angles = (positions - firsts).astype(F32)[:, None] * inverse[None, :]
    cosine, sine = jnp.cos(angles), jnp.sin(angles)
    cosine = jnp.concatenate([cosine, cosine], axis=1)
    sine = jnp.concatenate([-sine, sine], axis=1)
    qpos, qfirst, off = positions[:, None], firsts[:, None], inside[None, :]
    gains = jnp.stack([norm_query, norm_key]).astype(F32)[:, None, :]

    unit_attn, grad_out, x_all = arrange(layer_input, out_grad, cols, rows, n)
    x_own = x_all[:quarter].astype(F32)
    raw, q, kv_own = qkv_call(unit_attn, full_qkv, cosine, sine, gains, qh, kh, hd)
    kv = jnp.concatenate(ring_gather(kv_own, n), axis=0)
    full_out = jnp.concatenate(blocks_out, axis=0)
    blocks_gate = ring_gather(after(own_gate, blocks_out[1]), n)
    blocks_up = ring_gather(after(own_up, blocks_gate[1]), n)
    blocks_down = ring_gather(after(own_down, blocks_up[1]), n)
    full_gate = jnp.concatenate(blocks_gate, axis=0)
    full_up = jnp.concatenate(blocks_up, axis=0)
    full_down = jnp.concatenate(blocks_down, axis=0)

    attn_low, lse = attend(base, see, q, kv, qpos, qfirst, off, qh, kh, hd, scale)
    hidden = x_own + tp_scatter(dot(attn_low, full_out, NT, BF16))
    unit_mlp_own, rs_mlp = unit_rows(hidden)
    unit_mlp = tp_gather(unit_mlp_own.astype(BF16))

    gate = dot(unit_mlp, full_gate, NN)
    up = dot(unit_mlp, full_up, NN)
    sig = 1.0 / (1.0 + jnp.exp(-gate))
    silu = gate * sig
    act = (silu * up).astype(BF16)

    def cut(value, r):
        return value[:, r * width : (r + 1) * width]

    sum_down = ring_scatter(lambda r: dot(cut(grad_out, r), act, TN), n, width)
    grad_act = dot(grad_out, full_down, NN)
    d_up = (grad_act * silu).astype(BF16)
    d_gate = (grad_act * up * (sig * (1.0 + gate * (1.0 - sig)))).astype(BF16)
    sum_gate = ring_scatter(lambda r: dot(cut(unit_mlp, r), d_gate, TN), n, width)
    sum_up = ring_scatter(lambda r: dot(cut(unit_mlp, r), d_up, TN), n, width)
    m_mlp = tp_scatter((dot(d_gate, full_gate, NT) + dot(d_up, full_up, NT)).astype(BF16))
    grad_hidden = grad_out[:quarter].astype(F32) + norm_back(m_mlp, unit_mlp_own, rs_mlp)
    hidden_low = tp_gather(grad_hidden.astype(BF16))

    out_own = hidden + tp_scatter(dot(act, full_down, NT, BF16))
    layer_output = restore(tp_gather(out_own.astype(BF16)), cols, rows, n, BF16)

    sum_out = ring_scatter(lambda r: dot(cut(hidden_low, r), attn_low, TN), n, width)
    grad_heads = dot(hidden_low, full_out, NN, BF16)
    dq, dkv_all = attend_back(base, see, q, kv, grad_heads, attn_low, lse, qpos, qfirst, off, qh, kh, hd, scale)
    dkv = ring_scatter(lambda r: dkv_all[r * t : (r + 1) * t], n, t)
    d_qkv, d_gains = dqkv_call(dq, dkv, raw, cosine, sine, gains, qh, kh, hd)

    extra = 16
    gain_part = d_gains[:2].reshape(2, n, hd // n)
    gain_cols = jnp.take(gain_part, cols, axis=1)
    wide_qkv = d_qkv.shape[1]

    def qkv_part(r):
        tail = jnp.pad(gain_cols[:, r, :].reshape(1, -1), ((0, extra - 1), (0, wide_qkv - 2 * (hd // n))))
        return jnp.concatenate([dot(cut(unit_attn, r), d_qkv, TN), tail], axis=0)

    sum_qkv = ring_scatter(qkv_part, n, width + extra)
    m_attn = tp_scatter(dot(d_qkv, full_qkv, NT, BF16))
    unit_own, rs_own = unit_rows(x_own)
    input_own = grad_hidden + norm_back(m_attn, unit_own, rs_own)
    input_grad = restore(tp_gather(input_own.astype(BF16)), cols, rows, n, F32)

    head_gains = sum_qkv[width, : 2 * (hd // n)]
    sum_qkv = sum_qkv[:width]
    wide_own = jnp.concatenate([w_query, w_key, w_value], axis=1).astype(F32)
    d_norm_attn = jnp.sum(wide_own * sum_qkv, axis=1)
    d_norm_mlp = jnp.sum(w_gate.astype(F32) * sum_gate + w_up.astype(F32) * sum_up, axis=1)
    small = jnp.concatenate([d_norm_attn, d_norm_mlp, head_gains])
    small = jnp.pad(small, (0, -small.shape[0] % 1024)).reshape(-1, 128)
    small = tp_sum(small).reshape(-1)
    gain_at = 2 * width
    grad_qkv = sum_qkv * gain_attn
    q_cols, k_cols = qh * hd, (qh + kh) * hd
    return (
        layer_output,
        input_grad,
        grad_qkv[:, :q_cols],
        grad_qkv[:, q_cols:k_cols],
        grad_qkv[:, k_cols:],
        sum_out.T,
        sum_gate * gain_mlp,
        sum_up * gain_mlp,
        sum_down.T,
        small[:width],
        small[width:gain_at],
        small[gain_at : gain_at + hd // n],
        small[gain_at + hd // n : gain_at + 2 * (hd // n)],
    )


def solution(mesh):
    return jax.shard_map(
        partial(shards, mesh.shape["blk"]),
        mesh=mesh,
        in_specs=(
            P("blk", None),
            P("blk", "tp"),
            P("blk", "tp"),
            P("blk", "tp"),
            P("tp", "blk"),
            P("blk", "tp"),
            P("blk", "tp"),
            P("tp", "blk"),
            P("blk"),
            P("blk"),
            P(),
            P(),
            P("blk", None),
            P(),
            P(),
        ),
        out_specs=(
            P("blk", None),
            P("blk", None),
            P("blk", "tp"),
            P("blk", "tp"),
            P("blk", "tp"),
            P("tp", "blk"),
            P("blk", "tp"),
            P("blk", "tp"),
            P("tp", "blk"),
            P("blk"),
            P("blk"),
            P("blk"),
            P("blk"),
        ),
        check_vma=False,
    )
```

```python
from functools import partial

import jax
import jax.numpy as jnp
from jax import lax
from jax.experimental import pallas as pl
from jax.experimental.pallas import tpu as pltpu
from jax.sharding import PartitionSpec as P

EPS = 1e-06
ROPE_BASE = 1000000.0
F32 = jnp.float32
BF16 = jnp.bfloat16


def dot(a, b, dims, out=F32):
    return lax.dot_general(a, b, (dims, ((), ())), preferred_element_type=out)


NN = ((1,), (0,))
NT = ((1,), (1,))
TN = ((0,), (0,))


def ring_order(n):
    return list(range(0, n, 2)) + list(range(n - 1, 0, -2))


def ring_perms(n):
    order = ring_order(n)
    right = [(order[i], order[(i + 1) % n]) for i in range(n)]
    return right, [(b, a) for a, b in right]


def ring_gather(own, n):
    right, left = ring_perms(n)
    half = n // 2
    rows = own.shape[0] // 2
    blocks = [None] * n
    blocks[0] = own
    from_left = from_right = own
    for k in range(1, half):
        from_left = lax.ppermute(from_left, "blk", right)
        from_right = lax.ppermute(from_right, "blk", left)
        blocks[n - k] = from_left
        blocks[k] = from_right
    top = lax.ppermute(from_left[:rows], "blk", right)
    low = lax.ppermute(from_right[rows:], "blk", left)
    blocks[half] = jnp.concatenate([top, low], axis=0)
    return blocks


def ring_scatter(part, n, rows):
    right, left = ring_perms(n)
    half = n // 2
    cut = rows // 2
    far = part(half).astype(BF16)
    to_right = lax.ppermute(far[:cut], "blk", right).astype(F32)
    to_left = lax.ppermute(far[cut:], "blk", left).astype(F32)
    if half == 1:
        return part(0) + jnp.concatenate([to_right, to_left], axis=0)
    for k in range(half - 1, 0, -1):
        send_right, send_left = part(k), part(n - k)
        if k == half - 1:
            send_right = jnp.concatenate([send_right[:cut] + to_right, send_right[cut:]], axis=0)
            send_left = jnp.concatenate([send_left[:cut], send_left[cut:] + to_left], axis=0)
        else:
            send_right = send_right + to_right
            send_left = send_left + to_left
        to_right = lax.ppermute(send_right.astype(BF16), "blk", right).astype(F32)
        to_left = lax.ppermute(send_left.astype(BF16), "blk", left).astype(F32)
    return part(0) + to_right + to_left


CORE_SWAP = [(0, 1), (1, 0), (2, 3), (3, 2)]
X_SWAP = [(0, 2), (1, 3), (2, 0), (3, 1)]


def tp_scatter(value):
    q = value.shape[0] // 4
    value = value.reshape(4, q, value.shape[1])
    send = jnp.stack([value[1], value[3]]).astype(BF16)
    got = lax.ppermute(send, "tp", CORE_SWAP).astype(F32)
    far = (value[2].astype(F32) + got[1]).astype(BF16)
    got_far = lax.ppermute(far, "tp", X_SWAP).astype(F32)
    return value[0].astype(F32) + got[0] + got_far


def tp_gather(own):
    far = lax.ppermute(own, "tp", X_SWAP)
    pair = jnp.stack([own, far])
    other = lax.ppermute(pair, "tp", CORE_SWAP)
    return jnp.concatenate([own, other[0], far, other[1]], axis=0)


def tp_sum(value):
    value = value + lax.ppermute(value, "tp", CORE_SWAP)
    return value + lax.ppermute(value, "tp", X_SWAP)


def tp_pieces(own):
    core = lax.ppermute(own, "tp", CORE_SWAP)
    far = lax.ppermute(own, "tp", X_SWAP)
    return [own, core, far, lax.ppermute(far, "tp", CORE_SWAP)]


def tp_reduce(quarters):
    got_far = lax.ppermute(quarters[3], "tp", CORE_SWAP)
    got_near = lax.ppermute(quarters[1], "tp", CORE_SWAP)
    far = (quarters[2].astype(F32) + got_far.astype(F32)).astype(BF16)
    far = lax.ppermute(far, "tp", X_SWAP)
    return quarters[0].astype(F32) + got_near.astype(F32) + far.astype(F32)


NZ = 4


def z_shift(value, n, s):
    ny = n // NZ
    pairs = [(z * ny + y, (z + s) % NZ * ny + y) for z in range(NZ) for y in range(ny)]
    return lax.ppermute(value, "blk", pairs)


def y_shift(value, n, j):
    ny = n // NZ
    pairs = [(z * ny + y, z * ny + (y + j) % ny) for z in range(NZ) for y in range(ny)]
    return lax.ppermute(value, "blk", pairs)


def pack_kernel(zs_ref, gate_ref, up_ref, down_ref, gain_ref, *out_refs):
    part = gate_ref.shape[1] // NZ
    gain = gain_ref[...]
    for s in range(NZ):
        at = pl.ds(pl.multiple_of(zs_ref[s] * part, part), part)
        out_refs[s][:, :part] = (gate_ref[:, at].astype(F32) * gain).astype(BF16)
        out_refs[s][:, part : 2 * part] = (up_ref[:, at].astype(F32) * gain).astype(BF16)
        out_refs[s][:, 2 * part :] = down_ref[at, :].astype(F32).T.astype(BF16)


VMEM = pl.BlockSpec(memory_space=pltpu.VMEM)
SMEM = pl.BlockSpec(memory_space=pltpu.SMEM)


def pack(zs, w_gate, w_up, w_down, gain):
    rows, cols = w_gate.shape
    shape = jax.ShapeDtypeStruct((rows, 3 * cols // NZ), BF16)
    return pl.pallas_call(
        pack_kernel,
        in_specs=[SMEM, VMEM, VMEM, VMEM, VMEM],
        out_specs=[VMEM] * NZ,
        out_shape=[shape] * NZ,
        name="pack",
    )(zs, w_gate, w_up, w_down, gain)


def place_kernel(at_ref, *refs):
    out_ref = refs[-1]
    rows = refs[0].shape[0]
    for i, ref in enumerate(refs[:-1]):
        out_ref[pl.ds(pl.multiple_of(at_ref[i] * rows, rows), rows), :] = ref[...]


def place_rows(at, pieces):
    rows, cols = pieces[0].shape
    return pl.pallas_call(
        place_kernel,
        in_specs=[SMEM] + [VMEM] * len(pieces),
        out_specs=VMEM,
        out_shape=jax.ShapeDtypeStruct((len(pieces) * rows, cols), BF16),
        name="place_rows",
    )(at, *pieces)


def mlp_kernel(*refs):
    u_refs, g_refs, w_ref = refs[:4], refs[4:8], refs[8]
    act_ref, dgu_ref = refs[9], refs[10]
    gm_refs = refs[11:15]
    u_all, g_all = refs[15], refs[16]
    q, d = u_refs[0].shape
    part = w_ref.shape[1] // 3
    for i in range(4):
        u_all[i * q : (i + 1) * q, :] = u_refs[i][...]
        g_all[i * q : (i + 1) * q, :] = g_refs[i][...]
    gate_up = dot(u_all[...], w_ref[:, : 2 * part], NN)
    grad_act = dot(g_all[...], w_ref[:, 2 * part :], NN)
    gate, up = gate_up[:, :part], gate_up[:, part:]
    sig = 1.0 / (1.0 + jnp.exp(-gate))
    silu = gate * sig
    act_ref[...] = (silu * up).astype(BF16)
    dgu_ref[:, part:] = (grad_act * silu).astype(BF16)
    dgu_ref[:, :part] = (grad_act * up * (sig * (1.0 + gate * (1.0 - sig)))).astype(BF16)
    tile = 512

    @pl.loop(0, d // tile)
    def _(c):
        at = pl.ds(pl.multiple_of(c * tile, tile), tile)
        gm = dot(dgu_ref[...], w_ref[at, : 2 * part], NT).astype(BF16)
        for i in range(4):
            gm_refs[i][:, at] = gm[i * q : (i + 1) * q, :]


def mlp_call(u, g, w):
    q, d = u[0].shape
    part = w.shape[1] // 3
    quarter = jax.ShapeDtypeStruct((q, d), BF16)
    out = pl.pallas_call(
        mlp_kernel,
        in_specs=[VMEM] * 9,
        out_specs=[VMEM] * 6,
        out_shape=[
            jax.ShapeDtypeStruct((4 * q, part), BF16),
            jax.ShapeDtypeStruct((4 * q, 2 * part), BF16),
        ]
        + [quarter] * 4,
        scratch_shapes=[pltpu.VMEM((4 * q, d), BF16), pltpu.VMEM((4 * q, d), BF16)],
        cost_estimate=pl.CostEstimate(
            flops=8 * q * d * part * 5, bytes_accessed=2 * (12 * q * d + 3 * part * d), transcendentals=0
        ),
        name="mlp",
    )(*u, *g, w)
    return out[0], out[1], out[2:]


def down_kernel(act_ref, w_ref, *out_refs):
    q, d = out_refs[0].shape
    part = act_ref.shape[1]
    tile = 512

    @pl.loop(0, d // tile)
    def _(c):
        at = pl.ds(pl.multiple_of(c * tile, tile), tile)
        y = dot(act_ref[...], w_ref[at, 2 * part :], NT).astype(BF16)
        for i in range(4):
            out_refs[i][:, at] = y[i * q : (i + 1) * q, :]


def down_call(act, w):
    q, part = act.shape[0] // 4, act.shape[1]
    d = w.shape[0]
    return pl.pallas_call(
        down_kernel,
        in_specs=[VMEM, VMEM],
        out_specs=[VMEM] * 4,
        out_shape=[jax.ShapeDtypeStruct((q, d), BF16)] * 4,
        cost_estimate=pl.CostEstimate(
            flops=8 * q * d * part, bytes_accessed=2 * (4 * q * d + 3 * part * d), transcendentals=0
        ),
        name="down",
    )(act, w)


def wgrad_kernel(n, at_ref, *refs):
    u_refs, g_refs = refs[: 4 * NZ], refs[4 * NZ : 8 * NZ]
    dgu_refs, act_refs = refs[8 * NZ : 9 * NZ], refs[9 * NZ : 10 * NZ]
    out_refs, acc = refs[10 * NZ : -1], refs[-1]
    q, d = u_refs[0].shape
    part = act_refs[0].shape[1]
    tile = 256

    @pl.loop(0, d // tile)
    def _(c):
        at = pl.ds(pl.multiple_of(c * tile, tile), tile)
        gu = dn = None
        for s in range(NZ):
            u = jnp.concatenate([u_refs[4 * s + i][:, at] for i in range(4)], axis=0)
            g = jnp.concatenate([g_refs[4 * s + i][:, at] for i in range(4)], axis=0)
            gu_s = dot(u, dgu_refs[s][...], TN)
            dn_s = dot(g, act_refs[s][...], TN)
            gu = gu_s if gu is None else gu + gu_s
            dn = dn_s if dn is None else dn + dn_s
        acc[at, : 2 * part] = gu.astype(BF16)
        acc[at, 2 * part :] = dn.astype(BF16)

    rows = d // n
    for i, ref in enumerate(out_refs):
        ref[...] = acc[pl.ds(pl.multiple_of(at_ref[i] * rows, rows), rows), :]


def wgrad_call(n, at, u, g, dgu, act):
    q, d = u[0][0].shape
    part = act[0].shape[1]
    flat_u = [p for slot in u for p in slot]
    flat_g = [p for slot in g for p in slot]
    return pl.pallas_call(
        partial(wgrad_kernel, n),
        in_specs=[SMEM] + [VMEM] * (10 * NZ),
        out_specs=[VMEM] * n,
        out_shape=[jax.ShapeDtypeStruct((d // n, 3 * part), BF16)] * n,
        scratch_shapes=[pltpu.VMEM((d, 3 * part), BF16)],
        cost_estimate=pl.CostEstimate(
            flops=2 * 16 * q * d * part * 3, bytes_accessed=64 * q * d + 6 * d * part, transcendentals=0
        ),
        name="wgrad",
    )(at, *flat_u, *flat_g, *dgu, *act)


def finish_kernel(zs_ref, *refs):
    pieces = refs[:NZ]
    gate_ref, up_ref, gain_ref, d_gate, d_up, d_down, d_norm = refs[NZ:]
    part = gate_ref.shape[1] // NZ
    gain = gain_ref[...]
    norm = jnp.zeros((gate_ref.shape[0], 1), F32)
    for s in range(NZ):
        at = pl.ds(pl.multiple_of(zs_ref[s] * part, part), part)
        grad = pieces[s][:, :part].astype(F32)
        norm = norm + jnp.sum(grad * gate_ref[:, at].astype(F32), axis=1, keepdims=True)
        d_gate[:, at] = grad * gain
        grad = pieces[s][:, part : 2 * part].astype(F32)
        norm = norm + jnp.sum(grad * up_ref[:, at].astype(F32), axis=1, keepdims=True)
        d_up[:, at] = grad * gain
        d_down[at, :] = pieces[s][:, 2 * part :].astype(F32).T
    d_norm[...] = norm


def finish(zs, pieces, w_gate, w_up, gain):
    rows, cols = w_gate.shape
    return pl.pallas_call(
        finish_kernel,
        in_specs=[SMEM] + [VMEM] * (NZ + 3),
        out_specs=[VMEM] * 4,
        out_shape=[
            jax.ShapeDtypeStruct((rows, cols), F32),
            jax.ShapeDtypeStruct((rows, cols), F32),
            jax.ShapeDtypeStruct((cols, rows), F32),
            jax.ShapeDtypeStruct((rows, 1), F32),
        ],
        name="finish",
    )(zs, *pieces, w_gate, w_up, gain)


MESH = pl.DeviceIdType.MESH


class Wires:
    def __init__(self, send, recv):
        self.send, self.recv, self.sent, self.done = send, recv, [], []

    def go(self, src, dst, device):
        i = len(self.sent)
        copy = pltpu.make_async_remote_copy(
            src_ref=src,
            dst_ref=dst,
            send_sem=self.send.at[i],
            recv_sem=self.recv.at[i],
            device_id=device,
            device_id_type=MESH,
        )
        copy.start()
        self.sent.append(copy)
        return copy

    def drain(self, copies):
        for copy in copies:
            copy.wait_send()
            self.done.append(copy)

    def close(self):
        self.drain([copy for copy in self.sent if not any(copy is other for other in self.done)])


def greet(devices):
    barrier = pltpu.get_barrier_semaphore()
    for device in devices:
        pl.semaphore_signal(barrier, inc=1, device_id=device, device_id_type=MESH)
    pl.semaphore_wait(barrier, len(devices))


class Spot:
    def __init__(self, n):
        self.n, self.ny = n, n // NZ
        self.blk, self.tp = lax.axis_index("blk"), lax.axis_index("tp")
        self.z, self.y = self.blk // self.ny, self.blk % self.ny
        self.x, self.core = self.tp // 2, self.tp % 2
        self.tp_core = self.x * 2 + (1 - self.core)
        self.tp_far = (1 - self.x) * 2 + self.core
        self.core_dev = {"tp": self.tp_core}
        self.far_dev = {"tp": self.tp_far}

    def plane(self, s):
        return (self.z + s) % NZ

    def z_dev(self, s):
        return {"blk": self.plane(s) * self.ny + self.y}

    def y_dev(self, j):
        return {"blk": self.z * self.ny + (self.y + j) % self.ny}

    def peers(self):
        return (
            [self.core_dev, self.far_dev]
            + [self.z_dev(s) for s in range(1, NZ)]
            + [self.y_dev(j) for j in range(1, self.ny)]
        )


def rows_at(index, count):
    return pl.ds(pl.multiple_of(index * count, count), count)


def feed_copies(n):
    ny = n // NZ
    return 3 + 4 * (ny - 1) + 2 * 3 + 8 * 3 + 3 + 4 * 3 + 3 + 3


def feed_kernel(n, attn, wo, x_own, g_rows, *refs):
    packed = refs[:NZ]
    hidden_o, gh_o, heads_o, hl_o, dw_o, act_o, w_o = refs[NZ : NZ + 7]
    (u_all, g_all, dgu, o_part, o_far, o_core, o_x, part, far, near, core_in, x_in, z_in, m_acc, dw_tile, send, recv, dw_sem) = refs[NZ + 7 :]
    q, d = x_own.shape
    unit_w = 3 * (packed[0].shape[1] // 3)
    p = unit_w // 3
    bw = packed[0].shape[0]
    me = Spot(n)
    wires = Wires(send, recv)
    greet(me.peers())

    def quarter(plane, peer):
        return rows_at(plane * 4 + peer, q)

    mine = rows_at(me.blk, bw)
    w_z = {s: wires.go(packed[s], w_o.at[mine], me.z_dev(s)) for s in (1, 3, 2)}
    w_y = [wires.go(packed[0], w_o.at[mine], me.y_dev(j)) for j in range(1, me.ny)]
    w_o[mine, :] = packed[0][...]

    g_all[rows_at(me.z, 4 * q), :] = g_rows[...]

    def project(peer):
        return dot(attn[rows_at(peer, q), :], wo[...], NT)

    for i, x in enumerate((1 - me.x, me.x)):
        o_part[i] = project(x * 2 + 1 - me.core).astype(BF16)
    far_in = wires.go(o_part.at[0], o_core.at[0], me.core_dev)
    near_in = wires.go(o_part.at[1], o_core.at[1], me.core_dev)
    own_far = project(me.tp_far)
    far_in.wait_recv()
    o_far[...] = (own_far + o_core[0].astype(F32)).astype(BF16)
    x_sum = wires.go(o_far, o_x, me.far_dev)
    own_sum = project(me.tp) + x_own[...]
    near_in.wait_recv()
    own_sum = own_sum + o_core[1].astype(F32)
    x_sum.wait_recv()
    hidden = own_sum + o_x[...].astype(F32)
    hidden_o[...] = hidden
    rs = lax.rsqrt(jnp.mean(hidden * hidden, axis=-1, keepdims=True) + EPS)
    own_q = quarter(me.z, me.tp)
    u_all[own_q, :] = (hidden * rs).astype(BF16)

    def pass_on(buf, plane):
        at = quarter(plane, me.tp)
        return wires.go(buf.at[at], buf.at[at], me.far_dev), wires.go(buf.at[at], buf.at[at], me.core_dev)

    def pass_far(buf, plane, copies):
        copies[0].wait_recv()
        at = quarter(plane, me.tp_far)
        return wires.go(buf.at[at], buf.at[at], me.core_dev)

    own_pass = pass_on(u_all, me.z)
    u_z, g_z = {}, {}
    for s in (1, 3, 2):
        u_z[s] = wires.go(u_all.at[own_q], u_all.at[own_q], me.z_dev(s))
    for s in (1, 3, 2):
        w_z[s].wait_recv()
        at = rows_at(me.plane(-s) * me.ny + me.y, bw)
        w_y += [wires.go(w_o.at[at], w_o.at[at], me.y_dev(j)) for j in range(1, me.ny)]
    for s in (1, 3, 2):
        g_z[s] = wires.go(g_all.at[own_q], g_all.at[own_q], me.z_dev(s))
    own_far_pass = pass_far(u_all, me.z, own_pass)
    for copy in w_y:
        copy.wait_recv()
    own_pass[1].wait_recv()
    own_far_pass.wait_recv()

    def compute(i, plane):
        @pl.loop(0, 2)
        def _(k):
            at = pl.ds(pl.multiple_of(plane * (4 * q) + k * (2 * q), 2 * q), 2 * q)
            gate_up = dot(u_all[at, :], w_o[:, : 2 * p], NN)
            grad_act = dot(g_all[at, :], w_o[:, 2 * p :], NN)
            gate, up = gate_up[:, :p], gate_up[:, p:]
            sig = 1.0 / (1.0 + jnp.exp(-gate))
            silu = gate * sig
            act_o[at, :] = (silu * up).astype(BF16)
            dgu[at, p:] = (grad_act * silu).astype(BF16)
            dgu[at, :p] = (grad_act * up * (sig * (1.0 + gate * (1.0 - sig)))).astype(BF16)

        rows = rows_at(plane, 4 * q)
        tile = 512

        @pl.loop(0, d // tile)
        def _(c):
            at = pl.ds(pl.multiple_of(c * tile, tile), tile)
            part[i % 2, :, at] = dot(dgu[rows, :], w_o[at, : 2 * p], NT).astype(BF16)

    def reduce_core(i):
        out = []
        for k, x in enumerate((1 - me.x, me.x)):
            src = part.at[i % 2, rows_at(x * 2 + 1 - me.core, q)]
            out.append(wires.go(src, core_in.at[i, k], me.core_dev))
        return out

    def reduce_far(i, copies):
        copies[0].wait_recv()
        far[i] = (part[i % 2, rows_at(me.tp_far, q), :].astype(F32) + core_in[i, 0].astype(F32)).astype(BF16)
        return wires.go(far.at[i], x_in.at[i], me.far_dev)

    def reduce_near(i, copies, x_copy):
        copies[1].wait_recv()
        x_copy.wait_recv()
        return part[i % 2, rows_at(me.tp, q), :].astype(F32) + core_in[i, 1].astype(F32) + x_in[i].astype(F32)

    order = (1, 3, 2)

    def finish_slot(i):
        value = reduce_near(i, cores[i], fars[i])
        wires.drain(cores[i])
        if i == 0:
            m_acc[...] = value
            return None
        near[i - 1] = value.astype(BF16)
        return wires.go(near.at[i - 1], z_in.at[i - 1], me.z_dev(-order[i - 1]))

    def dw_copy(c, slot):
        rows = pl.ds(pl.multiple_of(c * 256, 256), 256)
        return pltpu.make_async_copy(dw_tile.at[slot], dw_o.at[rows], dw_sem.at[slot])

    def grads(first, last):
        @pl.loop(first, last)
        def _(c):
            slot = c % 2

            @pl.when(c >= 2)
            def _():
                dw_copy(c - 2, slot).wait()

            at = pl.ds(pl.multiple_of(c * 256, 256), 256)
            dw_tile[slot, :, : 2 * p] = dot(u_all[:, at], dgu[...], TN).astype(BF16)
            dw_tile[slot, :, 2 * p :] = dot(g_all[:, at], act_o[...], TN).astype(BF16)
            dw_copy(c, slot).start()

    compute(0, me.z)
    cores, fars, backs = [reduce_core(0)], [], []
    passes = []
    for s in order:
        plane = me.plane(-s)
        u_z[s].wait_recv()
        u_copies = pass_on(u_all, plane)
        g_z[s].wait_recv()
        passes.append((u_copies, pass_on(g_all, plane)))
    for i, s in enumerate(order):
        plane = me.plane(-s)
        u_copies, g_copies = passes[i]
        u_last = pass_far(u_all, plane, u_copies)
        g_last = pass_far(g_all, plane, g_copies)
        fars.append(reduce_far(i, cores[i]))
        if i >= 1:
            backs.append(finish_slot(i - 1))
        u_copies[1].wait_recv()
        g_copies[1].wait_recv()
        u_last.wait_recv()
        g_last.wait_recv()
        compute(i + 1, plane)
        cores.append(reduce_core(i + 1))
    tiles = d // 256
    fars.append(reduce_far(NZ - 1, cores[NZ - 1]))
    backs.append(finish_slot(NZ - 2))
    grads(0, tiles // 2)
    backs.append(finish_slot(NZ - 1))
    grads(tiles // 2, tiles)
    m = m_acc[...]
    for i in range(1, NZ):
        backs[i].wait_recv()
        m = m + z_in[i - 1].astype(F32)

    hidden = hidden_o[...]
    rs = lax.rsqrt(jnp.mean(hidden * hidden, axis=-1, keepdims=True) + EPS)
    unit = hidden * rs
    grad = g_rows[rows_at(me.tp, q), :].astype(F32) + (m - unit * jnp.mean(m * unit, axis=-1, keepdims=True)) * rs
    gh_o[...] = grad
    own = rows_at(me.tp, q)
    hl_o[own, :] = grad.astype(BF16)
    x_copy = wires.go(hl_o.at[own], hl_o.at[own], me.far_dev)
    c_copy = wires.go(hl_o.at[own], hl_o.at[own], me.core_dev)

    def heads(peer):
        heads_o[rows_at(peer, q), :] = dot(hl_o[rows_at(peer, q), :], wo[...], NN).astype(BF16)

    heads(me.tp)
    c_copy.wait_recv()
    heads(me.tp_core)
    x_copy.wait_recv()
    at = rows_at(me.tp_far, q)
    last = wires.go(hl_o.at[at], hl_o.at[at], me.core_dev)
    heads(me.tp_far)
    last.wait_recv()
    heads((1 - me.x) * 2 + 1 - me.core)
    for c in (tiles - 2, tiles - 1):
        dw_copy(c, c % 2).wait()
    wires.close()


def feed(n, attn, wo, x_own, g_rows, packed):
    q, d = x_own.shape
    t, a = attn.shape
    bw, w3 = packed[0].shape
    p = w3 // 3
    tokens = NZ * t
    copies = feed_copies(n)
    vm = pltpu.VMEM
    return pl.pallas_call(
        partial(feed_kernel, n),
        in_specs=[VMEM] * (4 + NZ),
        out_specs=[VMEM] * 4 + [pl.BlockSpec(memory_space=pl.ANY)] + [VMEM] * 2,
        out_shape=[
            jax.ShapeDtypeStruct((q, d), F32),
            jax.ShapeDtypeStruct((q, d), F32),
            jax.ShapeDtypeStruct((t, a), BF16),
            jax.ShapeDtypeStruct((t, d), BF16),
            jax.ShapeDtypeStruct((d, w3), BF16),
            jax.ShapeDtypeStruct((tokens, p), BF16),
            jax.ShapeDtypeStruct((d, w3), BF16),
        ],
        scratch_shapes=[
            vm((tokens, d), BF16),
            vm((tokens, d), BF16),
            vm((tokens, 2 * p), BF16),
            vm((2, q, d), BF16),
            vm((q, d), BF16),
            vm((2, q, d), BF16),
            vm((q, d), BF16),
            vm((2, t, d), BF16),
            vm((NZ, q, d), BF16),
            vm((NZ - 1, q, d), BF16),
            vm((NZ, 2, q, d), BF16),
            vm((NZ, q, d), BF16),
            vm((NZ - 1, q, d), BF16),
            vm((q, d), F32),
            vm((2, 256, w3), BF16),
            pltpu.SemaphoreType.DMA((copies,)),
            pltpu.SemaphoreType.DMA((copies,)),
            pltpu.SemaphoreType.DMA((2,)),
        ],
        compiler_params=pltpu.CompilerParams(
            collective_id=1, has_side_effects=True, vmem_limit_bytes=67000000
        ),
        name="feed",
    )(attn, wo, x_own, g_rows, *packed)


def columns_kernel(n, to_ring, cols_ref, x_ref, out_ref):
    width = x_ref.shape[1] // n
    for r in range(n):
        at = pl.ds(pl.multiple_of(cols_ref[r] * width, width), width)
        to = pl.ds(r * width, width)
        if to_ring:
            out_ref[:, to] = x_ref[:, at]
        else:
            out_ref[:, at] = x_ref[:, to]


def columns(x, cols, n, to_ring):
    t, d = x.shape
    if (d // n) % 128:
        index = cols if to_ring else jnp.argsort(cols)
        return jnp.take(x.reshape(t, n, d // n), index, axis=1).reshape(t, d)
    return pl.pallas_call(
        partial(columns_kernel, n, to_ring),
        in_specs=[SMEM, VMEM],
        out_specs=VMEM,
        out_shape=jax.ShapeDtypeStruct((t, d), x.dtype),
        name="columns",
    )(cols, x)


def arrange_kernel(n, cols_ref, x_ref, u_ref):
    width = x_ref.shape[1] // n
    x = x_ref[...].astype(F32)
    rs = lax.rsqrt(jnp.mean(x * x, axis=-1, keepdims=True) + EPS)
    for r in range(n):
        at = pl.ds(pl.multiple_of(cols_ref[r] * width, width), width)
        u_ref[:, r * width : (r + 1) * width] = (x_ref[:, at].astype(F32) * rs).astype(BF16)


def arrange(x, cols, n):
    t, d = x.shape
    quarter = t // 4
    if (d // n) % 128:
        wide = x.astype(F32)
        rs = lax.rsqrt(jnp.mean(wide * wide, axis=-1, keepdims=True) + EPS)
        return jnp.take((wide * rs).astype(BF16).reshape(t, n, d // n), cols, axis=1).reshape(t, d)
    spec = pl.BlockSpec((quarter, d), lambda j, c: (j, 0))
    return pl.pallas_call(
        partial(arrange_kernel, n),
        grid_spec=pltpu.PrefetchScalarGridSpec(num_scalar_prefetch=1, grid=(4,), in_specs=[spec], out_specs=spec),
        out_shape=jax.ShapeDtypeStruct((t, d), BF16),
        name="arrange",
    )(cols, x)


def restore_kernel(n, cols_ref, rows_ref, x0, x1, x2, x3, out_ref):
    width = out_ref.shape[1] // n
    step = pl.program_id(0)
    for j, x_ref in enumerate((x0, x1, x2, x3)):

        @pl.when(step == j)
        def _():
            if n == 1:
                out_ref[...] = x_ref[...].astype(out_ref.dtype)
            for r in range(n if n > 1 else 0):
                at = pl.ds(pl.multiple_of(cols_ref[r] * width, width), width)
                out_ref[:, at] = x_ref[:, r * width : (r + 1) * width].astype(out_ref.dtype)


def restore(pieces, cols, rows, n, dtype):
    quarter, d = pieces[0].shape
    if (d // n) % 128:
        pieces, n = [columns(p, cols, n, False) for p in pieces], 1
    whole = pl.BlockSpec((quarter, d), lambda j, c, r: (0, 0))
    return pl.pallas_call(
        partial(restore_kernel, n),
        grid_spec=pltpu.PrefetchScalarGridSpec(
            num_scalar_prefetch=2,
            grid=(4,),
            in_specs=[whole] * 4,
            out_specs=pl.BlockSpec((quarter, d), lambda j, c, r: (r[j], 0)),
        ),
        out_shape=jax.ShapeDtypeStruct((4 * quarter, d), dtype),
        name="restore",
    )(cols, rows, *pieces)


def turned(v, sine):
    return pltpu.roll(v, v.shape[1] // 2, 1) * sine


def qkv_kernel(heads, hd, u_ref, w_ref, cos_ref, sin_ref, gain_ref, raw_q, raw_k, q_ref, kv_ref):
    qh, kh = heads
    y = dot(u_ref[...], w_ref[...], NN)
    raw_q[...] = y[:, : qh * hd]
    raw_k[...] = y[:, qh * hd : (qh + kh) * hd]
    cosine, sine = cos_ref[...], sin_ref[...]
    for h in range(qh + kh):
        v = y[:, h * hd : (h + 1) * hd]
        rs = lax.rsqrt(jnp.mean(v * v, axis=-1, keepdims=True) + EPS)
        v = v * rs * gain_ref[0 if h < qh else 1]
        v = (v * cosine + turned(v, sine)).astype(BF16)
        if h < qh:
            q_ref[:, h * hd : (h + 1) * hd] = v
        else:
            kv_ref[:, (h - qh) * hd : (h - qh + 1) * hd] = v
    kv_ref[:, kh * hd :] = y[:, (qh + kh) * hd :].astype(BF16)


def qkv_call(u, w, cosine, sine, gains, qh, kh, hd):
    t, d = u.shape
    rows = t // 4
    width = w.shape[1]
    return pl.pallas_call(
        partial(qkv_kernel, (qh, kh), hd),
        grid=(4,),
        in_specs=[
            pl.BlockSpec((rows, d), lambda i: (i, 0)),
            pl.BlockSpec((d, width), lambda i: (0, 0)),
            pl.BlockSpec((rows, hd), lambda i: (i, 0)),
            pl.BlockSpec((rows, hd), lambda i: (i, 0)),
            pl.BlockSpec((2, 1, hd), lambda i: (0, 0, 0)),
        ],
        out_specs=[
            pl.BlockSpec((rows, qh * hd), lambda i: (i, 0)),
            pl.BlockSpec((rows, kh * hd), lambda i: (i, 0)),
            pl.BlockSpec((rows, qh * hd), lambda i: (i, 0)),
            pl.BlockSpec((rows, 2 * kh * hd), lambda i: (i, 0)),
        ],
        out_shape=[
            jax.ShapeDtypeStruct((t, qh * hd), F32),
            jax.ShapeDtypeStruct((t, kh * hd), F32),
            jax.ShapeDtypeStruct((t, qh * hd), BF16),
            jax.ShapeDtypeStruct((t, 2 * kh * hd), BF16),
        ],
        cost_estimate=pl.CostEstimate(
            flops=2 * t * d * width, bytes_accessed=2 * d * (t + width), transcendentals=0
        ),
        name="qkv",
    )(u, w, cosine, sine, gains)


def head_back_kernel(heads, hd, grad_ref, raw_ref, cos_ref, sin_ref, gain_ref, out_ref, dgain_ref):
    cosine, sine = cos_ref[...], sin_ref[...]
    total = jnp.zeros((1, hd), F32)
    gain = gain_ref[...]
    for h in range(heads):
        at = slice(h * hd, (h + 1) * hd)
        grad = grad_ref[:, at].astype(F32)
        grad = grad * cosine - turned(grad, sine)
        v = raw_ref[:, at]
        rs = lax.rsqrt(jnp.mean(v * v, axis=-1, keepdims=True) + EPS)
        unit = v * rs
        total = total + jnp.sum(grad * unit, axis=0, keepdims=True)
        m = grad * gain
        back = (m - unit * jnp.mean(m * unit, axis=-1, keepdims=True)) * rs
        out_ref[:, at] = back.astype(BF16)
    if heads * hd < grad_ref.shape[1]:
        out_ref[:, heads * hd :] = grad_ref[:, heads * hd :].astype(BF16)

    @pl.when(pl.program_id(0) == 0)
    def _():
        dgain_ref[...] = jnp.zeros_like(dgain_ref)

    dgain_ref[0:1, :] += total


def head_back(grad, raw, cosine, sine, gain, heads, hd, name):
    t, width = grad.shape
    rows = t // 4

    def rowwise(cols):
        return pl.BlockSpec((rows, cols), lambda i: (i, 0))

    return pl.pallas_call(
        partial(head_back_kernel, heads, hd),
        grid=(4,),
        in_specs=[
            rowwise(width),
            rowwise(heads * hd),
            rowwise(hd),
            rowwise(hd),
            pl.BlockSpec((1, hd), lambda i: (0, 0)),
        ],
        out_specs=[rowwise(width), pl.BlockSpec((8, hd), lambda i: (0, 0))],
        out_shape=[jax.ShapeDtypeStruct((t, width), BF16), jax.ShapeDtypeStruct((8, hd), F32)],
        name=name,
    )(grad, raw, cosine, sine, gain)


def tile_masks(base_ref, tile, qpos_ref, qfirst_ref, off_ref, q0, stretch):
    kpos = off_ref[...] + base_ref[tile]
    qpos = qpos_ref[pl.ds(q0, stretch), :]
    qfirst = qfirst_ref[pl.ds(q0, stretch), :]
    return (kpos <= qpos) & (kpos >= qfirst)


def attend_kernel(dims, scale, base_ref, see_ref, q_ref, kv_ref, qpos_ref, qfirst_ref, off_ref, out_ref, lse_ref, acc_ref, sum_ref):
    qh, kh, hd, stretch = dims
    group = qh // kh
    tile = pl.program_id(0)
    last = pl.num_programs(0) - 1

    @pl.when(tile == 0)
    def _():
        acc_ref[...] = jnp.zeros_like(acc_ref)
        sum_ref[...] = jnp.zeros_like(sum_ref)

    for e in range(2):
        q0 = e * stretch

        @pl.when(see_ref[e, tile] > 0)
        def _():
            mask = tile_masks(base_ref, tile, qpos_ref, qfirst_ref, off_ref, q0, stretch)
            for h in range(qh):
                k = kv_ref[:, (h // group) * hd : (h // group + 1) * hd]
                v = kv_ref[:, (kh + h // group) * hd : (kh + h // group + 1) * hd]
                q = q_ref[q0 : q0 + stretch, h * hd : (h + 1) * hd]
                s = dot(q, k, NT) * scale
                p = jnp.where(mask, jnp.exp(s), 0.0)
                sum_ref[h, q0 : q0 + stretch, :] += jnp.sum(p, axis=-1, keepdims=True)
                acc_ref[q0 : q0 + stretch, h * hd : (h + 1) * hd] += dot(p.astype(BF16), v, NN)

    @pl.when(tile == last)
    def _():
        for h in range(qh):
            total = sum_ref[h]
            out_ref[:, h * hd : (h + 1) * hd] = (acc_ref[:, h * hd : (h + 1) * hd] / total).astype(BF16)
            lse_ref[h] = jnp.log(total)


def attend(base, see, q, kv, qpos, qfirst, off, qh, kh, hd, scale):
    t = q.shape[0]
    stretch = t // 2
    tiles = kv.shape[0] // stretch

    def whole(shape):
        return pl.BlockSpec(shape, lambda i, *_: (0,) * len(shape))

    return pl.pallas_call(
        partial(attend_kernel, (qh, kh, hd, stretch), scale),
        grid_spec=pltpu.PrefetchScalarGridSpec(
            num_scalar_prefetch=2,
            grid=(tiles,),
            in_specs=[
                whole((t, qh * hd)),
                pl.BlockSpec((stretch, 2 * kh * hd), lambda i, *_: (i, 0)),
                whole((t, 1)),
                whole((t, 1)),
                whole((1, stretch)),
            ],
            out_specs=[whole((t, qh * hd)), whole((qh, t, 1))],
            scratch_shapes=[pltpu.VMEM((t, qh * hd), F32), pltpu.VMEM((qh, t, 1), F32)],
        ),
        out_shape=[
            jax.ShapeDtypeStruct((t, qh * hd), BF16),
            jax.ShapeDtypeStruct((qh, t, 1), F32),
        ],
        cost_estimate=pl.CostEstimate(
            flops=4 * t * kv.shape[0] * hd * qh, bytes_accessed=2 * kv.size, transcendentals=t * kv.shape[0]
        ),
        name="attend",
    )(base, see, q, kv, qpos, qfirst, off)


def attend_back_kernel(
    dims, scale, base_ref, see_ref, q_ref, kv_ref, do_ref, o_ref, lse_ref, qpos_ref, qfirst_ref, off_ref, dq_ref, dkv_ref, acc_ref, delta_ref
):
    qh, kh, hd, stretch = dims
    group = qh // kh
    tile = pl.program_id(0)
    last = pl.num_programs(0) - 1

    @pl.when(tile == 0)
    def _():
        acc_ref[...] = jnp.zeros_like(acc_ref)
        for h in range(qh):
            at = slice(h * hd, (h + 1) * hd)
            delta_ref[h] = jnp.sum(do_ref[:, at].astype(F32) * o_ref[:, at].astype(F32), axis=-1, keepdims=True)

    sees = [see_ref[0, tile] > 0, see_ref[1, tile] > 0]

    @pl.when(jnp.logical_not(sees[0]))
    def _():
        dkv_ref[...] = jnp.zeros_like(dkv_ref)

    def half(e, add):
        q0 = e * stretch
        mask = tile_masks(base_ref, tile, qpos_ref, qfirst_ref, off_ref, q0, stretch)
        for c in range(kh):
            k = kv_ref[:, c * hd : (c + 1) * hd]
            v = kv_ref[:, (kh + c) * hd : (kh + c + 1) * hd]
            dk = dv = None
            for h in range(c * group, (c + 1) * group):
                at = slice(h * hd, (h + 1) * hd)
                q = q_ref[q0 : q0 + stretch, at]
                do = do_ref[q0 : q0 + stretch, at]
                s = dot(q, k, NT) * scale
                p = jnp.where(mask, jnp.exp(s - lse_ref[h, q0 : q0 + stretch, :]), 0.0)
                dp = dot(do, v, NT)
                ds = (p * (dp - delta_ref[h, q0 : q0 + stretch, :])).astype(BF16)
                acc_ref[q0 : q0 + stretch, at] += dot(ds, k, NN)
                dk_h = dot(ds, q, TN)
                dv_h = dot(p.astype(BF16), do, TN)
                dk = dk_h if dk is None else dk + dk_h
                dv = dv_h if dv is None else dv + dv_h
            ck = slice(c * hd, (c + 1) * hd)
            cv = slice((kh + c) * hd, (kh + c + 1) * hd)
            if add:
                dkv_ref[:, ck] += dk * scale
                dkv_ref[:, cv] += dv
            else:
                dkv_ref[:, ck] = dk * scale
                dkv_ref[:, cv] = dv

    for e in range(2):

        @pl.when(sees[e])
        def _():
            half(e, e == 1)

    @pl.when(tile == last)
    def _():
        dq_ref[...] = acc_ref[...] * scale


def attend_back(base, see, q, kv, do, o, lse, qpos, qfirst, off, qh, kh, hd, scale):
    t = q.shape[0]
    stretch = t // 2
    tiles = kv.shape[0] // stretch

    def whole(shape):
        return pl.BlockSpec(shape, lambda i, *_: (0,) * len(shape))

    tile_spec = pl.BlockSpec((stretch, 2 * kh * hd), lambda i, *_: (i, 0))
    return pl.pallas_call(
        partial(attend_back_kernel, (qh, kh, hd, stretch), scale),
        grid_spec=pltpu.PrefetchScalarGridSpec(
            num_scalar_prefetch=2,
            grid=(tiles,),
            in_specs=[
                whole((t, qh * hd)),
                tile_spec,
                whole((t, qh * hd)),
                whole((t, qh * hd)),
                whole((qh, t, 1)),
                whole((t, 1)),
                whole((t, 1)),
                whole((1, stretch)),
            ],
            out_specs=[whole((t, qh * hd)), tile_spec],
            scratch_shapes=[pltpu.VMEM((t, qh * hd), F32), pltpu.VMEM((qh, t, 1), F32)],
        ),
        out_shape=[
            jax.ShapeDtypeStruct((t, qh * hd), F32),
            jax.ShapeDtypeStruct((kv.shape[0], 2 * kh * hd), F32),
        ],
        cost_estimate=pl.CostEstimate(
            flops=10 * t * kv.shape[0] * hd * qh, bytes_accessed=6 * kv.size, transcendentals=t * kv.shape[0]
        ),
        name="attend_back",
    )(base, see, q, kv, do, o, lse, qpos, qfirst, off)


def unit_rows(values):
    rs = lax.rsqrt(jnp.mean(values * values, axis=-1, keepdims=True) + EPS)
    return values * rs, rs


def norm_back(m, unit, rs):
    return (m - unit * jnp.mean(m * unit, axis=-1, keepdims=True)) * rs


def after(value, *others):
    return lax.optimization_barrier((value,) + others)[0]


def shards(
    n,
    layer_input,
    w_query,
    w_key,
    w_value,
    w_output,
    w_gate,
    w_up,
    w_down,
    norm_attn,
    norm_mlp,
    norm_query,
    norm_key,
    out_grad,
    doc_lengths,
    stretch_order,
):
    t, d = layer_input.shape
    hd = norm_query.shape[0]
    qh, kh = w_query.shape[1] // hd, w_key.shape[1] // hd
    stretch = t // 2
    quarter = t // 4
    width = d // n
    ny = n // NZ
    scale = hd ** (-0.5)
    blk, tp = lax.axis_index("blk"), lax.axis_index("tp")
    z, y = blk // ny, blk % ny

    order = ring_order(n)
    place = jnp.array([order.index(b) for b in range(n)], jnp.int32)
    me = lax.dynamic_index_in_dim(place, blk, keepdims=False)
    cols = jnp.take(jnp.array(order + order, jnp.int32), me + jnp.arange(n, dtype=jnp.int32))
    rows = jnp.arange(4, dtype=jnp.int32) ^ tp.astype(jnp.int32)
    planes = (z + jnp.arange(NZ, dtype=jnp.int32)) % NZ
    before = (z - jnp.arange(NZ, dtype=jnp.int32)) % NZ
    lines = (y + jnp.arange(ny, dtype=jnp.int32)) % ny
    block_at = (before[None, :] * ny + lines[:, None]).reshape(-1).astype(jnp.int32)

    gain_attn = norm_attn.astype(F32)[:, None]
    gain_mlp = norm_mlp.astype(F32)[:, None]
    own_qkv = (jnp.concatenate([w_query, w_key, w_value], axis=1).astype(F32) * gain_attn).astype(BF16)
    blocks_qkv = ring_gather(own_qkv, n)
    full_qkv = jnp.concatenate(blocks_qkv, axis=0)

    starts = jnp.cumsum(doc_lengths) - doc_lengths
    table = jnp.arange(stretch_order.shape[0], dtype=jnp.int32)

    def stretch_of(ids):
        return jnp.sum(jnp.where(ids[:, None] == table[None, :], stretch_order[None, :], 0), axis=1)

    def first_of(pos):
        return jnp.max(jnp.where(starts[None, :] <= pos[:, None], starts[None, :], 0), axis=1)

    inside = jnp.arange(stretch, dtype=jnp.int32)
    halves = jnp.arange(2, dtype=jnp.int32)
    base = stretch_of((cols[:, None] * 2 + halves[None, :]).reshape(-1)) * stretch
    positions = (base[:2, None] + inside[None, :]).reshape(-1)
    firsts = first_of(positions)
    base_first = first_of(base[:2])
    see = ((base[None, :] <= base[:2, None]) & (base[None, :] + (stretch - 1) >= base_first[:, None])).astype(jnp.int32)
    inverse = ROPE_BASE ** (-2.0 * jnp.arange(hd // 2, dtype=F32) / hd)
    angles = (positions - firsts).astype(F32)[:, None] * inverse[None, :]
    cosine, sine = jnp.cos(angles), jnp.sin(angles)
    cosine = jnp.concatenate([cosine, cosine], axis=1)
    sine = jnp.concatenate([-sine, sine], axis=1)
    qpos, qfirst, off = positions[:, None], firsts[:, None], inside[None, :]
    gain_query, gain_key = norm_query.astype(F32)[None, :], norm_key.astype(F32)[None, :]
    gains = jnp.stack([gain_query, gain_key])

    unit_attn = arrange(layer_input, cols, n)
    packed = pack(planes, w_gate, w_up, w_down, gain_mlp)
    raw_q, raw_k, q, kv_own = qkv_call(after(unit_attn, packed[0]), full_qkv, cosine, sine, gains, qh, kh, hd)
    blocks_out = ring_gather(after(w_output.T, blocks_qkv[n // 2 - 1], blocks_qkv[n // 2 + 1]), n)
    full_out = place_rows(cols, blocks_out)
    kv = jnp.concatenate(ring_gather(kv_own, n), axis=0)
    x_own = lax.dynamic_slice_in_dim(layer_input, tp * quarter, quarter, 0).astype(F32)
    attn_low, lse = attend(base, see, q, kv, qpos, qfirst, off, qh, kh, hd, scale)

    hidden, grad_hidden, grad_heads, hidden_low, grads, acts, w_mlp = feed(n, attn_low, full_out, x_own, out_grad, packed)

    def peers_first(value):
        return jnp.take(value.reshape(4, quarter, d), rows, axis=0)

    grads = [lax.dynamic_slice_in_dim(grads, block_at[i] * width, width, 0) for i in range(n)]
    owned = [g.astype(F32) for g in grads[:NZ]]
    for j in range(1, ny):
        for s in range(NZ):
            owned[s] = owned[s] + y_shift(after(grads[j * NZ + s], hidden_low), n, j).astype(F32)
    owned = [g.astype(BF16) for g in owned]
    owned = [owned[0]] + [z_shift(owned[s], n, -s) for s in range(1, NZ)]

    downs = []
    for s in range(NZ):
        act = lax.dynamic_slice_in_dim(acts, planes[s] * t, t, 0)
        quarters = peers_first(jnp.concatenate(down_call(act, w_mlp), axis=0))
        downs.append(tp_reduce([after(quarters[i], owned[0]) for i in range(4)]))
    out_own = hidden + downs[0] + sum(z_shift(downs[s].astype(BF16), n, s).astype(F32) for s in (1, 2, 3))

    def cut(value, r):
        return value[:, r * width : (r + 1) * width]

    hidden_low = columns(hidden_low, cols, n, True)
    dq, dkv_all = attend_back(base, see, q, kv, grad_heads, attn_low, lse, qpos, qfirst, off, qh, kh, hd, scale)
    dkv = ring_scatter(lambda r: dkv_all[r * t : (r + 1) * t], n, t)
    owned = [after(g, dq) for g in owned]
    grad_gate, grad_up, grad_down, d_norm_mlp = finish(planes, owned, w_gate, w_up, gain_mlp)
    d_q, dgain_q = head_back(dq, raw_q, cosine, sine, gain_query, qh, hd, "query_back")
    layer_output = restore(tp_pieces(after(out_own.astype(BF16), dq)), cols, rows, 1, BF16)
    d_kv, dgain_k = head_back(dkv, raw_k, cosine, sine, gain_key, kh, hd, "key_back")
    sum_out = ring_scatter(lambda r: dot(cut(after(hidden_low, dq), r), attn_low, TN), n, width)
    sum_q = ring_scatter(lambda r: dot(cut(unit_attn, r), d_q, TN), n, width)

    extra = 16
    gain_part = jnp.concatenate([dgain_q[:1], dgain_k[:1]]).reshape(2, n, hd // n)
    gain_cols = jnp.take(gain_part, cols, axis=1)

    def kv_part(r):
        tail = jnp.pad(gain_cols[:, r, :].reshape(1, -1), ((0, extra - 1), (0, d_kv.shape[1] - 2 * (hd // n))))
        return jnp.concatenate([dot(cut(unit_attn, r), d_kv, TN), tail], axis=0)

    sum_kv = ring_scatter(kv_part, n, width + extra)
    q_cols = qh * hd
    m_attn = (dot(d_q, full_qkv[:, :q_cols], NT) + dot(d_kv, full_qkv[:, q_cols:], NT)).astype(BF16)
    m_attn = tp_scatter(peers_first(m_attn).reshape(t, d))
    m_attn = columns(m_attn, cols, n, False)
    unit_own, rs_own = unit_rows(x_own)
    input_own = grad_hidden + norm_back(m_attn, unit_own, rs_own)
    input_grad = restore(tp_pieces(input_own.astype(BF16)), cols, rows, 1, F32)

    head_gains = sum_kv[width, : 2 * (hd // n)]
    sum_kv = sum_kv[:width]
    d_norm_attn = jnp.sum(w_query.astype(F32) * sum_q, axis=1)
    d_norm_attn += jnp.sum(w_key.astype(F32) * sum_kv[:, : kh * hd], axis=1)
    d_norm_attn += jnp.sum(w_value.astype(F32) * sum_kv[:, kh * hd :], axis=1)
    small = jnp.concatenate([d_norm_attn, d_norm_mlp[:, 0], head_gains])
    small = jnp.pad(small, (0, -small.shape[0] % 1024)).reshape(-1, 128)
    small = tp_sum(small).reshape(-1)
    gain_at = 2 * width
    return (
        layer_output,
        input_grad,
        sum_q * gain_attn,
        sum_kv[:, : kh * hd] * gain_attn,
        sum_kv[:, kh * hd :] * gain_attn,
        sum_out.T,
        grad_gate,
        grad_up,
        grad_down,
        small[:width],
        small[width:gain_at],
        small[gain_at : gain_at + hd // n],
        small[gain_at + hd // n : gain_at + 2 * (hd // n)],
    )


def solution(mesh):
    return jax.shard_map(
        partial(shards, mesh.shape["blk"]),
        mesh=mesh,
        in_specs=(
            P("blk", None),
            P("blk", "tp"),
            P("blk", "tp"),
            P("blk", "tp"),
            P("tp", "blk"),
            P("blk", "tp"),
            P("blk", "tp"),
            P("tp", "blk"),
            P("blk"),
            P("blk"),
            P(),
            P(),
            P("blk", None),
            P(),
            P(),
        ),
        out_specs=(
            P("blk", None),
            P("blk", None),
            P("blk", "tp"),
            P("blk", "tp"),
            P("blk", "tp"),
            P("tp", "blk"),
            P("blk", "tp"),
            P("blk", "tp"),
            P("tp", "blk"),
            P("blk"),
            P("blk"),
            P("blk"),
            P("blk"),
        ),
        check_vma=False,
    )
```

```python
from functools import partial

import jax
import jax.numpy as jnp
from jax import lax
from jax.experimental import pallas as pl
from jax.experimental.pallas import tpu as pltpu
from jax.sharding import PartitionSpec as P

EPS = 1e-06
ROPE_BASE = 1000000.0
F32 = jnp.float32
BF16 = jnp.bfloat16


def dot(a, b, dims, out=F32):
    return lax.dot_general(a, b, (dims, ((), ())), preferred_element_type=out)


NN = ((1,), (0,))
NT = ((1,), (1,))
TN = ((0,), (0,))


def ring_order(n):
    return list(range(0, n, 2)) + list(range(n - 1, 0, -2))


def ring_perms(n):
    order = ring_order(n)
    right = [(order[i], order[(i + 1) % n]) for i in range(n)]
    return right, [(b, a) for a, b in right]


def ring_gather(own, n):
    right, left = ring_perms(n)
    half = n // 2
    rows = own.shape[0] // 2
    blocks = [None] * n
    blocks[0] = own
    from_left = from_right = own
    for k in range(1, half):
        from_left = lax.ppermute(from_left, "blk", right)
        from_right = lax.ppermute(from_right, "blk", left)
        blocks[n - k] = from_left
        blocks[k] = from_right
    top = lax.ppermute(from_left[:rows], "blk", right)
    low = lax.ppermute(from_right[rows:], "blk", left)
    blocks[half] = jnp.concatenate([top, low], axis=0)
    return blocks


def ring_scatter(part, n, rows):
    right, left = ring_perms(n)
    half = n // 2
    cut = rows // 2
    far = part(half).astype(BF16)
    to_right = lax.ppermute(far[:cut], "blk", right).astype(F32)
    to_left = lax.ppermute(far[cut:], "blk", left).astype(F32)
    if half == 1:
        return part(0) + jnp.concatenate([to_right, to_left], axis=0)
    for k in range(half - 1, 0, -1):
        send_right, send_left = part(k), part(n - k)
        if k == half - 1:
            send_right = jnp.concatenate([send_right[:cut] + to_right, send_right[cut:]], axis=0)
            send_left = jnp.concatenate([send_left[:cut], send_left[cut:] + to_left], axis=0)
        else:
            send_right = send_right + to_right
            send_left = send_left + to_left
        to_right = lax.ppermute(send_right.astype(BF16), "blk", right).astype(F32)
        to_left = lax.ppermute(send_left.astype(BF16), "blk", left).astype(F32)
    return part(0) + to_right + to_left


NZ = 4


def z_shift(value, n, s):
    ny = n // NZ
    pairs = [(z * ny + y, (z + s) % NZ * ny + y) for z in range(NZ) for y in range(ny)]
    return lax.ppermute(value, "blk", pairs)


def pack_kernel(zs_ref, gate_ref, up_ref, down_ref, gain_ref, *out_refs):
    part = gate_ref.shape[1] // NZ
    gain = gain_ref[...]
    for s in range(NZ):
        at = pl.ds(pl.multiple_of(zs_ref[s] * part, part), part)
        out_refs[s][:, :part] = (gate_ref[:, at].astype(F32) * gain).astype(BF16)
        out_refs[s][:, part : 2 * part] = (up_ref[:, at].astype(F32) * gain).astype(BF16)
        out_refs[s][:, 2 * part :] = down_ref[at, :].astype(F32).T.astype(BF16)


VMEM = pl.BlockSpec(memory_space=pltpu.VMEM)
SMEM = pl.BlockSpec(memory_space=pltpu.SMEM)


def pack(zs, w_gate, w_up, w_down, gain):
    rows, cols = w_gate.shape
    shape = jax.ShapeDtypeStruct((rows, 3 * cols // NZ), BF16)
    return pl.pallas_call(
        pack_kernel,
        in_specs=[SMEM, VMEM, VMEM, VMEM, VMEM],
        out_specs=[VMEM] * NZ,
        out_shape=[shape] * NZ,
        name="pack",
    )(zs, w_gate, w_up, w_down, gain)


def finish_kernel(zs_ref, *refs):
    pieces = refs[:NZ]
    gain_ref, d_gate, d_up, d_down = refs[NZ:]
    part = d_gate.shape[1] // NZ
    gain = gain_ref[...]
    for s in range(NZ):
        at = pl.ds(pl.multiple_of(zs_ref[s] * part, part), part)
        d_gate[:, at] = pieces[s][:, :part].astype(F32) * gain
        d_up[:, at] = pieces[s][:, part : 2 * part].astype(F32) * gain
        d_down[at, :] = pieces[s][:, 2 * part :].astype(F32).T


def finish(zs, pieces, gain):
    rows, cols = pieces[0].shape[0], NZ * pieces[0].shape[1] // 3
    return pl.pallas_call(
        finish_kernel,
        in_specs=[SMEM] + [VMEM] * (NZ + 1),
        out_specs=[VMEM] * 3,
        out_shape=[
            jax.ShapeDtypeStruct((rows, cols), F32),
            jax.ShapeDtypeStruct((rows, cols), F32),
            jax.ShapeDtypeStruct((cols, rows), F32),
        ],
        name="finish",
    )(zs, *pieces, gain)


MESH = pl.DeviceIdType.MESH


class Wires:
    def __init__(self, send, recv):
        self.send, self.recv, self.sent, self.done = send, recv, [], []

    def go(self, src, dst, device):
        i = len(self.sent)
        copy = pltpu.make_async_remote_copy(
            src_ref=src,
            dst_ref=dst,
            send_sem=self.send.at[i],
            recv_sem=self.recv.at[i],
            device_id=device,
            device_id_type=MESH,
        )
        copy.start()
        self.sent.append(copy)
        return copy

    def drain(self, copies):
        for copy in copies:
            copy.wait_send()
            self.done.append(copy)

    def close(self):
        self.drain([copy for copy in self.sent if not any(copy is other for other in self.done)])


def greet(devices):
    barrier = pltpu.get_barrier_semaphore()
    for device in devices:
        pl.semaphore_signal(barrier, inc=1, device_id=device, device_id_type=MESH)
    pl.semaphore_wait(barrier, len(devices))


class Spot:
    def __init__(self, n):
        self.n, self.ny = n, n // NZ
        self.blk, self.tp = lax.axis_index("blk"), lax.axis_index("tp")
        self.z, self.y = self.blk // self.ny, self.blk % self.ny
        self.x, self.core = self.tp // 2, self.tp % 2
        self.tp_core = self.x * 2 + (1 - self.core)
        self.tp_far = (1 - self.x) * 2 + self.core
        self.core_dev = {"tp": self.tp_core}
        self.far_dev = {"tp": self.tp_far}
        self.place = jnp.where(self.blk % 2 == 0, self.blk // 2, n - 1 - self.blk // 2)
        self.right_dev = {"blk": self.at_place(1)}
        self.left_dev = {"blk": self.at_place(n - 1)}

    def at_place(self, r):
        p = (self.place + r) % self.n
        return jnp.where(p < self.n // 2, 2 * p, 2 * (self.n - 1 - p) + 1)

    def plane(self, s):
        return (self.z + s) % NZ

    def z_dev(self, s):
        return {"blk": self.plane(s) * self.ny + self.y}

    def y_dev(self, j):
        return {"blk": self.z * self.ny + (self.y + j) % self.ny}

    def peers(self):
        return (
            [self.core_dev, self.far_dev]
            + [self.z_dev(s) for s in range(1, NZ)]
            + [self.y_dev(j) for j in range(1, self.ny)]
        )


def rows_at(index, count):
    return pl.ds(pl.multiple_of(index * count, count), count)


def feed_copies(n):
    ny = n // NZ
    return 3 + 8 * (ny - 1) + 2 * 3 + 8 * 3 + 3 + 4 * 3 + 3 + 3


def feed_kernel(n, attn, wo, x_own, g_rows, *refs):
    packed = refs[:NZ]
    hidden_o, gh_o, heads_o, hl_o, dw_o, y_o, act_o, w_o = refs[NZ : NZ + 8]
    (u_all, g_all, dgu, o_part, o_far, o_core, o_x, part, far, near, core_in, x_in, z_in, m_acc, dw_tile, send, recv, dw_sem) = refs[NZ + 8 :]
    q, d = x_own.shape
    unit_w = 3 * (packed[0].shape[1] // 3)
    p = unit_w // 3
    bw = packed[0].shape[0]
    me = Spot(n)
    wires = Wires(send, recv)
    greet(me.peers())

    def quarter(plane, peer):
        return rows_at(plane * 4 + peer, q)

    mine = rows_at(me.blk, bw)
    w_z = {s: wires.go(packed[s], w_o.at[mine], me.z_dev(s)) for s in (1, 3, 2)}
    w_y = [wires.go(packed[0], w_o.at[mine], me.y_dev(j)) for j in range(1, me.ny)]
    w_o[mine, :] = packed[0][...]

    g_all[rows_at(me.z, 4 * q), :] = g_rows[...]

    def project(peer):
        return dot(attn[rows_at(peer, q), :], wo[...], NT)

    for i, x in enumerate((1 - me.x, me.x)):
        o_part[i] = project(x * 2 + 1 - me.core).astype(BF16)
    far_in = wires.go(o_part.at[0], o_core.at[0], me.core_dev)
    near_in = wires.go(o_part.at[1], o_core.at[1], me.core_dev)
    own_far = project(me.tp_far)
    far_in.wait_recv()
    o_far[...] = (own_far + o_core[0].astype(F32)).astype(BF16)
    x_sum = wires.go(o_far, o_x, me.far_dev)
    own_sum = project(me.tp) + x_own[...]
    near_in.wait_recv()
    own_sum = own_sum + o_core[1].astype(F32)
    x_sum.wait_recv()
    hidden = own_sum + o_x[...].astype(F32)
    hidden_o[...] = hidden
    rs = lax.rsqrt(jnp.mean(hidden * hidden, axis=-1, keepdims=True) + EPS)
    own_q = quarter(me.z, me.tp)
    u_all[own_q, :] = (hidden * rs).astype(BF16)

    def pass_on(buf, plane):
        at = quarter(plane, me.tp)
        return wires.go(buf.at[at], buf.at[at], me.far_dev), wires.go(buf.at[at], buf.at[at], me.core_dev)

    def pass_far(buf, plane, copies):
        copies[0].wait_recv()
        at = quarter(plane, me.tp_far)
        return wires.go(buf.at[at], buf.at[at], me.core_dev)

    own_pass = pass_on(u_all, me.z)
    u_z, g_z = {}, {}
    for s in (1, 3, 2):
        u_z[s] = wires.go(u_all.at[own_q], u_all.at[own_q], me.z_dev(s))
    for s in (1, 3, 2):
        w_z[s].wait_recv()
        at = rows_at(me.plane(-s) * me.ny + me.y, bw)
        w_y += [wires.go(w_o.at[at], w_o.at[at], me.y_dev(j)) for j in range(1, me.ny)]
    for s in (1, 3, 2):
        g_z[s] = wires.go(g_all.at[own_q], g_all.at[own_q], me.z_dev(s))
    own_far_pass = pass_far(u_all, me.z, own_pass)
    for copy in w_y:
        copy.wait_recv()
    own_pass[1].wait_recv()
    own_far_pass.wait_recv()

    def compute(i, plane):
        @pl.loop(0, 2)
        def _(k):
            at = pl.ds(pl.multiple_of(plane * (4 * q) + k * (2 * q), 2 * q), 2 * q)
            gate_up = dot(u_all[at, :], w_o[:, : 2 * p], NN)
            grad_act = dot(g_all[at, :], w_o[:, 2 * p :], NN)
            gate, up = gate_up[:, :p], gate_up[:, p:]
            sig = 1.0 / (1.0 + jnp.exp(-gate))
            silu = gate * sig
            act_o[at, :] = (silu * up).astype(BF16)
            dgu[at, p:] = (grad_act * silu).astype(BF16)
            dgu[at, :p] = (grad_act * up * (sig * (1.0 + gate * (1.0 - sig)))).astype(BF16)

        rows = rows_at(plane, 4 * q)
        tile = 512

        @pl.loop(0, d // tile)
        def _(c):
            at = pl.ds(pl.multiple_of(c * tile, tile), tile)
            part[i % 2, :, at] = dot(dgu[rows, :], w_o[at, : 2 * p], NT).astype(BF16)

    def reduce_core(i):
        out = []
        for k, x in enumerate((1 - me.x, me.x)):
            src = part.at[i % 2, rows_at(x * 2 + 1 - me.core, q)]
            out.append(wires.go(src, core_in.at[i, k], me.core_dev))
        return out

    def reduce_far(i, copies):
        copies[0].wait_recv()
        far[i] = (part[i % 2, rows_at(me.tp_far, q), :].astype(F32) + core_in[i, 0].astype(F32)).astype(BF16)
        return wires.go(far.at[i], x_in.at[i], me.far_dev)

    def reduce_near(i, copies, x_copy):
        copies[1].wait_recv()
        x_copy.wait_recv()
        return part[i % 2, rows_at(me.tp, q), :].astype(F32) + core_in[i, 1].astype(F32) + x_in[i].astype(F32)

    order = (1, 3, 2)

    def finish_slot(i):
        value = reduce_near(i, cores[i], fars[i])
        wires.drain(cores[i])
        if i == 0:
            m_acc[...] = value
            return None
        near[i - 1] = value.astype(BF16)
        return wires.go(near.at[i - 1], z_in.at[i - 1], me.z_dev(-order[i - 1]))

    def dw_copy(c, slot):
        rows = pl.ds(pl.multiple_of(c * 256, 256), 256)
        return pltpu.make_async_copy(dw_tile.at[slot], dw_o.at[rows], dw_sem.at[slot])

    def grads(first, last):
        @pl.loop(first, last)
        def _(c):
            slot = c % 2

            @pl.when(c >= first + 2)
            def _():
                dw_copy(c - 2, slot).wait()

            at = pl.ds(pl.multiple_of(c * 256, 256), 256)
            dw_tile[slot, :, : 2 * p] = dot(u_all[:, at], dgu[...], TN).astype(BF16)
            dw_tile[slot, :, 2 * p :] = dot(g_all[:, at], act_o[...], TN).astype(BF16)
            dw_copy(c, slot).start()

        for c in (last - 2, last - 1):
            dw_copy(c, c % 2).wait()
        planes = NZ * first * 256 // d, NZ * last * 256 // d
        return [
            wires.go(dw_o.at[rows_at(plane * me.ny + (me.y + j) % me.ny, bw)], y_o.at[(j - 1) * NZ + plane], me.y_dev(j))
            for plane in range(*planes)
            for j in range(1, me.ny)
        ]

    compute(0, me.z)
    cores, fars, backs = [reduce_core(0)], [], []
    passes = []
    for s in order:
        plane = me.plane(-s)
        u_z[s].wait_recv()
        u_copies = pass_on(u_all, plane)
        g_z[s].wait_recv()
        passes.append((u_copies, pass_on(g_all, plane)))
    for i, s in enumerate(order):
        plane = me.plane(-s)
        u_copies, g_copies = passes[i]
        u_last = pass_far(u_all, plane, u_copies)
        g_last = pass_far(g_all, plane, g_copies)
        fars.append(reduce_far(i, cores[i]))
        if i >= 1:
            backs.append(finish_slot(i - 1))
        u_copies[1].wait_recv()
        g_copies[1].wait_recv()
        u_last.wait_recv()
        g_last.wait_recv()
        compute(i + 1, plane)
        cores.append(reduce_core(i + 1))
    tiles = d // 256
    fars.append(reduce_far(NZ - 1, cores[NZ - 1]))
    backs.append(finish_slot(NZ - 2))
    y_copies = grads(0, tiles // 2)
    backs.append(finish_slot(NZ - 1))
    y_copies += grads(tiles // 2, tiles)
    m = m_acc[...]
    for i in range(1, NZ):
        backs[i].wait_recv()
        m = m + z_in[i - 1].astype(F32)

    hidden = hidden_o[...]
    rs = lax.rsqrt(jnp.mean(hidden * hidden, axis=-1, keepdims=True) + EPS)
    unit = hidden * rs
    grad = g_rows[rows_at(me.tp, q), :].astype(F32) + (m - unit * jnp.mean(m * unit, axis=-1, keepdims=True)) * rs
    gh_o[...] = grad
    own = rows_at(me.tp, q)
    hl_o[own, :] = grad.astype(BF16)
    x_copy = wires.go(hl_o.at[own], hl_o.at[own], me.far_dev)
    c_copy = wires.go(hl_o.at[own], hl_o.at[own], me.core_dev)

    def heads(peer):
        heads_o[rows_at(peer, q), :] = dot(hl_o[rows_at(peer, q), :], wo[...], NN).astype(BF16)

    heads(me.tp)
    c_copy.wait_recv()
    heads(me.tp_core)
    x_copy.wait_recv()
    at = rows_at(me.tp_far, q)
    last = wires.go(hl_o.at[at], hl_o.at[at], me.core_dev)
    heads(me.tp_far)
    last.wait_recv()
    heads((1 - me.x) * 2 + 1 - me.core)
    for copy in y_copies:
        copy.wait_recv()
    wires.close()


def feed(n, attn, wo, x_own, g_rows, packed):
    q, d = x_own.shape
    t, a = attn.shape
    bw, w3 = packed[0].shape
    p = w3 // 3
    tokens = NZ * t
    copies = feed_copies(n)
    vm = pltpu.VMEM
    return pl.pallas_call(
        partial(feed_kernel, n),
        in_specs=[VMEM] * (4 + NZ),
        out_specs=[VMEM] * 4 + [pl.BlockSpec(memory_space=pl.ANY)] * 2 + [VMEM] * 2,
        out_shape=[
            jax.ShapeDtypeStruct((q, d), F32),
            jax.ShapeDtypeStruct((q, d), F32),
            jax.ShapeDtypeStruct((t, a), BF16),
            jax.ShapeDtypeStruct((t, d), BF16),
            jax.ShapeDtypeStruct((d, w3), BF16),
            jax.ShapeDtypeStruct((NZ * (n // NZ - 1), bw, w3), BF16),
            jax.ShapeDtypeStruct((tokens, p), BF16),
            jax.ShapeDtypeStruct((d, w3), BF16),
        ],
        scratch_shapes=[
            vm((tokens, d), BF16),
            vm((tokens, d), BF16),
            vm((tokens, 2 * p), BF16),
            vm((2, q, d), BF16),
            vm((q, d), BF16),
            vm((2, q, d), BF16),
            vm((q, d), BF16),
            vm((2, t, d), BF16),
            vm((NZ, q, d), BF16),
            vm((NZ - 1, q, d), BF16),
            vm((NZ, 2, q, d), BF16),
            vm((NZ, q, d), BF16),
            vm((NZ - 1, q, d), BF16),
            vm((q, d), F32),
            vm((2, 256, w3), BF16),
            pltpu.SemaphoreType.DMA((copies,)),
            pltpu.SemaphoreType.DMA((copies,)),
            pltpu.SemaphoreType.DMA((2,)),
        ],
        compiler_params=pltpu.CompilerParams(
            collective_id=1, has_side_effects=True, vmem_limit_bytes=67000000
        ),
        name="feed",
    )(attn, wo, x_own, g_rows, *packed)


class RingSum:
    def __init__(self, wires, me, land, stage, part):
        self.wires, self.me, self.land, self.stage, self.part = wires, me, land, stage, part
        self.half = me.n // 2
        self.cut = land.shape[2] // 2
        self.got = None

    def start(self):
        top, low, cut = pl.ds(0, self.cut), pl.ds(self.cut, self.cut), self.half - 1
        self.stage[...] = self.part(self.half).astype(BF16)
        self.got = (
            self.wires.go(self.stage.at[top], self.land.at[0, cut, top], self.me.right_dev),
            self.wires.go(self.stage.at[low], self.land.at[1, cut, low], self.me.left_dev),
        )
        self.first = self.got

    def step(self, k):
        cut = self.cut
        for side, place in ((0, k), (1, self.me.n - k)):
            self.got[side].wait_recv()
            mine = self.part(place)
            if k == self.half - 1:
                keep, fresh = (slice(0, cut), slice(cut, None)) if side == 0 else (slice(cut, None), slice(0, cut))
                self.land[side, k, keep, :] = (self.land[side, k, keep, :].astype(F32) + mine[keep]).astype(BF16)
                self.land[side, k, fresh, :] = mine[fresh].astype(BF16)
            else:
                self.land[side, k] = (self.land[side, k].astype(F32) + mine).astype(BF16)
        self.got = tuple(
            self.wires.go(self.land.at[side, k], self.land.at[side, k - 1], dev)
            for side, dev in ((0, self.me.right_dev), (1, self.me.left_dev))
        )

    def total(self):
        for copy in self.got:
            copy.wait_recv()
        return self.part(0) + self.land[0, 0].astype(F32) + self.land[1, 0].astype(F32)


def tail_copies(n):
    return 2 * 3 * (n // 2) + 16 + 3 + 3 + 3 + 3 + 3 + 2 + 8


def tail_kernel(n, ringed, *refs):
    (dq, dkv, raw_q, raw_k, cos_ref, sin_ref, gain_ref, u1, wqkv, hl, attn, gh, x_own, hidden, act, w_down) = refs[:16]
    w_q, w_k, w_v, gain_attn, norm_in = refs[16:21]
    lo, ig, gq_o, gk_o, gv_o, go_o, small_o = refs[21:28]
    (d_qkv, gains, kv_land, kv_stage, o_land, o_stage, w_land, w_stage, m_part, m_core, m_x, part, core_in, x_in, z_in) = refs[28:43]
    ig_low, norm_land, small_core, small_x, o_whole, w_whole, send, recv = refs[43:]
    q, d = hidden.shape
    t, qw = dq.shape
    hd = cos_ref.shape[1]
    kw = raw_k.shape[1]
    bw = w_q.shape[0]
    me = Spot(n)
    wires = Wires(send, recv)
    greet(me.peers() + [me.right_dev, me.left_dev])

    norm_copies = [
        wires.go(norm_in.at[me.plane(s)], norm_land.at[s - 1], me.z_dev(s)) for s in range(1, NZ)
    ]

    def head_back(src, raw, heads, kind, to):
        gains[kind] = jnp.zeros((1, hd), F32)

        @pl.loop(0, 4)
        def _(k):
            at = pl.ds(pl.multiple_of(k * q, q), q)
            cosine, sine = cos_ref[at, :], sin_ref[at, :]
            for h in range(heads):
                cols = slice(h * hd, (h + 1) * hd)
                grad = src[at, cols].astype(F32)
                grad = grad * cosine - turned(grad, sine)
                v = raw[at, cols]
                rs = lax.rsqrt(jnp.mean(v * v, axis=-1, keepdims=True) + EPS)
                unit = v * rs
                gains[kind] += jnp.sum(grad * unit, axis=0, keepdims=True)
                m = grad * gain_ref[kind]
                back = (m - unit * jnp.mean(m * unit, axis=-1, keepdims=True)) * rs
                d_qkv[at, to + h * hd : to + (h + 1) * hd] = back.astype(BF16)

    slots = (1, 3, 2, 0)
    cores, fars, backs = {}, {}, {}

    def down(i):
        rows = rows_at(me.plane(-slots[i]), 4 * q)
        tile = 512

        @pl.loop(0, d // tile)
        def _(c):
            at = pl.ds(pl.multiple_of(c * tile, tile), tile)
            part[i % 2, :, at] = dot(act[rows, :], w_down[at, :], NT).astype(BF16)

        cores[i] = [
            wires.go(part.at[i % 2, rows_at(x * 2 + 1 - me.core, q)], core_in.at[i, k], me.core_dev)
            for k, x in enumerate((1 - me.x, me.x))
        ]

    def down_far(i):
        cores[i][0].wait_recv()
        core_in[i, 0] = (part[i % 2, rows_at(me.tp_far, q), :].astype(F32) + core_in[i, 0].astype(F32)).astype(BF16)
        fars[i] = wires.go(core_in.at[i, 0], x_in.at[i], me.far_dev)

    def down_near(i):
        cores[i][1].wait_recv()
        fars[i].wait_recv()
        value = part[i % 2, rows_at(me.tp, q), :].astype(F32) + core_in[i, 1].astype(F32) + x_in[i].astype(F32)
        wires.drain(cores[i])
        if slots[i] == 0:
            return value
        x_in[i] = value.astype(BF16)
        backs[i] = wires.go(x_in.at[i], z_in.at[i], me.z_dev(-slots[i]))

    def term(left, right, whole):
        if bw % 128 == 0:
            return lambda r: dot(left[:, rows_at(me.at_place(r), bw)], right[...], TN)

        @pl.loop(0, d // 256)
        def _(c):
            at = rows_at(c, 256)
            whole[at, :] = dot(left[:, at], right[...], TN).astype(BF16)

        return lambda r: whole[rows_at(me.at_place(r), bw), :].astype(F32)

    o_part = term(hl, attn, o_whole)

    o_ring = RingSum(wires, me, o_land, o_stage, o_part)

    half = n // 2
    if ringed:
        kv_ring = RingSum(wires, me, kv_land, kv_stage, lambda r: dkv[rows_at(me.at_place(r), t), :].astype(F32))
        kv_ring.start()
    head_back(dq, raw_q, qw // hd, 0, 0)
    fill = [
        lambda: (o_ring.start(), down(0)),
        lambda: (down_far(0), down(1)),
        lambda: (down_near(0), down_far(1), down(2)),
        lambda: (down_near(1), down_far(2), down(3)),
    ]
    for k in range(half - 1, 0, -1):
        if ringed:
            kv_ring.step(k)
        if fill:
            fill.pop(0)()
        if k < half - 1:
            o_ring.step(k + 1)
    for job in fill:
        job()
    if half > 1:
        o_ring.step(1)
    if ringed:
        kv_total = kv_ring.total().astype(BF16)
        wires.drain(kv_ring.first)
        kv_stage[...] = kv_total
        kv_sum = kv_stage
    else:
        kv_sum = dkv
    head_back(kv_sum, raw_k, kw // hd, 1, qw)
    d_qkv[:, qw + kw :] = kv_sum[:, kw:].astype(BF16)

    def m_term(peer):
        return dot(d_qkv[rows_at(peer, q), :], wqkv[...], NT)

    w_term = term(u1, d_qkv, w_whole)

    def qkv_part(r):
        body = w_term(r)
        extra = w_land.shape[2] - bw
        rest = jnp.concatenate([gains[0], gains[1], jnp.zeros((extra - 2, hd), F32)], axis=0)
        rest = jnp.concatenate([rest, jnp.zeros((extra, body.shape[1] - hd), F32)], axis=1)
        return jnp.concatenate([body, rest], axis=0)

    w_ring = RingSum(wires, me, w_land, w_stage, qkv_part)
    for i, x in enumerate((1 - me.x, me.x)):
        m_part[i] = m_term(x * 2 + 1 - me.core).astype(BF16)
    m_far = wires.go(m_part.at[0], m_core.at[0], me.core_dev)
    m_near = wires.go(m_part.at[1], m_core.at[1], me.core_dev)
    w_ring.start()
    own_far = m_term(me.tp_far)
    m_far.wait_recv()
    m_core[0] = (own_far + m_core[0].astype(F32)).astype(BF16)
    m_sum = wires.go(m_core.at[0], m_x, me.far_dev)
    own = m_term(me.tp)
    m_near.wait_recv()
    own = own + m_core[1].astype(F32)
    steps = list(range(half - 1, 0, -1))
    if steps:
        w_ring.step(steps.pop(0))
    m_sum.wait_recv()
    m = own + m_x[...].astype(F32)
    x = x_own[...].astype(F32)
    rs = lax.rsqrt(jnp.mean(x * x, axis=-1, keepdims=True) + EPS)
    unit = x * rs
    grad = gh[...] + (m - unit * jnp.mean(m * unit, axis=-1, keepdims=True)) * rs
    mine = rows_at(me.tp, q)
    ig_low[mine, :] = grad.astype(BF16)

    def spread(buf):
        far = wires.go(buf.at[mine], buf.at[mine], me.far_dev)
        core = wires.go(buf.at[mine], buf.at[mine], me.core_dev)
        return far, core

    def spread_far(buf, copies):
        copies[0].wait_recv()
        at = rows_at(me.tp_far, q)
        return wires.go(buf.at[at], buf.at[at], me.core_dev)

    ig_copies = spread(ig_low)
    if steps:
        w_ring.step(steps.pop(0))

    down_near(2)
    down_far(3)
    out = hidden[...] + down_near(3)
    for i in range(NZ - 1):
        backs[i].wait_recv()
        out = out + z_in[i].astype(F32)
    lo[mine, :] = out.astype(BF16)
    lo_copies = spread(lo)
    ig_last = spread_far(ig_low, ig_copies)
    while steps:
        w_ring.step(steps.pop(0))
    go_o[...] = o_ring.total().T

    lo_last = spread_far(lo, lo_copies)
    ig_copies[1].wait_recv()
    ig_last.wait_recv()
    ig[...] = ig_low[...].astype(F32)
    total = w_ring.total()
    grad = total[:bw]
    gain = gain_attn[...]
    norm = jnp.sum(grad[:, :qw] * w_q[...].astype(F32), axis=1, keepdims=True)
    norm = norm + jnp.sum(grad[:, qw : qw + kw] * w_k[...].astype(F32), axis=1, keepdims=True)
    norm = norm + jnp.sum(grad[:, qw + kw :] * w_v[...].astype(F32), axis=1, keepdims=True)
    small_o[:bw, :] = jnp.broadcast_to(norm, (bw, hd))
    mlp = norm_in[me.z]
    for s in range(1, NZ):
        norm_copies[s - 1].wait_recv()
        mlp = mlp + norm_land[s - 1]
    small_o[bw : 2 * bw, :] = mlp
    small_o[2 * bw :, :] = total[bw : bw + 16, :hd]
    copy = wires.go(small_o, small_core, me.core_dev)
    gq_o[...] = grad[:, :qw] * gain
    gk_o[...] = grad[:, qw : qw + kw] * gain
    gv_o[...] = grad[:, qw + kw :] * gain
    copy.wait_recv()
    small_core[...] += small_o[...]
    copy = wires.go(small_core, small_x, me.far_dev)
    lo_copies[1].wait_recv()
    lo_last.wait_recv()
    copy.wait_recv()
    wires.close()
    small_o[...] = small_core[...] + small_x[...]


def tail(n, ringed, dq, dkv, raw_q, raw_k, cosine, sine, gains, u1, wqkv, hl, attn, gh, x_own, hidden, act, w_down, w_q, w_k, w_v, gain_attn, norm_in):
    q, d = hidden.shape
    t, qw = dq.shape
    hd = cosine.shape[1]
    kw = raw_k.shape[1]
    wide = qw + 2 * kw
    bw = d // n
    half = n // 2
    copies = tail_copies(n)
    vm = pltpu.VMEM
    small = 2 * bw + 16
    shape = jax.ShapeDtypeStruct
    return pl.pallas_call(
        partial(tail_kernel, n, ringed),
        in_specs=[VMEM] * 21,
        out_specs=[VMEM] * 7,
        out_shape=[
            shape((t, d), BF16),
            shape((t, d), F32),
            shape((bw, qw), F32),
            shape((bw, kw), F32),
            shape((bw, kw), F32),
            shape((attn.shape[1], bw), F32),
            shape((small, hd), F32),
        ],
        scratch_shapes=[
            vm((t, wide), BF16),
            vm((2, 1, hd), F32),
            vm((2, half, t, 2 * kw) if ringed else (2, 1, 16, 128), BF16),
            vm((t, 2 * kw) if ringed else (16, 128), BF16),
            vm((2, half, bw, attn.shape[1]), BF16),
            vm((bw, attn.shape[1]), BF16),
            vm((2, half, bw + 32, wide), BF16),
            vm((bw + 32, wide), BF16),
            vm((2, q, d), BF16),
            vm((2, q, d), BF16),
            vm((q, d), BF16),
            vm((2, t, d), BF16),
            vm((NZ, 2, q, d), BF16),
            vm((NZ, q, d), BF16),
            vm((NZ - 1, q, d), BF16),
            vm((t, d), BF16),
            vm((NZ - 1, bw, hd), F32),
            vm((small, hd), F32),
            vm((small, hd), F32),
            vm((d, attn.shape[1]) if bw % 128 else (16, 128), BF16),
            vm((d, wide) if bw % 128 else (16, 128), BF16),
            pltpu.SemaphoreType.DMA((copies,)),
            pltpu.SemaphoreType.DMA((copies,)),
        ],
        compiler_params=pltpu.CompilerParams(
            collective_id=2, has_side_effects=True, vmem_limit_bytes=67000000
        ),
        name="tail",
    )(dq, dkv, raw_q, raw_k, cosine, sine, gains, u1, wqkv, hl, attn, gh, x_own, hidden, act, w_down, w_q, w_k, w_v, gain_attn, norm_in)


def turned(v, sine):
    return pltpu.roll(v, v.shape[1] // 2, 1) * sine


def qkv_kernel(heads, hd, u_ref, w_ref, cos_ref, sin_ref, gain_ref, raw_q, raw_k, q_ref, kv_ref):
    qh, kh = heads
    y = dot(u_ref[...], w_ref[...], NN)
    raw_q[...] = y[:, : qh * hd]
    raw_k[...] = y[:, qh * hd : (qh + kh) * hd]
    cosine, sine = cos_ref[...], sin_ref[...]
    for h in range(qh + kh):
        v = y[:, h * hd : (h + 1) * hd]
        rs = lax.rsqrt(jnp.mean(v * v, axis=-1, keepdims=True) + EPS)
        v = v * rs * gain_ref[0 if h < qh else 1]
        v = (v * cosine + turned(v, sine)).astype(BF16)
        if h < qh:
            q_ref[:, h * hd : (h + 1) * hd] = v
        else:
            kv_ref[:, (h - qh) * hd : (h - qh + 1) * hd] = v
    kv_ref[:, kh * hd :] = y[:, (qh + kh) * hd :].astype(BF16)


def qkv_call(u, w, cosine, sine, gains, qh, kh, hd):
    t, d = u.shape
    rows = t // 4
    width = w.shape[1]
    return pl.pallas_call(
        partial(qkv_kernel, (qh, kh), hd),
        grid=(4,),
        in_specs=[
            pl.BlockSpec((rows, d), lambda i: (i, 0)),
            pl.BlockSpec((d, width), lambda i: (0, 0)),
            pl.BlockSpec((rows, hd), lambda i: (i, 0)),
            pl.BlockSpec((rows, hd), lambda i: (i, 0)),
            pl.BlockSpec((2, 1, hd), lambda i: (0, 0, 0)),
        ],
        out_specs=[
            pl.BlockSpec((rows, qh * hd), lambda i: (i, 0)),
            pl.BlockSpec((rows, kh * hd), lambda i: (i, 0)),
            pl.BlockSpec((rows, qh * hd), lambda i: (i, 0)),
            pl.BlockSpec((rows, 2 * kh * hd), lambda i: (i, 0)),
        ],
        out_shape=[
            jax.ShapeDtypeStruct((t, qh * hd), F32),
            jax.ShapeDtypeStruct((t, kh * hd), F32),
            jax.ShapeDtypeStruct((t, qh * hd), BF16),
            jax.ShapeDtypeStruct((t, 2 * kh * hd), BF16),
        ],
        cost_estimate=pl.CostEstimate(
            flops=2 * t * d * width, bytes_accessed=2 * d * (t + width), transcendentals=0
        ),
        name="qkv",
    )(u, w, cosine, sine, gains)


def tile_masks(base_ref, tile, qpos_ref, qfirst_ref, off_ref, q0, stretch):
    kpos = off_ref[...] + base_ref[tile]
    qpos = qpos_ref[pl.ds(q0, stretch), :]
    qfirst = qfirst_ref[pl.ds(q0, stretch), :]
    return (kpos <= qpos) & (kpos >= qfirst)


def attend_kernel(dims, scale, base_ref, see_ref, q_ref, kv_ref, qpos_ref, qfirst_ref, off_ref, out_ref, lse_ref, acc_ref, sum_ref):
    qh, kh, hd, stretch = dims
    group = qh // kh
    tile = pl.program_id(0)
    last = pl.num_programs(0) - 1

    @pl.when(tile == 0)
    def _():
        acc_ref[...] = jnp.zeros_like(acc_ref)
        sum_ref[...] = jnp.zeros_like(sum_ref)

    for e in range(2):
        q0 = e * stretch

        @pl.when(see_ref[e, tile] > 0)
        def _():
            mask = tile_masks(base_ref, tile, qpos_ref, qfirst_ref, off_ref, q0, stretch)
            for h in range(qh):
                k = kv_ref[:, (h // group) * hd : (h // group + 1) * hd]
                v = kv_ref[:, (kh + h // group) * hd : (kh + h // group + 1) * hd]
                q = q_ref[q0 : q0 + stretch, h * hd : (h + 1) * hd]
                s = dot(q, k, NT) * scale
                p = jnp.where(mask, jnp.exp(s), 0.0)
                sum_ref[h, q0 : q0 + stretch, :] += jnp.sum(p, axis=-1, keepdims=True)
                acc_ref[q0 : q0 + stretch, h * hd : (h + 1) * hd] += dot(p.astype(BF16), v, NN)

    @pl.when(tile == last)
    def _():
        for h in range(qh):
            total = sum_ref[h]
            out_ref[:, h * hd : (h + 1) * hd] = (acc_ref[:, h * hd : (h + 1) * hd] / total).astype(BF16)
            lse_ref[h] = jnp.log(total)


def attend(base, see, q, kv, qpos, qfirst, off, qh, kh, hd, scale):
    t = q.shape[0]
    stretch = t // 2
    tiles = kv.shape[0] // stretch

    def whole(shape):
        return pl.BlockSpec(shape, lambda i, *_: (0,) * len(shape))

    return pl.pallas_call(
        partial(attend_kernel, (qh, kh, hd, stretch), scale),
        grid_spec=pltpu.PrefetchScalarGridSpec(
            num_scalar_prefetch=2,
            grid=(tiles,),
            in_specs=[
                whole((t, qh * hd)),
                pl.BlockSpec((stretch, 2 * kh * hd), lambda i, *_: (i, 0)),
                whole((t, 1)),
                whole((t, 1)),
                whole((1, stretch)),
            ],
            out_specs=[whole((t, qh * hd)), whole((qh, t, 1))],
            scratch_shapes=[pltpu.VMEM((t, qh * hd), F32), pltpu.VMEM((qh, t, 1), F32)],
        ),
        out_shape=[
            jax.ShapeDtypeStruct((t, qh * hd), BF16),
            jax.ShapeDtypeStruct((qh, t, 1), F32),
        ],
        cost_estimate=pl.CostEstimate(
            flops=4 * t * kv.shape[0] * hd * qh, bytes_accessed=2 * kv.size, transcendentals=t * kv.shape[0]
        ),
        name="attend",
    )(base, see, q, kv, qpos, qfirst, off)


def attend_back_kernel(
    dims, scale, base_ref, see_ref, q_ref, kv_ref, do_ref, o_ref, lse_ref, qpos_ref, qfirst_ref, off_ref, dq_ref, dkv_out, acc_ref, delta_ref, dkv_ref
):
    qh, kh, hd, stretch = dims
    group = qh // kh
    tile = pl.program_id(0)
    last = pl.num_programs(0) - 1

    @pl.when(tile == 0)
    def _():
        acc_ref[...] = jnp.zeros_like(acc_ref)
        for h in range(qh):
            at = slice(h * hd, (h + 1) * hd)
            delta_ref[h] = jnp.sum(do_ref[:, at].astype(F32) * o_ref[:, at].astype(F32), axis=-1, keepdims=True)

    sees = [see_ref[0, tile] > 0, see_ref[1, tile] > 0]

    @pl.when(jnp.logical_not(sees[0]))
    def _():
        dkv_ref[...] = jnp.zeros_like(dkv_ref)

    def half(e, add):
        q0 = e * stretch
        mask = tile_masks(base_ref, tile, qpos_ref, qfirst_ref, off_ref, q0, stretch)
        for c in range(kh):
            k = kv_ref[:, c * hd : (c + 1) * hd]
            v = kv_ref[:, (kh + c) * hd : (kh + c + 1) * hd]
            dk = dv = None
            for h in range(c * group, (c + 1) * group):
                at = slice(h * hd, (h + 1) * hd)
                q = q_ref[q0 : q0 + stretch, at]
                do = do_ref[q0 : q0 + stretch, at]
                s = dot(q, k, NT) * scale
                p = jnp.where(mask, jnp.exp(s - lse_ref[h, q0 : q0 + stretch, :]), 0.0)
                dp = dot(do, v, NT)
                ds = (p * (dp - delta_ref[h, q0 : q0 + stretch, :])).astype(BF16)
                acc_ref[q0 : q0 + stretch, at] += dot(ds, k, NN)
                dk_h = dot(ds, q, TN)
                dv_h = dot(p.astype(BF16), do, TN)
                dk = dk_h if dk is None else dk + dk_h
                dv = dv_h if dv is None else dv + dv_h
            ck = slice(c * hd, (c + 1) * hd)
            cv = slice((kh + c) * hd, (kh + c + 1) * hd)
            if add:
                dkv_ref[:, ck] += dk * scale
                dkv_ref[:, cv] += dv
            else:
                dkv_ref[:, ck] = dk * scale
                dkv_ref[:, cv] = dv

    for e in range(2):

        @pl.when(sees[e])
        def _():
            half(e, e == 1)

    dkv_out[...] = dkv_ref[...].astype(BF16)

    @pl.when(tile == last)
    def _():
        dq_ref[...] = (acc_ref[...] * scale).astype(BF16)


def attend_back(base, see, q, kv, do, o, lse, qpos, qfirst, off, qh, kh, hd, scale):
    t = q.shape[0]
    stretch = t // 2
    tiles = kv.shape[0] // stretch

    def whole(shape):
        return pl.BlockSpec(shape, lambda i, *_: (0,) * len(shape))

    tile_spec = pl.BlockSpec((stretch, 2 * kh * hd), lambda i, *_: (i, 0))
    return pl.pallas_call(
        partial(attend_back_kernel, (qh, kh, hd, stretch), scale),
        grid_spec=pltpu.PrefetchScalarGridSpec(
            num_scalar_prefetch=2,
            grid=(tiles,),
            in_specs=[
                whole((t, qh * hd)),
                tile_spec,
                whole((t, qh * hd)),
                whole((t, qh * hd)),
                whole((qh, t, 1)),
                whole((t, 1)),
                whole((t, 1)),
                whole((1, stretch)),
            ],
            out_specs=[whole((t, qh * hd)), tile_spec],
            scratch_shapes=[
                pltpu.VMEM((t, qh * hd), F32),
                pltpu.VMEM((qh, t, 1), F32),
                pltpu.VMEM((stretch, 2 * kh * hd), F32),
            ],
        ),
        out_shape=[
            jax.ShapeDtypeStruct((t, qh * hd), BF16),
            jax.ShapeDtypeStruct((kv.shape[0], 2 * kh * hd), BF16),
        ],
        cost_estimate=pl.CostEstimate(
            flops=10 * t * kv.shape[0] * hd * qh, bytes_accessed=6 * kv.size, transcendentals=t * kv.shape[0]
        ),
        name="attend_back",
    )(base, see, q, kv, do, o, lse, qpos, qfirst, off)


def unit_rows(values):
    rs = lax.rsqrt(jnp.mean(values * values, axis=-1, keepdims=True) + EPS)
    return values * rs, rs


def after(value, *others):
    return lax.optimization_barrier((value,) + others)[0]


def shards(
    n,
    layer_input,
    w_query,
    w_key,
    w_value,
    w_output,
    w_gate,
    w_up,
    w_down,
    norm_attn,
    norm_mlp,
    norm_query,
    norm_key,
    out_grad,
    doc_lengths,
    stretch_order,
):
    t, d = layer_input.shape
    hd = norm_query.shape[0]
    qh, kh = w_query.shape[1] // hd, w_key.shape[1] // hd
    stretch = t // 2
    quarter = t // 4
    width = d // n
    ny = n // NZ
    scale = hd ** (-0.5)
    blk, tp = lax.axis_index("blk"), lax.axis_index("tp")
    z, y = blk // ny, blk % ny

    order = ring_order(n)
    place = jnp.array([order.index(b) for b in range(n)], jnp.int32)
    me = lax.dynamic_index_in_dim(place, blk, keepdims=False)
    cols = jnp.take(jnp.array(order + order, jnp.int32), me + jnp.arange(n, dtype=jnp.int32))
    planes = (z + jnp.arange(NZ, dtype=jnp.int32)) % NZ

    def assemble(blocks):
        rows = blocks[0].shape[0]
        full = jnp.zeros((n * rows, blocks[0].shape[1]), blocks[0].dtype)
        for r in range(n):
            full = lax.dynamic_update_slice_in_dim(full, blocks[r], cols[r] * rows, 0)
        return full

    gain_attn = norm_attn.astype(F32)[:, None]
    gain_mlp = norm_mlp.astype(F32)[:, None]
    own_qkv = (jnp.concatenate([w_query, w_key, w_value], axis=1).astype(F32) * gain_attn).astype(BF16)
    blocks_qkv = ring_gather(own_qkv, n)
    full_qkv = assemble(blocks_qkv)

    starts = jnp.cumsum(doc_lengths) - doc_lengths

    def first_of(pos):
        return jnp.max(jnp.where(starts[None, :] <= pos[:, None], starts[None, :], 0), axis=1)

    inside = jnp.arange(stretch, dtype=jnp.int32)
    base = stretch_order * stretch
    base_own = lax.dynamic_slice_in_dim(base, 2 * blk, 2, 0)
    positions = (base_own[:, None] + inside[None, :]).reshape(-1)
    firsts = first_of(positions)
    base_first = first_of(base_own)
    see = ((base[None, :] <= base_own[:, None]) & (base[None, :] + (stretch - 1) >= base_first[:, None])).astype(jnp.int32)
    inverse = ROPE_BASE ** (-2.0 * jnp.arange(hd // 2, dtype=F32) / hd)
    angles = (positions - firsts).astype(F32)[:, None] * inverse[None, :]
    cosine, sine = jnp.cos(angles), jnp.sin(angles)
    cosine = jnp.concatenate([cosine, cosine], axis=1)
    sine = jnp.concatenate([-sine, sine], axis=1)
    qpos, qfirst, off = positions[:, None], firsts[:, None], inside[None, :]
    gains = jnp.stack([norm_query.astype(F32)[None, :], norm_key.astype(F32)[None, :]])

    unit_attn = unit_rows(layer_input.astype(F32))[0].astype(BF16)
    packed = pack(planes, w_gate, w_up, w_down, gain_mlp)
    raw_q, raw_k, q, kv_own = qkv_call(after(unit_attn, packed[0]), full_qkv, cosine, sine, gains, qh, kh, hd)
    blocks_out = ring_gather(after(w_output.T, blocks_qkv[n // 2 - 1], blocks_qkv[n // 2 + 1]), n)
    full_out = assemble(blocks_out)
    kv = assemble(ring_gather(kv_own, n))
    x_low = lax.dynamic_slice_in_dim(layer_input, tp * quarter, quarter, 0)
    attn_low, lse = attend(base, see, q, kv, qpos, qfirst, off, qh, kh, hd, scale)

    hidden, grad_hidden, grad_heads, hidden_low, grads, y_grads, acts, w_mlp = feed(
        n, attn_low, full_out, x_low.astype(F32), out_grad, packed
    )

    w3 = grads.shape[1]

    def line(value):
        return lax.dynamic_index_in_dim(value.reshape(NZ, ny, width, w3), y, 1, keepdims=False)

    owned = line(grads).astype(F32) + jnp.sum(y_grads.reshape(ny - 1, NZ, width, w3).astype(F32), axis=0)
    pair = 2 * w3 // 3
    norm_mlp_terms = jnp.sum(owned[:, :, :pair] * line(w_mlp)[:, :, :pair].astype(F32), axis=2, keepdims=True)
    norm_mlp_terms = jnp.broadcast_to(norm_mlp_terms, (NZ, width, hd))
    owned = owned.astype(BF16)
    pieces = [lax.dynamic_index_in_dim(owned, (z - s) % NZ, 0, keepdims=False) for s in range(NZ)]
    pieces = pieces[:1] + [z_shift(pieces[s], n, -s) for s in range(1, NZ)]

    dq, dkv = attend_back(base, see, q, kv, grad_heads, attn_low, lse, qpos, qfirst, off, qh, kh, hd, scale)
    ringed = n <= 8
    if not ringed:
        dkv = [lax.dynamic_slice_in_dim(dkv, cols[r] * t, t, 0).astype(F32) for r in range(n)]
        dkv = ring_scatter(lambda r: dkv[r], n, t)
    layer_output, input_grad, grad_q, grad_k, grad_v, grad_out_w, small = tail(
        n, ringed, dq, dkv, raw_q, raw_k, cosine, sine, gains, unit_attn, full_qkv, hidden_low, attn_low, grad_hidden,
        x_low, hidden, acts, w_mlp[:, pair:], w_query, w_key, w_value, gain_attn, norm_mlp_terms,
    )
    pieces = [after(piece, small) for piece in pieces]
    grad_gate, grad_up, grad_down = finish(planes, pieces, gain_mlp)
    heads = small[2 * width :, :]
    part = hd // n
    return (
        layer_output,
        input_grad,
        grad_q,
        grad_k,
        grad_v,
        grad_out_w,
        grad_gate,
        grad_up,
        grad_down,
        small[:width, 0],
        small[width : 2 * width, 0] / gain_mlp[:, 0],
        lax.dynamic_slice(heads, (0, blk * part), (1, part))[0],
        lax.dynamic_slice(heads, (1, blk * part), (1, part))[0],
    )


def solution(mesh):
    return jax.shard_map(
        partial(shards, mesh.shape["blk"]),
        mesh=mesh,
        in_specs=(
            P("blk", None),
            P("blk", "tp"),
            P("blk", "tp"),
            P("blk", "tp"),
            P("tp", "blk"),
            P("blk", "tp"),
            P("blk", "tp"),
            P("tp", "blk"),
            P("blk"),
            P("blk"),
            P(),
            P(),
            P("blk", None),
            P(),
            P(),
        ),
        out_specs=(
            P("blk", None),
            P("blk", None),
            P("blk", "tp"),
            P("blk", "tp"),
            P("blk", "tp"),
            P("tp", "blk"),
            P("blk", "tp"),
            P("blk", "tp"),
            P("tp", "blk"),
            P("blk"),
            P("blk"),
            P("blk"),
            P("blk"),
        ),
        check_vma=False,
    )
```

```python
from functools import partial

import jax
import jax.numpy as jnp
from jax import lax
from jax.experimental import pallas as pl
from jax.experimental.pallas import tpu as pltpu
from jax.sharding import PartitionSpec as P

EPS = 1e-06
ROPE_BASE = 1000000.0
F32 = jnp.float32
BF16 = jnp.bfloat16


def dot(a, b, dims, out=F32):
    return lax.dot_general(a, b, (dims, ((), ())), preferred_element_type=out)


NN = ((1,), (0,))
NT = ((1,), (1,))
TN = ((0,), (0,))


def ring_order(n):
    return list(range(0, n, 2)) + list(range(n - 1, 0, -2))


def ring_perms(n):
    order = ring_order(n)
    right = [(order[i], order[(i + 1) % n]) for i in range(n)]
    return right, [(b, a) for a, b in right]


def ring_scatter(part, n, rows):
    right, left = ring_perms(n)
    half = n // 2
    cut = rows // 2
    far = part(half).astype(BF16)
    to_right = lax.ppermute(far[:cut], "blk", right).astype(F32)
    to_left = lax.ppermute(far[cut:], "blk", left).astype(F32)
    if half == 1:
        return part(0) + jnp.concatenate([to_right, to_left], axis=0)
    for k in range(half - 1, 0, -1):
        send_right, send_left = part(k), part(n - k)
        if k == half - 1:
            send_right = jnp.concatenate([send_right[:cut] + to_right, send_right[cut:]], axis=0)
            send_left = jnp.concatenate([send_left[:cut], send_left[cut:] + to_left], axis=0)
        else:
            send_right = send_right + to_right
            send_left = send_left + to_left
        to_right = lax.ppermute(send_right.astype(BF16), "blk", right).astype(F32)
        to_left = lax.ppermute(send_left.astype(BF16), "blk", left).astype(F32)
    return part(0) + to_right + to_left


NZ = 4


def z_shift(value, n, s):
    ny = n // NZ
    pairs = [(z * ny + y, (z + s) % NZ * ny + y) for z in range(NZ) for y in range(ny)]
    return lax.ppermute(value, "blk", pairs)


def z_swap(value, n, k):
    ny = n // NZ
    pairs = [(z * ny + y, (z ^ k) * ny + y) for z in range(NZ) for y in range(ny)]
    return lax.ppermute(value, "blk", pairs)


VMEM = pl.BlockSpec(memory_space=pltpu.VMEM)
SMEM = pl.BlockSpec(memory_space=pltpu.SMEM)


def finish_kernel(zs_ref, *refs):
    pieces = refs[:NZ]
    gain_ref, d_gate, d_up, d_down = refs[NZ:]
    part = d_gate.shape[1] // NZ
    gain = gain_ref[...]
    for s in range(NZ):
        at = pl.ds(pl.multiple_of(zs_ref[s] * part, part), part)
        d_gate[:, at] = pieces[s][:, :part].astype(F32) * gain
        d_up[:, at] = pieces[s][:, part : 2 * part].astype(F32) * gain
        d_down[at, :] = pieces[s][:, 2 * part :].astype(F32).T


def finish(zs, pieces, gain):
    rows, cols = pieces[0].shape[0], NZ * pieces[0].shape[1] // 3
    return pl.pallas_call(
        finish_kernel,
        in_specs=[SMEM] + [VMEM] * (NZ + 1),
        out_specs=[VMEM] * 3,
        out_shape=[
            jax.ShapeDtypeStruct((rows, cols), F32),
            jax.ShapeDtypeStruct((rows, cols), F32),
            jax.ShapeDtypeStruct((cols, rows), F32),
        ],
        name="finish",
    )(zs, *pieces, gain)


MESH = pl.DeviceIdType.MESH


class Wires:
    def __init__(self, send, recv):
        self.send, self.recv, self.sent, self.done = send, recv, [], []

    def go(self, src, dst, device):
        i = len(self.sent)
        copy = pltpu.make_async_remote_copy(
            src_ref=src,
            dst_ref=dst,
            send_sem=self.send.at[i],
            recv_sem=self.recv.at[i],
            device_id=device,
            device_id_type=MESH,
        )
        copy.start()
        self.sent.append(copy)
        return copy

    def drain(self, copies):
        for copy in copies:
            copy.wait_send()
            self.done.append(copy)

    def close(self):
        self.drain([copy for copy in self.sent if not any(copy is other for other in self.done)])


def greet(devices):
    barrier = pltpu.get_barrier_semaphore()
    for device in devices:
        pl.semaphore_signal(barrier, inc=1, device_id=device, device_id_type=MESH)
    pl.semaphore_wait(barrier, len(devices))


class Spot:
    def __init__(self, n):
        self.n, self.ny = n, n // NZ
        self.blk, self.tp = lax.axis_index("blk"), lax.axis_index("tp")
        self.z, self.y = self.blk // self.ny, self.blk % self.ny
        self.x, self.core = self.tp // 2, self.tp % 2
        self.tp_core = self.x * 2 + (1 - self.core)
        self.tp_far = (1 - self.x) * 2 + self.core
        self.core_dev = {"tp": self.tp_core}
        self.far_dev = {"tp": self.tp_far}
        self.place = jnp.where(self.blk % 2 == 0, self.blk // 2, n - 1 - self.blk // 2)
        self.right_dev = {"blk": self.at_place(1)}
        self.left_dev = {"blk": self.at_place(n - 1)}

    def at_place(self, r):
        p = (self.place + r) % self.n
        return jnp.where(p < self.n // 2, 2 * p, 2 * (self.n - 1 - p) + 1)

    def plane(self, s):
        return (self.z + s) % NZ

    def z_dev(self, s):
        return {"blk": self.plane(s) * self.ny + self.y}

    def plane_x(self, k):
        return (self.z + 1 - 2 * (self.z % 2), (self.z + 2) % NZ, NZ - 1 - self.z)[k - 1]

    def x_dev(self, k):
        return {"blk": self.plane_x(k) * self.ny + self.y}

    def y_dev(self, j):
        return {"blk": self.z * self.ny + (self.y + j) % self.ny}

    def peers(self):
        return (
            [self.core_dev, self.far_dev]
            + [self.z_dev(s) for s in range(1, NZ)]
            + [self.y_dev(j) for j in range(1, self.ny)]
        )


def rows_at(index, count):
    return pl.ds(pl.multiple_of(index * count, count), count)


def feed_copies(n):
    return 60 + 8 * (n // NZ - 1)


def feed_kernel(n, attn, wo, x_own, g_rows, g_one, g_two, *refs):
    packed = refs[:NZ]
    hidden_o, gh_o, heads_o, hl_o, dw_o, y_o, act_o, w_o = refs[NZ : NZ + 8]
    (u_all, g_all, dgu, o_part, o_far, o_core, o_x, part, near, core_in, x_in, z_in, m_acc, dw_tile, send, recv, dw_sem) = refs[NZ + 8 :]
    q, d = x_own.shape
    p = packed[0].shape[1] // 3
    bw = packed[0].shape[0]
    me = Spot(n)
    wires = Wires(send, recv)
    greet(me.peers())

    def quarter(plane, peer):
        return rows_at(plane * 4 + peer, q)

    def pass_on(buf, plane, src=None):
        at = quarter(plane, me.tp)
        src = buf.at[at] if src is None else src
        return wires.go(src, buf.at[at], me.far_dev), wires.go(src, buf.at[at], me.core_dev)

    def pass_far(buf, plane, copies):
        copies[0].wait_recv()
        at = quarter(plane, me.tp_far)
        return copies[1], wires.go(buf.at[at], buf.at[at], me.core_dev)

    def arrived(copies):
        for copy in copies:
            copy.wait_recv()

    mine = rows_at(me.blk, bw)
    two = rows_at(me.plane(2) * me.ny + me.y, bw)
    w_z = {1: wires.go(packed[1], w_o.at[mine], me.z_dev(1)), 3: wires.go(packed[2], w_o.at[mine], me.z_dev(3))}
    near_plane, over_plane, last_plane = me.plane_x(1), me.plane_x(2), me.plane_x(3)
    near_dev, over_dev = me.x_dev(1), me.x_dev(2)
    g_three = wires.go(g_two, g_all.at[quarter(over_plane, me.tp)], near_dev)
    g_one_pass = pass_on(g_all, near_plane, g_one)
    w_y = [wires.go(packed[0], w_o.at[mine], me.y_dev(j)) for j in range(1, me.ny)]
    w_y += [wires.go(packed[3], w_o.at[two], me.y_dev(j)) for j in range(1, me.ny)]

    def project(peer):
        return dot(attn[rows_at(peer, q), :], wo[...], NT)

    for i, x in enumerate((1 - me.x, me.x)):
        o_part[i] = project(x * 2 + 1 - me.core).astype(BF16)
    far_in = wires.go(o_part.at[0], o_core.at[0], me.core_dev)
    near_in = wires.go(o_part.at[1], o_core.at[1], me.core_dev)
    own_far = project(me.tp_far)
    far_in.wait_recv()
    o_far[...] = (own_far + o_core[0].astype(F32)).astype(BF16)
    x_sum = wires.go(o_far, o_x, me.far_dev)
    own_sum = project(me.tp) + x_own[...]
    w_o[mine, :] = packed[0][...]
    w_o[two, :] = packed[3][...]
    g_all[rows_at(me.z, 4 * q), :] = g_rows[...]
    g_all[quarter(near_plane, me.tp), :] = g_one[...]
    g_all[quarter(over_plane, me.tp), :] = g_two[...]
    near_in.wait_recv()
    own_sum = own_sum + o_core[1].astype(F32)
    x_sum.wait_recv()
    hidden = own_sum + o_x[...].astype(F32)
    hidden_o[...] = hidden
    rs = lax.rsqrt(jnp.mean(hidden * hidden, axis=-1, keepdims=True) + EPS)
    own_q = quarter(me.z, me.tp)
    u_all[own_q, :] = (hidden * rs).astype(BF16)

    own_pass = pass_on(u_all, me.z)
    u_one = wires.go(u_all.at[own_q], u_all.at[own_q], near_dev)
    u_two = wires.go(u_all.at[own_q], u_all.at[own_q], over_dev)
    g_one_pass = pass_far(g_all, near_plane, g_one_pass)
    g_two_pass = pass_on(g_all, over_plane, g_two)
    for s in (1, 3):
        w_z[s].wait_recv()
        at = rows_at(me.plane(-s) * me.ny + me.y, bw)
        w_y += [wires.go(w_o.at[at], w_o.at[at], me.y_dev(j)) for j in range(1, me.ny)]
    own_pass = pass_far(u_all, me.z, own_pass)
    arrived(w_y)
    arrived(own_pass)

    def compute(i, plane):
        @pl.loop(0, 2)
        def _(k):
            at = pl.ds(pl.multiple_of(plane * (4 * q) + k * (2 * q), 2 * q), 2 * q)
            gate_up = dot(u_all[at, :], w_o[:, : 2 * p], NN)
            grad_act = dot(g_all[at, :], w_o[:, 2 * p :], NN)
            gate, up = gate_up[:, :p], gate_up[:, p:]
            sig = 1.0 / (1.0 + jnp.exp(-gate))
            silu = gate * sig
            act_o[at, :] = (silu * up).astype(BF16)
            dgu[at, p:] = (grad_act * silu).astype(BF16)
            dgu[at, :p] = (grad_act * up * (sig * (1.0 + gate * (1.0 - sig)))).astype(BF16)

        rows = rows_at(plane, 4 * q)
        tile = 512

        @pl.loop(0, d // tile)
        def _(c):
            at = pl.ds(pl.multiple_of(c * tile, tile), tile)
            part[i % 2, :, at] = dot(dgu[rows, :], w_o[at, : 2 * p], NT).astype(BF16)

    cores, fars = {}, {}

    def reduce_core(i):
        cores[i] = []
        for k, x in enumerate((1 - me.x, me.x)):
            src = part.at[i % 2, rows_at(x * 2 + 1 - me.core, q)]
            cores[i].append(wires.go(src, core_in.at[i, k], me.core_dev))

    def reduce_far(i):
        cores[i][0].wait_recv()
        core_in[i, 0] = (part[i % 2, rows_at(me.tp_far, q), :].astype(F32) + core_in[i, 0].astype(F32)).astype(BF16)
        fars[i] = wires.go(core_in.at[i, 0], x_in.at[i], me.far_dev)

    def reduce_near(i):
        cores[i][1].wait_recv()
        fars[i].wait_recv()
        value = part[i % 2, rows_at(me.tp, q), :].astype(F32) + core_in[i, 1].astype(F32) + x_in[i].astype(F32)
        wires.drain(cores[i])
        return value

    def dw_copy(c, slot):
        rows = pl.ds(pl.multiple_of(c * 256, 256), 256)
        return pltpu.make_async_copy(dw_tile.at[slot], dw_o.at[rows], dw_sem.at[slot])

    def grads(first, last):
        @pl.loop(first, last)
        def _(c):
            slot = c % 2

            @pl.when(c >= first + 2)
            def _():
                dw_copy(c - 2, slot).wait()

            at = pl.ds(pl.multiple_of(c * 256, 256), 256)
            dw_tile[slot, :, : 2 * p] = dot(u_all[:, at], dgu[...], TN).astype(BF16)
            dw_tile[slot, :, 2 * p :] = dot(g_all[:, at], act_o[...], TN).astype(BF16)
            dw_copy(c, slot).start()

        for c in (last - 2, last - 1):
            dw_copy(c, c % 2).wait()
        planes = NZ * first * 256 // d, NZ * last * 256 // d
        return [
            wires.go(dw_o.at[rows_at(plane * me.ny + (me.y + j) % me.ny, bw)], y_o.at[(j - 1) * NZ + plane], me.y_dev(j))
            for plane in range(*planes)
            for j in range(1, me.ny)
        ]

    compute(0, me.z)
    reduce_core(0)
    u_one.wait_recv()
    u_one_pass = pass_on(u_all, near_plane)
    u_two.wait_recv()
    u_three = wires.go(u_all.at[quarter(over_plane, me.tp)], u_all.at[quarter(over_plane, me.tp)], near_dev)
    u_two_pass = pass_on(u_all, over_plane)
    reduce_far(0)
    g_two_pass = pass_far(g_all, over_plane, g_two_pass)
    u_one_pass = pass_far(u_all, near_plane, u_one_pass)
    arrived(g_one_pass)
    arrived(u_one_pass)
    compute(1, near_plane)
    reduce_core(1)
    u_two_pass = pass_far(u_all, over_plane, u_two_pass)
    u_three.wait_recv()
    u_three_pass = pass_on(u_all, last_plane)
    g_three.wait_recv()
    g_three_pass = pass_on(g_all, last_plane)
    m_acc[...] = reduce_near(0)
    reduce_far(1)
    arrived(g_two_pass)
    arrived(u_two_pass)
    compute(2, over_plane)
    reduce_core(2)
    u_three_pass = pass_far(u_all, last_plane, u_three_pass)
    near[0] = reduce_near(1).astype(BF16)
    z_one = wires.go(near.at[0], z_in.at[0], near_dev)
    g_three_pass = pass_far(g_all, last_plane, g_three_pass)
    reduce_far(2)
    arrived(u_three_pass)
    arrived(g_three_pass)
    compute(3, last_plane)
    reduce_core(3)
    tiles = d // 256
    y_copies = grads(0, tiles // 4)
    reduce_far(3)
    near[1] = reduce_near(2).astype(BF16)
    y_copies += grads(tiles // 4, 3 * tiles // 4)
    near[2] = reduce_near(3).astype(BF16)
    z_three = wires.go(near.at[2], z_in.at[1], near_dev)
    y_copies += grads(3 * tiles // 4, tiles)
    z_three.wait_recv()
    near[1] = (near[1].astype(F32) + z_in[1].astype(F32)).astype(BF16)
    z_two = wires.go(near.at[1], z_in.at[2], over_dev)
    z_one.wait_recv()
    m = m_acc[...] + z_in[0].astype(F32)
    z_two.wait_recv()
    m = m + z_in[2].astype(F32)

    hidden = hidden_o[...]
    rs = lax.rsqrt(jnp.mean(hidden * hidden, axis=-1, keepdims=True) + EPS)
    unit = hidden * rs
    grad = g_rows[rows_at(me.tp, q), :].astype(F32) + (m - unit * jnp.mean(m * unit, axis=-1, keepdims=True)) * rs
    gh_o[...] = grad
    own = rows_at(me.tp, q)
    hl_o[own, :] = grad.astype(BF16)
    x_copy = wires.go(hl_o.at[own], hl_o.at[own], me.far_dev)
    c_copy = wires.go(hl_o.at[own], hl_o.at[own], me.core_dev)

    def heads(peer):
        heads_o[rows_at(peer, q), :] = dot(hl_o[rows_at(peer, q), :], wo[...], NN).astype(BF16)

    heads(me.tp)
    c_copy.wait_recv()
    heads(me.tp_core)
    x_copy.wait_recv()
    at = rows_at(me.tp_far, q)
    last = wires.go(hl_o.at[at], hl_o.at[at], me.core_dev)
    heads(me.tp_far)
    last.wait_recv()
    heads((1 - me.x) * 2 + 1 - me.core)
    arrived(y_copies)
    wires.close()


def feed(n, attn, wo, x_own, g_rows, g_one, g_two, packed):
    q, d = x_own.shape
    t, a = attn.shape
    bw, w3 = packed[0].shape
    p = w3 // 3
    tokens = NZ * t
    copies = feed_copies(n)
    vm = pltpu.VMEM
    return pl.pallas_call(
        partial(feed_kernel, n),
        in_specs=[VMEM] * (6 + NZ),
        out_specs=[VMEM] * 4 + [pl.BlockSpec(memory_space=pl.ANY)] * 2 + [VMEM] * 2,
        out_shape=[
            jax.ShapeDtypeStruct((q, d), F32),
            jax.ShapeDtypeStruct((q, d), F32),
            jax.ShapeDtypeStruct((t, a), BF16),
            jax.ShapeDtypeStruct((t, d), BF16),
            jax.ShapeDtypeStruct((d, w3), BF16),
            jax.ShapeDtypeStruct((NZ * (n // NZ - 1), bw, w3), BF16),
            jax.ShapeDtypeStruct((tokens, p), BF16),
            jax.ShapeDtypeStruct((d, w3), BF16),
        ],
        scratch_shapes=[
            vm((tokens, d), BF16),
            vm((tokens, d), BF16),
            vm((tokens, 2 * p), BF16),
            vm((2, q, d), BF16),
            vm((q, d), BF16),
            vm((2, q, d), BF16),
            vm((q, d), BF16),
            vm((2, t, d), BF16),
            vm((NZ - 1, q, d), BF16),
            vm((NZ, 2, q, d), BF16),
            vm((NZ, q, d), BF16),
            vm((NZ - 1, q, d), BF16),
            vm((q, d), F32),
            vm((2, 256, w3), BF16),
            pltpu.SemaphoreType.DMA((copies,)),
            pltpu.SemaphoreType.DMA((copies,)),
            pltpu.SemaphoreType.DMA((2,)),
        ],
        compiler_params=pltpu.CompilerParams(
            collective_id=1, has_side_effects=True, vmem_limit_bytes=67000000
        ),
        name="feed",
    )(attn, wo, x_own, g_rows, g_one, g_two, *packed)


class RingSum:
    def __init__(self, wires, me, land, stage, part):
        self.wires, self.me, self.land, self.stage, self.part = wires, me, land, stage, part
        self.half = me.n // 2
        self.cut = land.shape[2] // 2
        self.got = None

    def start(self):
        top, low, cut = pl.ds(0, self.cut), pl.ds(self.cut, self.cut), self.half - 1
        self.stage[...] = self.part(self.half).astype(BF16)
        self.got = (
            self.wires.go(self.stage.at[top], self.land.at[0, cut, top], self.me.right_dev),
            self.wires.go(self.stage.at[low], self.land.at[1, cut, low], self.me.left_dev),
        )
        self.first = self.got

    def step(self, k):
        cut = self.cut
        for side, place in ((0, k), (1, self.me.n - k)):
            self.got[side].wait_recv()
            mine = self.part(place)
            if k == self.half - 1:
                keep, fresh = (slice(0, cut), slice(cut, None)) if side == 0 else (slice(cut, None), slice(0, cut))
                self.land[side, k, keep, :] = (self.land[side, k, keep, :].astype(F32) + mine[keep]).astype(BF16)
                self.land[side, k, fresh, :] = mine[fresh].astype(BF16)
            else:
                self.land[side, k] = (self.land[side, k].astype(F32) + mine).astype(BF16)
        self.got = tuple(
            self.wires.go(self.land.at[side, k], self.land.at[side, k - 1], dev)
            for side, dev in ((0, self.me.right_dev), (1, self.me.left_dev))
        )

    def total(self):
        for copy in self.got:
            copy.wait_recv()
        return self.part(0) + self.land[0, 0].astype(F32) + self.land[1, 0].astype(F32)


def tail_copies(n):
    return 2 * 3 * (n // 2) + 16 + 3 + 3 + 3 + 3 + 3 + 2 + 8


def tail_kernel(n, ringed, *refs):
    (dq, dkv, raw_q, raw_k, cos_ref, sin_ref, gain_ref, u1, wqkv, hl, attn, gh, x_own, hidden, act, w_down) = refs[:16]
    w_q, w_k, w_v, gain_attn, norm_in = refs[16:21]
    lo, ig, gq_o, gk_o, gv_o, go_o, small_o = refs[21:28]
    (d_qkv, gains, kv_land, kv_stage, o_land, o_stage, w_land, w_stage, m_part, m_core, m_x, part, core_in, x_in, z_in) = refs[28:43]
    ig_low, norm_land, small_core, small_x, o_whole, w_whole, send, recv = refs[43:]
    q, d = hidden.shape
    t, qw = dq.shape
    hd = cos_ref.shape[1]
    kw = raw_k.shape[1]
    bw = w_q.shape[0]
    me = Spot(n)
    wires = Wires(send, recv)
    greet(me.peers() + [me.right_dev, me.left_dev])

    norm_copies = [
        wires.go(norm_in.at[me.plane(s)], norm_land.at[s - 1], me.z_dev(s)) for s in range(1, NZ)
    ]

    def head_back(src, raw, heads, kind, to):
        gains[kind] = jnp.zeros((1, hd), F32)

        @pl.loop(0, 4)
        def _(k):
            at = pl.ds(pl.multiple_of(k * q, q), q)
            cosine, sine = cos_ref[at, :], sin_ref[at, :]
            for h in range(heads):
                cols = slice(h * hd, (h + 1) * hd)
                grad = src[at, cols].astype(F32)
                grad = grad * cosine - turned(grad, sine)
                v = raw[at, cols]
                rs = lax.rsqrt(jnp.mean(v * v, axis=-1, keepdims=True) + EPS)
                unit = v * rs
                gains[kind] += jnp.sum(grad * unit, axis=0, keepdims=True)
                m = grad * gain_ref[kind]
                back = (m - unit * jnp.mean(m * unit, axis=-1, keepdims=True)) * rs
                d_qkv[at, to + h * hd : to + (h + 1) * hd] = back.astype(BF16)

    slots = (1, 3, 2, 0)
    cores, fars, backs = {}, {}, {}

    def down(i):
        rows = rows_at(me.plane(-slots[i]), 4 * q)
        tile = 512

        @pl.loop(0, d // tile)
        def _(c):
            at = pl.ds(pl.multiple_of(c * tile, tile), tile)
            part[i % 2, :, at] = dot(act[rows, :], w_down[at, :], NT).astype(BF16)

        cores[i] = [
            wires.go(part.at[i % 2, rows_at(x * 2 + 1 - me.core, q)], core_in.at[i, k], me.core_dev)
            for k, x in enumerate((1 - me.x, me.x))
        ]

    def down_far(i):
        cores[i][0].wait_recv()
        core_in[i, 0] = (part[i % 2, rows_at(me.tp_far, q), :].astype(F32) + core_in[i, 0].astype(F32)).astype(BF16)
        fars[i] = wires.go(core_in.at[i, 0], x_in.at[i], me.far_dev)

    def down_near(i):
        cores[i][1].wait_recv()
        fars[i].wait_recv()
        value = part[i % 2, rows_at(me.tp, q), :].astype(F32) + core_in[i, 1].astype(F32) + x_in[i].astype(F32)
        wires.drain(cores[i])
        if slots[i] == 0:
            return value
        x_in[i] = value.astype(BF16)
        backs[i] = wires.go(x_in.at[i], z_in.at[i], me.z_dev(-slots[i]))

    def term(left, right, whole):
        if bw % 128 == 0:
            return lambda r: dot(left[:, rows_at(me.at_place(r), bw)], right[...], TN)

        @pl.loop(0, d // 256)
        def _(c):
            at = rows_at(c, 256)
            whole[at, :] = dot(left[:, at], right[...], TN).astype(BF16)

        return lambda r: whole[rows_at(me.at_place(r), bw), :].astype(F32)

    o_part = term(hl, attn, o_whole)

    o_ring = RingSum(wires, me, o_land, o_stage, o_part)

    half = n // 2
    if ringed:
        kv_ring = RingSum(wires, me, kv_land, kv_stage, lambda r: dkv[rows_at(me.at_place(r), t), :].astype(F32))
        kv_ring.start()
    head_back(dq, raw_q, qw // hd, 0, 0)
    fill = [
        lambda: (o_ring.start(), down(0)),
        lambda: (down_far(0), down(1)),
        lambda: (down_near(0), down_far(1), down(2)),
        lambda: (down_near(1), down_far(2), down(3)),
    ]
    for k in range(half - 1, 0, -1):
        if ringed:
            kv_ring.step(k)
        if fill:
            fill.pop(0)()
        if k < half - 1:
            o_ring.step(k + 1)
    for job in fill:
        job()
    if half > 1:
        o_ring.step(1)
    if ringed:
        kv_total = kv_ring.total().astype(BF16)
        wires.drain(kv_ring.first)
        kv_stage[...] = kv_total
        kv_sum = kv_stage
    else:
        kv_sum = dkv
    head_back(kv_sum, raw_k, kw // hd, 1, qw)
    d_qkv[:, qw + kw :] = kv_sum[:, kw:].astype(BF16)

    def m_term(peer):
        return dot(d_qkv[rows_at(peer, q), :], wqkv[...], NT)

    w_term = term(u1, d_qkv, w_whole)

    def qkv_part(r):
        body = w_term(r)
        extra = w_land.shape[2] - bw
        rest = jnp.concatenate([gains[0], gains[1], jnp.zeros((extra - 2, hd), F32)], axis=0)
        rest = jnp.concatenate([rest, jnp.zeros((extra, body.shape[1] - hd), F32)], axis=1)
        return jnp.concatenate([body, rest], axis=0)

    w_ring = RingSum(wires, me, w_land, w_stage, qkv_part)
    for i, x in enumerate((1 - me.x, me.x)):
        m_part[i] = m_term(x * 2 + 1 - me.core).astype(BF16)
    m_far = wires.go(m_part.at[0], m_core.at[0], me.core_dev)
    m_near = wires.go(m_part.at[1], m_core.at[1], me.core_dev)
    w_ring.start()
    own_far = m_term(me.tp_far)
    m_far.wait_recv()
    m_core[0] = (own_far + m_core[0].astype(F32)).astype(BF16)
    m_sum = wires.go(m_core.at[0], m_x, me.far_dev)
    own = m_term(me.tp)
    m_near.wait_recv()
    own = own + m_core[1].astype(F32)
    steps = list(range(half - 1, 0, -1))
    if steps:
        w_ring.step(steps.pop(0))
    m_sum.wait_recv()
    m = own + m_x[...].astype(F32)
    x = x_own[...].astype(F32)
    rs = lax.rsqrt(jnp.mean(x * x, axis=-1, keepdims=True) + EPS)
    unit = x * rs
    grad = gh[...] + (m - unit * jnp.mean(m * unit, axis=-1, keepdims=True)) * rs
    mine = rows_at(me.tp, q)
    ig_low[mine, :] = grad.astype(BF16)

    def spread(buf):
        far = wires.go(buf.at[mine], buf.at[mine], me.far_dev)
        core = wires.go(buf.at[mine], buf.at[mine], me.core_dev)
        return far, core

    def spread_far(buf, copies):
        copies[0].wait_recv()
        at = rows_at(me.tp_far, q)
        return wires.go(buf.at[at], buf.at[at], me.core_dev)

    ig_copies = spread(ig_low)
    if steps:
        w_ring.step(steps.pop(0))

    down_near(2)
    down_far(3)
    out = hidden[...] + down_near(3)
    for i in range(NZ - 1):
        backs[i].wait_recv()
        out = out + z_in[i].astype(F32)
    lo[mine, :] = out.astype(BF16)
    lo_copies = spread(lo)
    ig_last = spread_far(ig_low, ig_copies)
    while steps:
        w_ring.step(steps.pop(0))
    go_o[...] = o_ring.total().T

    lo_last = spread_far(lo, lo_copies)
    ig_copies[1].wait_recv()
    ig_last.wait_recv()
    ig[...] = ig_low[...].astype(F32)
    total = w_ring.total()
    grad = total[:bw]
    gain = gain_attn[...]
    norm = jnp.sum(grad[:, :qw] * w_q[...].astype(F32), axis=1, keepdims=True)
    norm = norm + jnp.sum(grad[:, qw : qw + kw] * w_k[...].astype(F32), axis=1, keepdims=True)
    norm = norm + jnp.sum(grad[:, qw + kw :] * w_v[...].astype(F32), axis=1, keepdims=True)
    small_o[:bw, :] = jnp.broadcast_to(norm, (bw, hd))
    mlp = norm_in[me.z]
    for s in range(1, NZ):
        norm_copies[s - 1].wait_recv()
        mlp = mlp + norm_land[s - 1]
    small_o[bw : 2 * bw, :] = mlp
    small_o[2 * bw :, :] = total[bw : bw + 16, :hd]
    copy = wires.go(small_o, small_core, me.core_dev)
    gq_o[...] = grad[:, :qw] * gain
    gk_o[...] = grad[:, qw : qw + kw] * gain
    gv_o[...] = grad[:, qw + kw :] * gain
    copy.wait_recv()
    small_core[...] += small_o[...]
    copy = wires.go(small_core, small_x, me.far_dev)
    lo_copies[1].wait_recv()
    lo_last.wait_recv()
    copy.wait_recv()
    wires.close()
    small_o[...] = small_core[...] + small_x[...]


def tail(n, ringed, dq, dkv, raw_q, raw_k, cosine, sine, gains, u1, wqkv, hl, attn, gh, x_own, hidden, act, w_down, w_q, w_k, w_v, gain_attn, norm_in):
    q, d = hidden.shape
    t, qw = dq.shape
    hd = cosine.shape[1]
    kw = raw_k.shape[1]
    wide = qw + 2 * kw
    bw = d // n
    half = n // 2
    copies = tail_copies(n)
    vm = pltpu.VMEM
    small = 2 * bw + 16
    shape = jax.ShapeDtypeStruct
    return pl.pallas_call(
        partial(tail_kernel, n, ringed),
        in_specs=[VMEM] * 21,
        out_specs=[VMEM] * 7,
        out_shape=[
            shape((t, d), BF16),
            shape((t, d), F32),
            shape((bw, qw), F32),
            shape((bw, kw), F32),
            shape((bw, kw), F32),
            shape((attn.shape[1], bw), F32),
            shape((small, hd), F32),
        ],
        scratch_shapes=[
            vm((t, wide), BF16),
            vm((2, 1, hd), F32),
            vm((2, half, t, 2 * kw) if ringed else (2, 1, 16, 128), BF16),
            vm((t, 2 * kw) if ringed else (16, 128), BF16),
            vm((2, half, bw, attn.shape[1]), BF16),
            vm((bw, attn.shape[1]), BF16),
            vm((2, half, bw + 32, wide), BF16),
            vm((bw + 32, wide), BF16),
            vm((2, q, d), BF16),
            vm((2, q, d), BF16),
            vm((q, d), BF16),
            vm((2, t, d), BF16),
            vm((NZ, 2, q, d), BF16),
            vm((NZ, q, d), BF16),
            vm((NZ - 1, q, d), BF16),
            vm((t, d), BF16),
            vm((NZ - 1, bw, hd), F32),
            vm((small, hd), F32),
            vm((small, hd), F32),
            vm((d, attn.shape[1]) if bw % 128 else (16, 128), BF16),
            vm((d, wide) if bw % 128 else (16, 128), BF16),
            pltpu.SemaphoreType.DMA((copies,)),
            pltpu.SemaphoreType.DMA((copies,)),
        ],
        compiler_params=pltpu.CompilerParams(
            collective_id=2, has_side_effects=True, vmem_limit_bytes=67000000
        ),
        name="tail",
    )(dq, dkv, raw_q, raw_k, cosine, sine, gains, u1, wqkv, hl, attn, gh, x_own, hidden, act, w_down, w_q, w_k, w_v, gain_attn, norm_in)


def turned(v, sine):
    return pltpu.roll(v, v.shape[1] // 2, 1) * sine


class RingGather:
    def __init__(self, wires, me, buf, rows):
        self.wires, self.me, self.buf, self.rows = wires, me, buf, rows
        self.half = me.n // 2
        self.got = None

    def send(self, right, left):
        buf = self.buf
        self.got = (
            self.wires.go(buf.at[right], buf.at[right], self.me.right_dev),
            self.wires.go(buf.at[left], buf.at[left], self.me.left_dev),
        )

    def wait(self):
        for copy in self.got:
            copy.wait_recv()

    def step(self, k):
        if k > 1:
            self.wait()
        rows = self.rows
        right, left = self.me.at_place(self.me.n - k + 1) * rows, self.me.at_place(k - 1) * rows
        size = rows
        if k == self.half:
            size = rows // 2
            left = left + size
        self.send(pl.ds(pl.multiple_of(right, size), size), pl.ds(pl.multiple_of(left, size), size))


def head_copies(n):
    return 3 * n + 1


def head_kernel(n, x, w_q, w_k, w_v, gain_attn, w_out, w_gate, w_up, w_down, gain_mlp, cos_ref, sin_ref, gain_ref, *refs):
    raw_q, raw_k, q_o, kv_o, u1, wqkv, wo = refs[:7]
    packed, w_far = refs[7:10], refs[10]
    own_far, send, recv = refs[11:]
    t, d = x.shape
    hd = cos_ref.shape[1]
    qw, kw = w_q.shape[1], w_k.shape[1]
    bw = w_q.shape[0]
    p = w_gate.shape[1] // NZ
    me = Spot(n)
    wires = Wires(send, recv)
    greet([me.right_dev, me.left_dev, me.z_dev(2)])
    half = n // 2
    mine = rows_at(me.blk, bw)

    gain = gain_attn[...]
    wqkv[mine, :qw] = (w_q[...].astype(F32) * gain).astype(BF16)
    wqkv[mine, qw : qw + kw] = (w_k[...].astype(F32) * gain).astype(BF16)
    wqkv[mine, qw + kw :] = (w_v[...].astype(F32) * gain).astype(BF16)
    w_ring = RingGather(wires, me, wqkv, bw)
    w_ring.step(1)

    def unit():
        @pl.loop(0, 4)
        def _(k):
            at = rows_at(k, t // 4)
            v = x[at, :].astype(F32)
            u1[at, :] = (v * lax.rsqrt(jnp.mean(v * v, axis=-1, keepdims=True) + EPS)).astype(BF16)

    def pack(s, to):
        at = rows_at(me.plane(s), p)
        gain = gain_mlp[...]
        to[:, :p] = (w_gate[:, at].astype(F32) * gain).astype(BF16)
        to[:, p : 2 * p] = (w_up[:, at].astype(F32) * gain).astype(BF16)
        to[:, 2 * p :] = w_down[at, :].astype(F32).T.astype(BF16)

    def output_block():
        wo[mine, :] = w_out[...].astype(F32).T.astype(BF16)

    jobs = [
        lambda: (unit(), output_block()),
        lambda: (pack(2, own_far), pack(0, packed[0])),
        lambda: (pack(1, packed[1]), pack(3, packed[2])),
    ]
    for k in range(2, half + 1):
        if jobs:
            jobs.pop(0)()
        w_ring.step(k)
    for job in jobs:
        job()
    far = wires.go(own_far, w_far, me.z_dev(2))
    w_ring.wait()

    rows = t // 2

    @pl.loop(0, 2)
    def _(k):
        at = rows_at(k, rows)
        own = pl.ds(pl.multiple_of(me.blk * t + k * rows, rows), rows)
        y = dot(u1[at, :], wqkv[...], NN)
        raw_q[at, :] = y[:, :qw]
        raw_k[at, :] = y[:, qw : qw + kw]
        cosine, sine = cos_ref[at, :], sin_ref[at, :]
        for h in range((qw + kw) // hd):
            v = y[:, h * hd : (h + 1) * hd]
            rs = lax.rsqrt(jnp.mean(v * v, axis=-1, keepdims=True) + EPS)
            v = v * rs * gain_ref[0 if h * hd < qw else 1]
            v = (v * cosine + turned(v, sine)).astype(BF16)
            if h * hd < qw:
                q_o[at, h * hd : (h + 1) * hd] = v
            else:
                kv_o[own, h * hd - qw : (h + 1) * hd - qw] = v
        kv_o[own, kw:] = y[:, qw + kw :].astype(BF16)

    kv_ring = RingGather(wires, me, kv_o, t)
    o_ring = RingGather(wires, me, wo, bw)
    for k in range(1, half + 1):
        kv_ring.step(k)
        o_ring.step(k)
    kv_ring.wait()
    o_ring.wait()
    far.wait_recv()
    wires.close()


def head(n, x, w_q, w_k, w_v, gain_attn, w_out, w_gate, w_up, w_down, gain_mlp, cosine, sine, gains):
    t, d = x.shape
    bw, qw = w_q.shape
    kw = w_k.shape[1]
    w3 = 3 * w_gate.shape[1] // NZ
    shape = jax.ShapeDtypeStruct
    copies = head_copies(n)
    return pl.pallas_call(
        partial(head_kernel, n),
        in_specs=[VMEM] * 13,
        out_specs=[VMEM] * 11,
        out_shape=[
            shape((t, qw), F32),
            shape((t, kw), F32),
            shape((t, qw), BF16),
            shape((n * t, 2 * kw), BF16),
            shape((t, d), BF16),
            shape((d, qw + 2 * kw), BF16),
            shape((d, qw), BF16),
        ]
        + [shape((bw, w3), BF16)] * 4,
        scratch_shapes=[
            pltpu.VMEM((bw, w3), BF16),
            pltpu.SemaphoreType.DMA((copies,)),
            pltpu.SemaphoreType.DMA((copies,)),
        ],
        compiler_params=pltpu.CompilerParams(
            collective_id=3, has_side_effects=True, vmem_limit_bytes=67000000
        ),
        name="head",
    )(x, w_q, w_k, w_v, gain_attn, w_out, w_gate, w_up, w_down, gain_mlp, cosine, sine, gains)


def tile_masks(base_ref, tile, qpos_ref, qfirst_ref, off_ref, q0, stretch):
    kpos = off_ref[...] + base_ref[tile]
    qpos = qpos_ref[pl.ds(q0, stretch), :]
    qfirst = qfirst_ref[pl.ds(q0, stretch), :]
    return (kpos <= qpos) & (kpos >= qfirst)


def attend_kernel(dims, scale, base_ref, see_ref, q_ref, kv_ref, qpos_ref, qfirst_ref, off_ref, out_ref, lse_ref, acc_ref, sum_ref):
    qh, kh, hd, stretch = dims
    group = qh // kh
    tile = pl.program_id(0)
    last = pl.num_programs(0) - 1

    @pl.when(tile == 0)
    def _():
        acc_ref[...] = jnp.zeros_like(acc_ref)
        sum_ref[...] = jnp.zeros_like(sum_ref)

    for e in range(2):
        q0 = e * stretch

        @pl.when(see_ref[e, tile] > 0)
        def _():
            mask = tile_masks(base_ref, tile, qpos_ref, qfirst_ref, off_ref, q0, stretch)
            for h in range(qh):
                k = kv_ref[:, (h // group) * hd : (h // group + 1) * hd]
                v = kv_ref[:, (kh + h // group) * hd : (kh + h // group + 1) * hd]
                q = q_ref[q0 : q0 + stretch, h * hd : (h + 1) * hd]
                s = dot(q, k, NT) * scale
                p = jnp.where(mask, jnp.exp(s), 0.0)
                sum_ref[h, q0 : q0 + stretch, :] += jnp.sum(p, axis=-1, keepdims=True)
                acc_ref[q0 : q0 + stretch, h * hd : (h + 1) * hd] += dot(p.astype(BF16), v, NN)

    @pl.when(tile == last)
    def _():
        for h in range(qh):
            total = sum_ref[h]
            out_ref[:, h * hd : (h + 1) * hd] = (acc_ref[:, h * hd : (h + 1) * hd] / total).astype(BF16)
            lse_ref[h] = jnp.log(total)


def attend(base, see, q, kv, qpos, qfirst, off, qh, kh, hd, scale):
    t = q.shape[0]
    stretch = t // 2
    tiles = kv.shape[0] // stretch

    def whole(shape):
        return pl.BlockSpec(shape, lambda i, *_: (0,) * len(shape))

    return pl.pallas_call(
        partial(attend_kernel, (qh, kh, hd, stretch), scale),
        grid_spec=pltpu.PrefetchScalarGridSpec(
            num_scalar_prefetch=2,
            grid=(tiles,),
            in_specs=[
                whole((t, qh * hd)),
                pl.BlockSpec((stretch, 2 * kh * hd), lambda i, *_: (i, 0)),
                whole((t, 1)),
                whole((t, 1)),
                whole((1, stretch)),
            ],
            out_specs=[whole((t, qh * hd)), whole((qh, t, 1))],
            scratch_shapes=[pltpu.VMEM((t, qh * hd), F32), pltpu.VMEM((qh, t, 1), F32)],
        ),
        out_shape=[
            jax.ShapeDtypeStruct((t, qh * hd), BF16),
            jax.ShapeDtypeStruct((qh, t, 1), F32),
        ],
        cost_estimate=pl.CostEstimate(
            flops=4 * t * kv.shape[0] * hd * qh, bytes_accessed=2 * kv.size, transcendentals=t * kv.shape[0]
        ),
        name="attend",
    )(base, see, q, kv, qpos, qfirst, off)


def attend_back_kernel(
    dims, scale, base_ref, see_ref, q_ref, kv_ref, do_ref, o_ref, lse_ref, qpos_ref, qfirst_ref, off_ref, dq_ref, dkv_out, acc_ref, delta_ref, dkv_ref
):
    qh, kh, hd, stretch = dims
    group = qh // kh
    tile = pl.program_id(0)
    last = pl.num_programs(0) - 1

    @pl.when(tile == 0)
    def _():
        acc_ref[...] = jnp.zeros_like(acc_ref)
        for h in range(qh):
            at = slice(h * hd, (h + 1) * hd)
            delta_ref[h] = jnp.sum(do_ref[:, at].astype(F32) * o_ref[:, at].astype(F32), axis=-1, keepdims=True)

    sees = [see_ref[0, tile] > 0, see_ref[1, tile] > 0]

    @pl.when(jnp.logical_not(sees[0]))
    def _():
        dkv_ref[...] = jnp.zeros_like(dkv_ref)

    def half(e, add):
        q0 = e * stretch
        mask = tile_masks(base_ref, tile, qpos_ref, qfirst_ref, off_ref, q0, stretch)
        for c in range(kh):
            k = kv_ref[:, c * hd : (c + 1) * hd]
            v = kv_ref[:, (kh + c) * hd : (kh + c + 1) * hd]
            dk = dv = None
            for h in range(c * group, (c + 1) * group):
                at = slice(h * hd, (h + 1) * hd)
                q = q_ref[q0 : q0 + stretch, at]
                do = do_ref[q0 : q0 + stretch, at]
                s = dot(q, k, NT) * scale
                p = jnp.where(mask, jnp.exp(s - lse_ref[h, q0 : q0 + stretch, :]), 0.0)
                dp = dot(do, v, NT)
                ds = (p * (dp - delta_ref[h, q0 : q0 + stretch, :])).astype(BF16)
                acc_ref[q0 : q0 + stretch, at] += dot(ds, k, NN)
                dk_h = dot(ds, q, TN)
                dv_h = dot(p.astype(BF16), do, TN)
                dk = dk_h if dk is None else dk + dk_h
                dv = dv_h if dv is None else dv + dv_h
            ck = slice(c * hd, (c + 1) * hd)
            cv = slice((kh + c) * hd, (kh + c + 1) * hd)
            if add:
                dkv_ref[:, ck] += dk * scale
                dkv_ref[:, cv] += dv
            else:
                dkv_ref[:, ck] = dk * scale
                dkv_ref[:, cv] = dv

    for e in range(2):

        @pl.when(sees[e])
        def _():
            half(e, e == 1)

    dkv_out[...] = dkv_ref[...].astype(BF16)

    @pl.when(tile == last)
    def _():
        dq_ref[...] = (acc_ref[...] * scale).astype(BF16)


def attend_back(base, see, q, kv, do, o, lse, qpos, qfirst, off, qh, kh, hd, scale):
    t = q.shape[0]
    stretch = t // 2
    tiles = kv.shape[0] // stretch

    def whole(shape):
        return pl.BlockSpec(shape, lambda i, *_: (0,) * len(shape))

    tile_spec = pl.BlockSpec((stretch, 2 * kh * hd), lambda i, *_: (i, 0))
    return pl.pallas_call(
        partial(attend_back_kernel, (qh, kh, hd, stretch), scale),
        grid_spec=pltpu.PrefetchScalarGridSpec(
            num_scalar_prefetch=2,
            grid=(tiles,),
            in_specs=[
                whole((t, qh * hd)),
                tile_spec,
                whole((t, qh * hd)),
                whole((t, qh * hd)),
                whole((qh, t, 1)),
                whole((t, 1)),
                whole((t, 1)),
                whole((1, stretch)),
            ],
            out_specs=[whole((t, qh * hd)), tile_spec],
            scratch_shapes=[
                pltpu.VMEM((t, qh * hd), F32),
                pltpu.VMEM((qh, t, 1), F32),
                pltpu.VMEM((stretch, 2 * kh * hd), F32),
            ],
        ),
        out_shape=[
            jax.ShapeDtypeStruct((t, qh * hd), BF16),
            jax.ShapeDtypeStruct((kv.shape[0], 2 * kh * hd), BF16),
        ],
        cost_estimate=pl.CostEstimate(
            flops=10 * t * kv.shape[0] * hd * qh, bytes_accessed=6 * kv.size, transcendentals=t * kv.shape[0]
        ),
        name="attend_back",
    )(base, see, q, kv, do, o, lse, qpos, qfirst, off)


def after(value, *others):
    return lax.optimization_barrier((value,) + others)[0]


def shards(
    n,
    layer_input,
    w_query,
    w_key,
    w_value,
    w_output,
    w_gate,
    w_up,
    w_down,
    norm_attn,
    norm_mlp,
    norm_query,
    norm_key,
    out_grad,
    doc_lengths,
    stretch_order,
):
    t, d = layer_input.shape
    hd = norm_query.shape[0]
    qh, kh = w_query.shape[1] // hd, w_key.shape[1] // hd
    stretch = t // 2
    quarter = t // 4
    width = d // n
    ny = n // NZ
    scale = hd ** (-0.5)
    blk, tp = lax.axis_index("blk"), lax.axis_index("tp")
    z, y = blk // ny, blk % ny

    order = ring_order(n)
    place = jnp.array([order.index(b) for b in range(n)], jnp.int32)
    me = lax.dynamic_index_in_dim(place, blk, keepdims=False)
    cols = jnp.take(jnp.array(order + order, jnp.int32), me + jnp.arange(n, dtype=jnp.int32))
    planes = (z + jnp.arange(NZ, dtype=jnp.int32)) % NZ

    gain_attn = norm_attn.astype(F32)[:, None]
    gain_mlp = norm_mlp.astype(F32)[:, None]

    starts = jnp.cumsum(doc_lengths) - doc_lengths

    def first_of(pos):
        return jnp.max(jnp.where(starts[None, :] <= pos[:, None], starts[None, :], 0), axis=1)

    inside = jnp.arange(stretch, dtype=jnp.int32)
    base = stretch_order * stretch
    base_own = lax.dynamic_slice_in_dim(base, 2 * blk, 2, 0)
    positions = (base_own[:, None] + inside[None, :]).reshape(-1)
    firsts = first_of(positions)
    base_first = first_of(base_own)
    see = ((base[None, :] <= base_own[:, None]) & (base[None, :] + (stretch - 1) >= base_first[:, None])).astype(jnp.int32)
    inverse = ROPE_BASE ** (-2.0 * jnp.arange(hd // 2, dtype=F32) / hd)
    angles = (positions - firsts).astype(F32)[:, None] * inverse[None, :]
    cosine, sine = jnp.cos(angles), jnp.sin(angles)
    cosine = jnp.concatenate([cosine, cosine], axis=1)
    sine = jnp.concatenate([-sine, sine], axis=1)
    qpos, qfirst, off = positions[:, None], firsts[:, None], inside[None, :]
    gains = jnp.stack([norm_query.astype(F32)[None, :], norm_key.astype(F32)[None, :]])

    raw_q, raw_k, q, kv, unit_attn, full_qkv, full_out, *packed = head(
        n, layer_input, w_query, w_key, w_value, gain_attn, w_output, w_gate, w_up, w_down, gain_mlp, cosine, sine, gains
    )
    x_low = lax.dynamic_slice_in_dim(layer_input, tp * quarter, quarter, 0)
    g_low = lax.dynamic_slice_in_dim(out_grad, tp * quarter, quarter, 0)
    g_one, g_two = z_swap(after(g_low, q), n, 1), z_swap(after(g_low, q), n, 2)
    attn_low, lse = attend(base, see, q, kv, qpos, qfirst, off, qh, kh, hd, scale)

    hidden, grad_hidden, grad_heads, hidden_low, grads, y_grads, acts, w_mlp = feed(
        n, attn_low, full_out, x_low.astype(F32), out_grad, g_one, g_two, packed
    )

    w3 = grads.shape[1]

    def line(value):
        return lax.dynamic_index_in_dim(value.reshape(NZ, ny, width, w3), y, 1, keepdims=False)

    owned = line(grads).astype(F32) + jnp.sum(y_grads.reshape(ny - 1, NZ, width, w3).astype(F32), axis=0)
    pair = 2 * w3 // 3
    norm_mlp_terms = jnp.sum(owned[:, :, :pair] * line(w_mlp)[:, :, :pair].astype(F32), axis=2, keepdims=True)
    norm_mlp_terms = jnp.broadcast_to(norm_mlp_terms, (NZ, width, hd))
    owned = owned.astype(BF16)
    pieces = [lax.dynamic_index_in_dim(owned, (z - s) % NZ, 0, keepdims=False) for s in range(NZ)]
    pieces = pieces[:1] + [z_shift(pieces[s], n, -s) for s in range(1, NZ)]

    dq, dkv = attend_back(base, see, q, kv, grad_heads, attn_low, lse, qpos, qfirst, off, qh, kh, hd, scale)
    ringed = n <= 8
    if not ringed:
        dkv = [lax.dynamic_slice_in_dim(dkv, cols[r] * t, t, 0).astype(F32) for r in range(n)]
        dkv = ring_scatter(lambda r: dkv[r], n, t)
    layer_output, input_grad, grad_q, grad_k, grad_v, grad_out_w, small = tail(
        n, ringed, dq, dkv, raw_q, raw_k, cosine, sine, gains, unit_attn, full_qkv, hidden_low, attn_low, grad_hidden,
        x_low, hidden, acts, w_mlp[:, pair:], w_query, w_key, w_value, gain_attn, norm_mlp_terms,
    )
    pieces = [after(piece, small) for piece in pieces]
    grad_gate, grad_up, grad_down = finish(planes, pieces, gain_mlp)
    heads = small[2 * width :, :]
    part = hd // n
    return (
        layer_output,
        input_grad,
        grad_q,
        grad_k,
        grad_v,
        grad_out_w,
        grad_gate,
        grad_up,
        grad_down,
        small[:width, 0],
        small[width : 2 * width, 0] / gain_mlp[:, 0],
        lax.dynamic_slice(heads, (0, blk * part), (1, part))[0],
        lax.dynamic_slice(heads, (1, blk * part), (1, part))[0],
    )


def solution(mesh):
    return jax.shard_map(
        partial(shards, mesh.shape["blk"]),
        mesh=mesh,
        in_specs=(
            P("blk", None),
            P("blk", "tp"),
            P("blk", "tp"),
            P("blk", "tp"),
            P("tp", "blk"),
            P("blk", "tp"),
            P("blk", "tp"),
            P("tp", "blk"),
            P("blk"),
            P("blk"),
            P(),
            P(),
            P("blk", None),
            P(),
            P(),
        ),
        out_specs=(
            P("blk", None),
            P("blk", None),
            P("blk", "tp"),
            P("blk", "tp"),
            P("blk", "tp"),
            P("tp", "blk"),
            P("blk", "tp"),
            P("blk", "tp"),
            P("tp", "blk"),
            P("blk"),
            P("blk"),
            P("blk"),
            P("blk"),
        ),
        check_vma=False,
    )
```

```python
from functools import partial

import jax
import jax.numpy as jnp
from jax import lax
from jax.experimental import pallas as pl
from jax.experimental.pallas import tpu as pltpu
from jax.sharding import PartitionSpec as P

EPS = 1e-06
ROPE_BASE = 1000000.0
F32 = jnp.float32
BF16 = jnp.bfloat16


def dot(a, b, dims, out=F32):
    return lax.dot_general(a, b, (dims, ((), ())), preferred_element_type=out)


NN = ((1,), (0,))
NT = ((1,), (1,))
TN = ((0,), (0,))


def ring_order(n):
    return list(range(0, n, 2)) + list(range(n - 1, 0, -2))


def ring_perms(n):
    order = ring_order(n)
    right = [(order[i], order[(i + 1) % n]) for i in range(n)]
    return right, [(b, a) for a, b in right]


def ring_scatter(part, n, rows):
    right, left = ring_perms(n)
    half = n // 2
    cut = rows // 2
    far = part(half).astype(BF16)
    to_right = lax.ppermute(far[:cut], "blk", right).astype(F32)
    to_left = lax.ppermute(far[cut:], "blk", left).astype(F32)
    if half == 1:
        return part(0) + jnp.concatenate([to_right, to_left], axis=0)
    for k in range(half - 1, 0, -1):
        send_right, send_left = part(k), part(n - k)
        if k == half - 1:
            send_right = jnp.concatenate([send_right[:cut] + to_right, send_right[cut:]], axis=0)
            send_left = jnp.concatenate([send_left[:cut], send_left[cut:] + to_left], axis=0)
        else:
            send_right = send_right + to_right
            send_left = send_left + to_left
        to_right = lax.ppermute(send_right.astype(BF16), "blk", right).astype(F32)
        to_left = lax.ppermute(send_left.astype(BF16), "blk", left).astype(F32)
    return part(0) + to_right + to_left


NZ = 4


def z_swap(value, n, k):
    ny = n // NZ
    pairs = [(z * ny + y, (z ^ k) * ny + y) for z in range(NZ) for y in range(ny)]
    return lax.ppermute(value, "blk", pairs)


VMEM = pl.BlockSpec(memory_space=pltpu.VMEM)
SMEM = pl.BlockSpec(memory_space=pltpu.SMEM)
HBM = pl.BlockSpec(memory_space=pl.ANY)


def finish_kernel(zs_ref, *refs):
    pieces = refs[:NZ]
    gain_ref, d_gate, d_up, d_down = refs[NZ:]
    part = d_gate.shape[1] // NZ
    gain = gain_ref[...]
    for s in range(NZ):
        at = pl.ds(pl.multiple_of(zs_ref[s] * part, part), part)
        d_gate[:, at] = pieces[s][:, :part].astype(F32) * gain
        d_up[:, at] = pieces[s][:, part : 2 * part].astype(F32) * gain
        d_down[at, :] = pieces[s][:, 2 * part :].astype(F32).T


def finish(zs, pieces, gain):
    rows, cols = pieces[0].shape[0], NZ * pieces[0].shape[1] // 3
    return pl.pallas_call(
        finish_kernel,
        in_specs=[SMEM] + [VMEM] * (NZ + 1),
        out_specs=[VMEM] * 3,
        out_shape=[
            jax.ShapeDtypeStruct((rows, cols), F32),
            jax.ShapeDtypeStruct((rows, cols), F32),
            jax.ShapeDtypeStruct((cols, rows), F32),
        ],
        name="finish",
    )(zs, *pieces, gain)


MESH = pl.DeviceIdType.MESH


class Wires:
    def __init__(self, send, recv):
        self.send, self.recv, self.sent, self.done = send, recv, [], []

    def go(self, src, dst, device):
        i = len(self.sent)
        copy = pltpu.make_async_remote_copy(
            src_ref=src,
            dst_ref=dst,
            send_sem=self.send.at[i],
            recv_sem=self.recv.at[i],
            device_id=device,
            device_id_type=MESH,
        )
        copy.start()
        self.sent.append(copy)
        return copy

    def drain(self, copies):
        for copy in copies:
            copy.wait_send()
            self.done.append(copy)

    def close(self):
        self.drain([copy for copy in self.sent if not any(copy is other for other in self.done)])


def greet(devices):
    barrier = pltpu.get_barrier_semaphore()
    for device in devices:
        pl.semaphore_signal(barrier, inc=1, device_id=device, device_id_type=MESH)
    pl.semaphore_wait(barrier, len(devices))


class Spot:
    def __init__(self, n):
        self.n, self.ny = n, n // NZ
        self.blk, self.tp = lax.axis_index("blk"), lax.axis_index("tp")
        self.z, self.y = self.blk // self.ny, self.blk % self.ny
        self.x, self.core = self.tp // 2, self.tp % 2
        self.tp_core = self.x * 2 + (1 - self.core)
        self.tp_far = (1 - self.x) * 2 + self.core
        self.core_dev = {"tp": self.tp_core}
        self.far_dev = {"tp": self.tp_far}
        self.place = jnp.where(self.blk % 2 == 0, self.blk // 2, n - 1 - self.blk // 2)
        self.right_dev = {"blk": self.at_place(1)}
        self.left_dev = {"blk": self.at_place(n - 1)}

    def at_place(self, r):
        p = (self.place + r) % self.n
        return jnp.where(p < self.n // 2, 2 * p, 2 * (self.n - 1 - p) + 1)

    def plane(self, s):
        return (self.z + s) % NZ

    def z_dev(self, s):
        return {"blk": self.plane(s) * self.ny + self.y}

    def plane_x(self, k):
        return (self.z + 1 - 2 * (self.z % 2), (self.z + 2) % NZ, NZ - 1 - self.z)[k - 1]

    def x_dev(self, k):
        return {"blk": self.plane_x(k) * self.ny + self.y}

    def y_dev(self, j):
        return {"blk": self.z * self.ny + (self.y + j) % self.ny}

    def peers(self):
        return (
            [self.core_dev, self.far_dev]
            + [self.z_dev(s) for s in range(1, NZ)]
            + [self.y_dev(j) for j in range(1, self.ny)]
        )


def rows_at(index, count):
    return pl.ds(pl.multiple_of(index * count, count), count)


def feed_copies(n):
    return 64 + 8 * (n // NZ - 1)


def feed_kernel(n, attn, wo, x_own, g_rows, g_one, g_two, *refs):
    packed = refs[:NZ]
    hidden_o, gh_o, heads_o, hl_o, dw_o, y_o, act_o, w_o, own_o, norm_o, *owned = refs[NZ : NZ + 13]
    (u_all, g_all, dgu, o_part, o_core, o_x, part, near, core_in, x_in, z_in, dw_tile, dw_sum, dw_in, send, recv, dw_sem, in_sem) = refs[NZ + 13 :]
    q, d = x_own.shape
    p = packed[0].shape[1] // 3
    bw = packed[0].shape[0]
    me = Spot(n)
    wires = Wires(send, recv)
    greet(me.peers())

    def quarter(plane, peer):
        return rows_at(plane * 4 + peer, q)

    def pass_on(buf, plane, src=None):
        at = quarter(plane, me.tp)
        src = buf.at[at] if src is None else src
        return wires.go(src, buf.at[at], me.far_dev), wires.go(src, buf.at[at], me.core_dev)

    def pass_far(buf, plane, copies):
        copies[0].wait_recv()
        at = quarter(plane, me.tp_far)
        return copies[1], wires.go(buf.at[at], buf.at[at], me.core_dev)

    def arrived(copies):
        for copy in copies:
            copy.wait_recv()

    mine = rows_at(me.blk, bw)
    two = rows_at(me.plane(2) * me.ny + me.y, bw)
    w_z = {1: wires.go(packed[1], w_o.at[mine], me.z_dev(1)), 3: wires.go(packed[2], w_o.at[mine], me.z_dev(3))}
    near_plane, over_plane, last_plane = me.plane_x(1), me.plane_x(2), me.plane_x(3)
    near_dev, over_dev = me.x_dev(1), me.x_dev(2)
    g_three = wires.go(g_two, g_all.at[quarter(over_plane, me.tp)], near_dev)
    g_one_pass = pass_on(g_all, near_plane, g_one)
    w_y = [wires.go(packed[0], w_o.at[mine], me.y_dev(j)) for j in range(1, me.ny)]
    w_y += [wires.go(packed[3], w_o.at[two], me.y_dev(j)) for j in range(1, me.ny)]

    def project(peer):
        return dot(attn[rows_at(peer, q), :], wo[...], NT)

    for i, x in enumerate((1 - me.x, me.x)):
        o_part[i] = project(x * 2 + 1 - me.core).astype(BF16)
    far_in = wires.go(o_part.at[0], o_core.at[0], me.core_dev)
    near_in = wires.go(o_part.at[1], o_core.at[1], me.core_dev)
    own_far = project(me.tp_far)
    far_in.wait_recv()
    o_core[0] = (own_far + o_core[0].astype(F32)).astype(BF16)
    x_sum = wires.go(o_core.at[0], o_x, me.far_dev)
    own_sum = project(me.tp) + x_own[...]
    w_o[mine, :] = packed[0][...]
    w_o[two, :] = packed[3][...]
    g_all[rows_at(me.z, 4 * q), :] = g_rows[...]
    g_all[quarter(near_plane, me.tp), :] = g_one[...]
    g_all[quarter(over_plane, me.tp), :] = g_two[...]
    near_in.wait_recv()
    own_sum = own_sum + o_core[1].astype(F32)
    x_sum.wait_recv()
    hidden = own_sum + o_x[...].astype(F32)
    hidden_o[...] = hidden
    rs = lax.rsqrt(jnp.mean(hidden * hidden, axis=-1, keepdims=True) + EPS)
    own_q = quarter(me.z, me.tp)
    u_all[own_q, :] = (hidden * rs).astype(BF16)

    own_pass = pass_on(u_all, me.z)
    u_one = wires.go(u_all.at[own_q], u_all.at[own_q], near_dev)
    u_two = wires.go(u_all.at[own_q], u_all.at[own_q], over_dev)
    g_one_pass = pass_far(g_all, near_plane, g_one_pass)
    g_two_pass = pass_on(g_all, over_plane, g_two)
    for s in (1, 3):
        w_z[s].wait_recv()
        at = rows_at(me.plane(-s) * me.ny + me.y, bw)
        w_y += [wires.go(w_o.at[at], w_o.at[at], me.y_dev(j)) for j in range(1, me.ny)]
    own_pass = pass_far(u_all, me.z, own_pass)
    arrived(w_y)
    arrived(own_pass)

    def compute(i, plane):
        @pl.loop(0, 2)
        def _(k):
            at = pl.ds(pl.multiple_of(plane * (4 * q) + k * (2 * q), 2 * q), 2 * q)
            gate_up = dot(u_all[at, :], w_o[:, : 2 * p], NN)
            grad_act = dot(g_all[at, :], w_o[:, 2 * p :], NN)
            gate, up = gate_up[:, :p], gate_up[:, p:]
            sig = 1.0 / (1.0 + jnp.exp(-gate))
            silu = gate * sig
            act_o[at, :] = (silu * up).astype(BF16)
            dgu[at, p:] = (grad_act * silu).astype(BF16)
            dgu[at, :p] = (grad_act * up * (sig * (1.0 + gate * (1.0 - sig)))).astype(BF16)

        rows = rows_at(plane, 4 * q)
        tile = 512

        @pl.loop(0, d // tile)
        def _(c):
            at = pl.ds(pl.multiple_of(c * tile, tile), tile)
            part[i % 2, :, at] = dot(dgu[rows, :], w_o[at, : 2 * p], NT).astype(BF16)

    cores, fars = {}, {}

    def reduce_core(i):
        cores[i] = []
        for k, x in enumerate((1 - me.x, me.x)):
            src = part.at[i % 2, rows_at(x * 2 + 1 - me.core, q)]
            cores[i].append(wires.go(src, core_in.at[i, k], me.core_dev))

    def reduce_prep(i):
        for k, peer in enumerate((me.tp_far, me.tp)):
            cores[i][k].wait_recv()
            core_in[i, k] = (part[i % 2, rows_at(peer, q), :].astype(F32) + core_in[i, k].astype(F32)).astype(BF16)
        wires.drain(cores[i])

    def reduce_far(i):
        fars[i] = wires.go(core_in.at[i, 0], x_in.at[i], me.far_dev)

    def reduce_near(i):
        fars[i].wait_recv()
        return core_in[i, 1].astype(F32) + x_in[i].astype(F32)

    tiles = d // (256 * NZ)

    def planes(k):
        return me.plane_x(k) if k else me.z

    def dw_copy(plane, c):
        rows = rows_at(plane * tiles + c, 256)
        return pltpu.make_async_copy(dw_tile.at[c % 2], dw_o.at[rows], dw_sem.at[c % 2])

    y_copies = {}

    def grads(k):
        plane = planes(k)

        @pl.loop(0, tiles)
        def _(c):
            @pl.when(c >= 2)
            def _():
                dw_copy(plane, c - 2).wait()

            at = rows_at(plane * tiles + c, 256)
            dw_tile[c % 2, :, : 2 * p] = dot(u_all[:, at], dgu[...], TN).astype(BF16)
            dw_tile[c % 2, :, 2 * p :] = dot(g_all[:, at], act_o[...], TN).astype(BF16)
            dw_copy(plane, c).start()

        for c in range(max(0, tiles - 2), tiles):
            dw_copy(plane, c).wait()
        y_copies[k] = [
            wires.go(dw_o.at[rows_at(plane * me.ny + (me.y + j) % me.ny, bw)], y_o.at[(j - 1) * NZ + k], me.y_dev(j))
            for j in range(1, me.ny)
        ]

    z_copies = []

    def to_owner(k):
        plane = planes(k)
        at = rows_at(plane * me.ny + me.y, bw)
        loads = [pltpu.make_async_copy(dw_o.at[at], dw_in.at[0], in_sem.at[0])]
        loads[0].start()
        for j in range(1, me.ny):
            y_copies[k][j - 1].wait_recv()
            loads.append(pltpu.make_async_copy(y_o.at[(j - 1) * NZ + k], dw_in.at[j], in_sem.at[j]))
            loads[j].start()
        total = None
        for j, load in enumerate(loads):
            load.wait()
            term = dw_in[j].astype(F32)
            total = term if total is None else total + term
        norm = jnp.sum(total[:, : 2 * p] * w_o[at, : 2 * p].astype(F32), axis=1, keepdims=True)
        norm_o[k] = jnp.broadcast_to(norm, norm_o.shape[1:])
        if k == 0:
            own_o[...] = total.astype(BF16)
        else:
            dw_sum[k - 1] = total.astype(BF16)
            z_copies.append(wires.go(dw_sum.at[k - 1], owned[k - 1], me.x_dev(k)))

    compute(0, me.z)
    reduce_core(0)
    u_one.wait_recv()
    u_one_pass = pass_on(u_all, near_plane)
    u_two.wait_recv()
    u_three = wires.go(u_all.at[quarter(over_plane, me.tp)], u_all.at[quarter(over_plane, me.tp)], near_dev)
    u_two_pass = pass_on(u_all, over_plane)
    reduce_prep(0)
    g_two_pass = pass_far(g_all, over_plane, g_two_pass)
    u_one_pass = pass_far(u_all, near_plane, u_one_pass)
    arrived(g_one_pass)
    arrived(u_one_pass)
    compute(1, near_plane)
    reduce_core(1)
    u_three.wait_recv()
    u_three_pass = pass_on(u_all, last_plane)
    g_three.wait_recv()
    g_three_pass = pass_on(g_all, last_plane)
    u_two_pass = pass_far(u_all, over_plane, u_two_pass)
    reduce_prep(1)
    arrived(g_two_pass)
    arrived(u_two_pass)
    compute(2, over_plane)
    reduce_core(2)
    u_three_pass = pass_far(u_all, last_plane, u_three_pass)
    reduce_prep(2)
    g_three_pass = pass_far(g_all, last_plane, g_three_pass)
    reduce_far(2)
    arrived(u_three_pass)
    arrived(g_three_pass)
    compute(3, last_plane)
    reduce_core(3)
    reduce_prep(3)
    reduce_far(3)
    grads(3)
    grads(2)
    near[1] = reduce_near(2).astype(BF16)
    near[2] = reduce_near(3).astype(BF16)
    z_three = wires.go(near.at[2], z_in.at[1], near_dev)
    reduce_far(1)
    reduce_far(0)
    grads(1)
    to_owner(3)
    z_three.wait_recv()
    near[1] = (near[1].astype(F32) + z_in[1].astype(F32)).astype(BF16)
    z_two = wires.go(near.at[1], z_in.at[2], over_dev)
    near[0] = reduce_near(1).astype(BF16)
    z_one = wires.go(near.at[0], z_in.at[0], near_dev)
    grads(0)
    m = reduce_near(0)
    z_one.wait_recv()
    m = m + z_in[0].astype(F32)
    z_two.wait_recv()
    m = m + z_in[2].astype(F32)

    hidden = hidden_o[...]
    rs = lax.rsqrt(jnp.mean(hidden * hidden, axis=-1, keepdims=True) + EPS)
    unit = hidden * rs
    grad = g_rows[rows_at(me.tp, q), :].astype(F32) + (m - unit * jnp.mean(m * unit, axis=-1, keepdims=True)) * rs
    gh_o[...] = grad
    own = rows_at(me.tp, q)
    hl_o[own, :] = grad.astype(BF16)
    x_copy = wires.go(hl_o.at[own], hl_o.at[own], me.far_dev)
    c_copy = wires.go(hl_o.at[own], hl_o.at[own], me.core_dev)

    def heads(peer):
        heads_o[rows_at(peer, q), :] = dot(hl_o[rows_at(peer, q), :], wo[...], NN).astype(BF16)

    to_owner(2)
    heads(me.tp)
    c_copy.wait_recv()
    heads(me.tp_core)
    x_copy.wait_recv()
    at = rows_at(me.tp_far, q)
    last = wires.go(hl_o.at[at], hl_o.at[at], me.core_dev)
    heads(me.tp_far)
    to_owner(1)
    last.wait_recv()
    heads((1 - me.x) * 2 + 1 - me.core)
    to_owner(0)
    arrived(z_copies)
    wires.close()


def feed(n, attn, wo, x_own, g_rows, g_one, g_two, packed):
    q, d = x_own.shape
    t, a = attn.shape
    bw, w3 = packed[0].shape
    p = w3 // 3
    tokens = NZ * t
    copies = feed_copies(n)
    vm = pltpu.VMEM
    return pl.pallas_call(
        partial(feed_kernel, n),
        in_specs=[VMEM] * (6 + NZ),
        out_specs=[VMEM] * 4 + [HBM] * 2 + [VMEM] * 4 + [HBM] * 3,
        out_shape=[
            jax.ShapeDtypeStruct((q, d), F32),
            jax.ShapeDtypeStruct((q, d), F32),
            jax.ShapeDtypeStruct((t, a), BF16),
            jax.ShapeDtypeStruct((t, d), BF16),
            jax.ShapeDtypeStruct((d, w3), BF16),
            jax.ShapeDtypeStruct((NZ * (n // NZ - 1), bw, w3), BF16),
            jax.ShapeDtypeStruct((tokens, p), BF16),
            jax.ShapeDtypeStruct((d, w3), BF16),
            jax.ShapeDtypeStruct((bw, w3), BF16),
            jax.ShapeDtypeStruct((NZ, bw, 128), F32),
        ]
        + [jax.ShapeDtypeStruct((bw, w3), BF16)] * 3,
        scratch_shapes=[
            vm((tokens, d), BF16),
            vm((tokens, d), BF16),
            vm((tokens, 2 * p), BF16),
            vm((2, q, d), BF16),
            vm((2, q, d), BF16),
            vm((q, d), BF16),
            vm((2, t, d), BF16),
            vm((NZ - 1, q, d), BF16),
            vm((NZ, 2, q, d), BF16),
            vm((NZ, q, d), BF16),
            vm((NZ - 1, q, d), BF16),
            vm((2, 256, w3), BF16),
            vm((3, bw, w3), BF16),
            vm((n // NZ, bw, w3), BF16),
            pltpu.SemaphoreType.DMA((copies,)),
            pltpu.SemaphoreType.DMA((copies,)),
            pltpu.SemaphoreType.DMA((2,)),
            pltpu.SemaphoreType.DMA((n // NZ,)),
        ],
        compiler_params=pltpu.CompilerParams(
            collective_id=1, has_side_effects=True, vmem_limit_bytes=67000000
        ),
        name="feed",
    )(attn, wo, x_own, g_rows, g_one, g_two, *packed)


class RingSum:
    def __init__(self, wires, me, land, stage, part):
        self.wires, self.me, self.land, self.stage, self.part = wires, me, land, stage, part
        self.half = me.n // 2
        self.cut = land.shape[2] // 2
        self.got = None

    def start(self):
        top, low, cut = pl.ds(0, self.cut), pl.ds(self.cut, self.cut), self.half - 1
        self.stage[...] = self.part(self.half).astype(BF16)
        self.got = (
            self.wires.go(self.stage.at[top], self.land.at[0, cut, top], self.me.right_dev),
            self.wires.go(self.stage.at[low], self.land.at[1, cut, low], self.me.left_dev),
        )
        self.first = self.got

    def step(self, k):
        cut = self.cut
        sent = []
        for side, place, dev in ((0, k, self.me.right_dev), (1, self.me.n - k, self.me.left_dev)):
            mine = self.part(place)
            self.got[side].wait_recv()
            if k == self.half - 1:
                keep, fresh = (slice(0, cut), slice(cut, None)) if side == 0 else (slice(cut, None), slice(0, cut))
                self.land[side, k, keep, :] = (self.land[side, k, keep, :].astype(F32) + mine[keep]).astype(BF16)
                self.land[side, k, fresh, :] = mine[fresh].astype(BF16)
            else:
                self.land[side, k] = (self.land[side, k].astype(F32) + mine).astype(BF16)
            sent.append(self.wires.go(self.land.at[side, k], self.land.at[side, k - 1], dev))
        self.got = tuple(sent)

    def total(self):
        mine = self.part(0)
        for copy in self.got:
            copy.wait_recv()
        return mine + self.land[0, 0].astype(F32) + self.land[1, 0].astype(F32)


def tail_copies(n):
    return 2 * 4 * (n // 2) + 16 + 3 + 3 + 3 + 3 + 3 + 2 + 8


def tail_kernel(n, ringed, scale, *refs):
    ins = 8 if ringed else 2
    (raw_q, raw_k, cos_ref, sin_ref, gain_ref, u1, wqkv, hl, attn, gh, x_own, hidden, act, w_mlp) = refs[ins : ins + 14]
    w_q, w_k, w_v, gain_attn, norm_in = refs[ins + 14 : ins + 19]
    lo, ig_low, gq_o, gk_o, gv_o, go_o, small_o = refs[ins + 19 : ins + 26]
    (d_qkv, gains, kv_land, kv_stage, o_land, o_stage, q_land, w_land, w_stage, m_part, m_core, m_x, part, core_in, x_in, z_in) = refs[ins + 26 : ins + 42]
    norm_land, small_core, small_x, o_whole, w_whole, w_down, dq_acc, kv_acc, delta, send, recv, load_sem = refs[ins + 42 :]
    q, d = hidden.shape
    t, qw = raw_q.shape
    hd = cos_ref.shape[1]
    kw = raw_k.shape[1]
    bw = w_q.shape[0]
    p = act.shape[1]
    load = pltpu.make_async_copy(w_mlp.at[:, pl.ds(2 * p, p)], w_down, load_sem)
    load.start()
    me = Spot(n)
    wires = Wires(send, recv)
    greet(me.peers() + [me.right_dev, me.left_dev])

    norm_copies = [
        wires.go(norm_in.at[k], norm_land.at[k - 1], me.x_dev(k)) for k in range(1, NZ)
    ]

    def head_back(src, raw, heads, kind, to):
        gains[kind] = jnp.zeros((1, hd), F32)

        @pl.loop(0, 4)
        def _(k):
            at = pl.ds(pl.multiple_of(k * q, q), q)
            cosine, sine = cos_ref[at, :], sin_ref[at, :]
            for h in range(heads):
                cols = slice(h * hd, (h + 1) * hd)
                grad = src[at, cols].astype(F32)
                grad = grad * cosine - turned(grad, sine)
                v = raw[at, cols].astype(F32)
                rs = lax.rsqrt(jnp.mean(v * v, axis=-1, keepdims=True) + EPS)
                unit = v * rs
                gains[kind] += jnp.sum(grad * unit, axis=0, keepdims=True)
                m = grad * gain_ref[kind]
                back = (m - unit * jnp.mean(m * unit, axis=-1, keepdims=True)) * rs
                d_qkv[at, to + h * hd : to + (h + 1) * hd] = back.astype(BF16)

    slots = (3, 1, 2, 0)
    cores, fars, backs = {}, {}, {}

    def slot_plane(i):
        return me.plane_x(slots[i]) if slots[i] else me.z

    def down(i):
        rows = rows_at(slot_plane(i), 4 * q)
        tile = 512

        @pl.loop(0, d // tile)
        def _(c):
            at = pl.ds(pl.multiple_of(c * tile, tile), tile)
            part[i % 2, :, at] = dot(act[rows, :], w_down[at, :], NT).astype(BF16)

        cores[i] = [
            wires.go(part.at[i % 2, rows_at(x * 2 + 1 - me.core, q)], core_in.at[i, k], me.core_dev)
            for k, x in enumerate((1 - me.x, me.x))
        ]

    def down_far(i):
        cores[i][0].wait_recv()
        core_in[i, 0] = (part[i % 2, rows_at(me.tp_far, q), :].astype(F32) + core_in[i, 0].astype(F32)).astype(BF16)
        fars[i] = wires.go(core_in.at[i, 0], x_in.at[i], me.far_dev)

    def down_near(i):
        cores[i][1].wait_recv()
        fars[i].wait_recv()
        value = part[i % 2, rows_at(me.tp, q), :].astype(F32) + core_in[i, 1].astype(F32) + x_in[i].astype(F32)
        wires.drain(cores[i])
        if slots[i] == 0:
            return value
        if slots[i] == 2:
            backs[0].wait_recv()
            value = value + z_in[0].astype(F32)
        x_in[i] = value.astype(BF16)
        backs[i] = wires.go(x_in.at[i], z_in.at[i], me.x_dev(2 if slots[i] == 2 else 1))

    def term(left, right, whole):
        if bw % 128 == 0:
            return lambda r: dot(left[:, rows_at(me.at_place(r), bw)], right[...], TN)

        @pl.loop(0, d // 256)
        def _(c):
            at = rows_at(c, 256)
            whole[at, :] = dot(left[:, at], right[...], TN).astype(BF16)

        return lambda r: whole[rows_at(me.at_place(r), bw), :].astype(F32)

    o_part = term(hl, attn, o_whole)

    o_ring = RingSum(wires, me, o_land, o_stage, o_part)

    half = n // 2
    if ringed:
        base_ref, off_ref, qpos_ref, qfirst_ref, q_ref, kv_ref, do_ref, lse_ref = refs[:8]
        stretch, kh = t // 2, kw // hd
        group = qw // kw
        dq = dq_acc
        dq_acc[...] = jnp.zeros_like(dq_acc)
        for h in range(qw // hd):
            cols = slice(h * hd, (h + 1) * hd)
            delta[:, h : h + 1] = jnp.sum(do_ref[:, cols].astype(F32) * attn[:, cols].astype(F32), axis=-1, keepdims=True)

        def kv_terms(r):
            block = me.at_place(r)
            @pl.loop(0, 2)
            def _(e):
                keys = rows_at(2 * block + e, stretch)
                to = rows_at(e, stretch)
                kpos = off_ref[...] + base_ref[2 * block + e]
                mask = (kpos <= qpos_ref[...]) & (kpos >= qfirst_ref[...])
                for c in range(kh):
                    ck = slice(c * hd, (c + 1) * hd)
                    cv = slice((kh + c) * hd, (kh + c + 1) * hd)
                    k, v = kv_ref[keys, ck], kv_ref[keys, cv]
                    dk = dv = None
                    for h in range(c * group, (c + 1) * group):
                        cols = slice(h * hd, (h + 1) * hd)
                        qh, do = q_ref[:, cols], do_ref[:, cols]
                        prob = jnp.where(mask, jnp.exp(dot(qh, k, NT) * scale - lse_ref[:, h : h + 1]), 0.0)
                        ds = (prob * (dot(do, v, NT) - delta[:, h : h + 1])).astype(BF16)
                        dq_acc[:, cols] += dot(ds, k, NN)
                        dk_h, dv_h = dot(ds, qh, TN), dot(prob.astype(BF16), do, TN)
                        dk = dk_h if dk is None else dk + dk_h
                        dv = dv_h if dv is None else dv + dv_h
                    kv_acc[to, ck] = dk * scale
                    kv_acc[to, cv] = dv

            return kv_acc[...]

        kv_ring = RingSum(wires, me, kv_land, kv_stage, kv_terms)
        kv_ring.start()
    else:
        dq, dkv = refs[:2]
    load.wait()
    fill = [
        lambda: (o_ring.start(), down(0)),
        lambda: (down_far(0), down(1)),
        lambda: (down_near(0), down_far(1), down(2)),
        lambda: (down_near(1), down_far(2), down(3)),
    ]
    for k in range(half - 1, 0, -1):
        if ringed:
            kv_ring.step(k)
        if fill:
            fill.pop(0)()
        if k < half - 1:
            o_ring.step(k + 1)
    for job in fill:
        job()
    if half > 1:
        o_ring.step(1)
    if ringed:
        kv_total = kv_ring.total().astype(BF16)
        wires.drain(kv_ring.first)
        kv_stage[...] = kv_total
        kv_sum = kv_stage
        dq_acc[...] = dq_acc[...] * scale
    else:
        kv_sum = dkv
    head_back(dq, raw_q, qw // hd, 0, 0)
    head_back(kv_sum, raw_k, kw // hd, 1, qw)
    d_qkv[:, qw + kw :] = kv_sum[:, kw:].astype(BF16)

    def m_term(peer):
        return dot(d_qkv[rows_at(peer, q), :], wqkv[...], NT)

    q_cols, kv_cols = pl.ds(0, qw), pl.ds(qw, 2 * kw)
    split = bw % 128 != 0
    q_term = term(u1, d_qkv.at[:, q_cols], w_whole.at[:, q_cols] if split else None)
    kv_w_term = term(u1, d_qkv.at[:, kv_cols], w_whole.at[:, kv_cols] if split else None)

    def kv_part(r):
        body = kv_w_term(r)
        extra = w_land.shape[2] - bw
        rest = jnp.concatenate([gains[0], gains[1], jnp.zeros((extra - 2, hd), F32)], axis=0)
        rest = jnp.concatenate([rest, jnp.zeros((extra, body.shape[1] - hd), F32)], axis=1)
        return jnp.concatenate([body, rest], axis=0)

    rings = (RingSum(wires, me, q_land, o_stage, q_term), RingSum(wires, me, w_land, w_stage, kv_part))
    for i, x in enumerate((1 - me.x, me.x)):
        m_part[i] = m_term(x * 2 + 1 - me.core).astype(BF16)
    m_far = wires.go(m_part.at[0], m_core.at[0], me.core_dev)
    m_near = wires.go(m_part.at[1], m_core.at[1], me.core_dev)
    wires.drain(o_ring.first)
    for ring in rings:
        ring.start()
    own_far = m_term(me.tp_far)
    m_far.wait_recv()
    m_core[0] = (own_far + m_core[0].astype(F32)).astype(BF16)
    m_sum = wires.go(m_core.at[0], m_x, me.far_dev)
    own = m_term(me.tp)
    m_near.wait_recv()
    own = own + m_core[1].astype(F32)
    steps = list(range(half - 1, 0, -1))

    def tick():
        k = steps.pop(0)
        for ring in rings:
            ring.step(k)

    if steps:
        tick()
    m_sum.wait_recv()
    m = own + m_x[...].astype(F32)
    x = x_own[...].astype(F32)
    rs = lax.rsqrt(jnp.mean(x * x, axis=-1, keepdims=True) + EPS)
    unit = x * rs
    grad = gh[...] + (m - unit * jnp.mean(m * unit, axis=-1, keepdims=True)) * rs
    mine = rows_at(me.tp, q)
    ig_low[mine, :] = grad.astype(BF16)

    def spread(buf):
        far = wires.go(buf.at[mine], buf.at[mine], me.far_dev)
        core = wires.go(buf.at[mine], buf.at[mine], me.core_dev)
        return far, core

    def spread_far(buf, copies):
        copies[0].wait_recv()
        at = rows_at(me.tp_far, q)
        return wires.go(buf.at[at], buf.at[at], me.core_dev)

    ig_copies = spread(ig_low)
    if steps:
        tick()

    down_near(2)
    down_far(3)
    out = hidden[...] + down_near(3)
    for i in (1, 2):
        backs[i].wait_recv()
        out = out + z_in[i].astype(F32)
    lo[mine, :] = out.astype(BF16)
    lo_copies = spread(lo)
    ig_last = spread_far(ig_low, ig_copies)
    while steps:
        tick()
    go_o[...] = o_ring.total().T

    lo_last = spread_far(lo, lo_copies)
    ig_copies[1].wait_recv()
    ig_last.wait_recv()
    grad_q = rings[0].total()
    total = rings[1].total()
    grad = total[:bw]
    gain = gain_attn[...]
    norm = jnp.sum(grad_q * w_q[...].astype(F32), axis=1, keepdims=True)
    norm = norm + jnp.sum(grad[:, :kw] * w_k[...].astype(F32), axis=1, keepdims=True)
    norm = norm + jnp.sum(grad[:, kw:] * w_v[...].astype(F32), axis=1, keepdims=True)
    small_o[:bw, :] = jnp.broadcast_to(norm, (bw, hd))
    mlp = norm_in[0]
    for s in range(1, NZ):
        norm_copies[s - 1].wait_recv()
        mlp = mlp + norm_land[s - 1]
    small_o[bw : 2 * bw, :] = mlp
    small_o[2 * bw :, :] = total[bw : bw + 16, :hd]
    copy = wires.go(small_o, small_core, me.core_dev)
    gq_o[...] = grad_q * gain
    gk_o[...] = grad[:, :kw] * gain
    gv_o[...] = grad[:, kw:] * gain
    copy.wait_recv()
    small_core[...] += small_o[...]
    copy = wires.go(small_core, small_x, me.far_dev)
    lo_copies[1].wait_recv()
    lo_last.wait_recv()
    copy.wait_recv()
    wires.close()
    small_o[...] = small_core[...] + small_x[...]


def tail(n, scale, attention, raw_q, raw_k, cosine, sine, gains, u1, wqkv, hl, attn, gh, x_own, hidden, act, w_mlp, w_q, w_k, w_v, gain_attn, norm_in):
    ringed = len(attention) > 2
    q, d = hidden.shape
    t, qw = raw_q.shape
    hd = cosine.shape[1]
    kw = raw_k.shape[1]
    wide = qw + 2 * kw
    bw = d // n
    p = act.shape[1]
    half = n // 2
    copies = tail_copies(n)
    vm = pltpu.VMEM
    small = 2 * bw + 16
    shape = jax.ShapeDtypeStruct
    none = (16, 128)
    return pl.pallas_call(
        partial(tail_kernel, n, ringed, scale),
        in_specs=([SMEM] + [VMEM] * 7 if ringed else [VMEM] * 2) + [VMEM] * 13 + [HBM] + [VMEM] * 5,
        out_specs=[VMEM] * 7,
        out_shape=[
            shape((t, d), BF16),
            shape((t, d), BF16),
            shape((bw, qw), F32),
            shape((bw, kw), F32),
            shape((bw, kw), F32),
            shape((attn.shape[1], bw), F32),
            shape((small, hd), F32),
        ],
        scratch_shapes=[
            vm((t, wide), BF16),
            vm((2, 1, hd), F32),
            vm((2, half, t, 2 * kw) if ringed else (2, 1) + none, BF16),
            vm((t, 2 * kw) if ringed else none, BF16),
            vm((2, half, bw, attn.shape[1]), BF16),
            vm((bw, attn.shape[1]), BF16),
            vm((2, half, bw, qw), BF16),
            vm((2, half, bw + 32, 2 * kw), BF16),
            vm((bw + 32, 2 * kw), BF16),
            vm((2, q, d), BF16),
            vm((2, q, d), BF16),
            vm((q, d), BF16),
            vm((2, t, d), BF16),
            vm((NZ, 2, q, d), BF16),
            vm((NZ, q, d), BF16),
            vm((NZ - 1, q, d), BF16),
            vm((NZ - 1, bw, hd), F32),
            vm((small, hd), F32),
            vm((small, hd), F32),
            vm((d, attn.shape[1]) if bw % 128 else none, BF16),
            vm((d, wide) if bw % 128 else none, BF16),
            vm((d, p), BF16),
            vm((t, qw) if ringed else none, F32),
            vm((t, 2 * kw) if ringed else none, F32),
            vm((t, qw // hd) if ringed else none, F32),
            pltpu.SemaphoreType.DMA((copies,)),
            pltpu.SemaphoreType.DMA((copies,)),
            pltpu.SemaphoreType.DMA,
        ],
        compiler_params=pltpu.CompilerParams(
            collective_id=2, has_side_effects=True, vmem_limit_bytes=67000000
        ),
        name="tail",
    )(*attention, raw_q, raw_k, cosine, sine, gains, u1, wqkv, hl, attn, gh, x_own, hidden, act, w_mlp, w_q, w_k, w_v, gain_attn, norm_in)


def turned(v, sine):
    return pltpu.roll(v, v.shape[1] // 2, 1) * sine


class RingGather:
    def __init__(self, wires, me, buf, rows):
        self.wires, self.me, self.buf, self.rows = wires, me, buf, rows
        self.half = me.n // 2
        self.got = None

    def send(self, right, left):
        buf = self.buf
        self.got = (
            self.wires.go(buf.at[right], buf.at[right], self.me.right_dev),
            self.wires.go(buf.at[left], buf.at[left], self.me.left_dev),
        )

    def wait(self):
        for copy in self.got:
            copy.wait_recv()

    def step(self, k):
        if k > 1:
            self.wait()
        rows = self.rows
        right, left = self.me.at_place(self.me.n - k + 1) * rows, self.me.at_place(k - 1) * rows
        size = rows
        if k == self.half:
            size = rows // 2
            left = left + size
        self.send(pl.ds(pl.multiple_of(right, size), size), pl.ds(pl.multiple_of(left, size), size))


def head_copies(n):
    return 3 * n + 1


def head_kernel(n, x, w_q, w_k, w_v, gain_attn, w_out, w_gate, w_up, w_down, gain_mlp, cos_ref, sin_ref, gain_ref, *refs):
    raw_q, raw_k, q_o, kv_o, u1, wqkv, wo = refs[:7]
    packed, w_far = refs[7:10], refs[10]
    own_far, send, recv = refs[11:]
    t, d = x.shape
    hd = cos_ref.shape[1]
    qw, kw = w_q.shape[1], w_k.shape[1]
    bw = w_q.shape[0]
    p = w_gate.shape[1] // NZ
    me = Spot(n)
    wires = Wires(send, recv)
    greet([me.right_dev, me.left_dev, me.z_dev(2)])
    half = n // 2
    mine = rows_at(me.blk, bw)

    gain = gain_attn[...]
    wqkv[mine, :qw] = (w_q[...].astype(F32) * gain).astype(BF16)
    wqkv[mine, qw : qw + kw] = (w_k[...].astype(F32) * gain).astype(BF16)
    wqkv[mine, qw + kw :] = (w_v[...].astype(F32) * gain).astype(BF16)
    w_ring = RingGather(wires, me, wqkv, bw)
    w_ring.step(1)

    def unit():
        @pl.loop(0, 4)
        def _(k):
            at = rows_at(k, t // 4)
            v = x[at, :].astype(F32)
            u1[at, :] = (v * lax.rsqrt(jnp.mean(v * v, axis=-1, keepdims=True) + EPS)).astype(BF16)

    def pack(s, to):
        at = rows_at(me.plane(s), p)
        gain = gain_mlp[...]
        to[:, :p] = (w_gate[:, at].astype(F32) * gain).astype(BF16)
        to[:, p : 2 * p] = (w_up[:, at].astype(F32) * gain).astype(BF16)
        to[:, 2 * p :] = w_down[at, :].astype(F32).T.astype(BF16)

    def output_block():
        wo[mine, :] = w_out[...].astype(F32).T.astype(BF16)

    jobs = [
        lambda: (unit(), output_block()),
        lambda: (pack(2, own_far), pack(0, packed[0])),
        lambda: (pack(1, packed[1]), pack(3, packed[2])),
    ]
    for k in range(2, half + 1):
        if jobs:
            jobs.pop(0)()
        w_ring.step(k)
    for job in jobs:
        job()
    far = wires.go(own_far, w_far, me.z_dev(2))
    w_ring.wait()

    rows = t // 2

    @pl.loop(0, 2)
    def _(k):
        at = rows_at(k, rows)
        own = pl.ds(pl.multiple_of(me.blk * t + k * rows, rows), rows)
        y = dot(u1[at, :], wqkv[...], NN)
        raw_q[at, :] = y[:, :qw].astype(BF16)
        raw_k[at, :] = y[:, qw : qw + kw].astype(BF16)
        cosine, sine = cos_ref[at, :], sin_ref[at, :]
        for h in range((qw + kw) // hd):
            v = y[:, h * hd : (h + 1) * hd]
            rs = lax.rsqrt(jnp.mean(v * v, axis=-1, keepdims=True) + EPS)
            v = v * rs * gain_ref[0 if h * hd < qw else 1]
            v = (v * cosine + turned(v, sine)).astype(BF16)
            if h * hd < qw:
                q_o[at, h * hd : (h + 1) * hd] = v
            else:
                kv_o[own, h * hd - qw : (h + 1) * hd - qw] = v
        kv_o[own, kw:] = y[:, qw + kw :].astype(BF16)

    kv_ring = RingGather(wires, me, kv_o, t)
    o_ring = RingGather(wires, me, wo, bw)
    for k in range(1, half + 1):
        kv_ring.step(k)
        o_ring.step(k)
    kv_ring.wait()
    o_ring.wait()
    far.wait_recv()
    wires.close()


def head(n, x, w_q, w_k, w_v, gain_attn, w_out, w_gate, w_up, w_down, gain_mlp, cosine, sine, gains):
    t, d = x.shape
    bw, qw = w_q.shape
    kw = w_k.shape[1]
    w3 = 3 * w_gate.shape[1] // NZ
    shape = jax.ShapeDtypeStruct
    copies = head_copies(n)
    return pl.pallas_call(
        partial(head_kernel, n),
        in_specs=[VMEM] * 13,
        out_specs=[VMEM] * 11,
        out_shape=[
            shape((t, qw), BF16),
            shape((t, kw), BF16),
            shape((t, qw), BF16),
            shape((n * t, 2 * kw), BF16),
            shape((t, d), BF16),
            shape((d, qw + 2 * kw), BF16),
            shape((d, qw), BF16),
        ]
        + [shape((bw, w3), BF16)] * 4,
        scratch_shapes=[
            pltpu.VMEM((bw, w3), BF16),
            pltpu.SemaphoreType.DMA((copies,)),
            pltpu.SemaphoreType.DMA((copies,)),
        ],
        compiler_params=pltpu.CompilerParams(
            collective_id=3, has_side_effects=True, vmem_limit_bytes=67000000
        ),
        name="head",
    )(x, w_q, w_k, w_v, gain_attn, w_out, w_gate, w_up, w_down, gain_mlp, cosine, sine, gains)


def tile_masks(base_ref, tile, qpos_ref, qfirst_ref, off_ref, q0, stretch):
    kpos = off_ref[...] + base_ref[tile]
    qpos = qpos_ref[pl.ds(q0, stretch), :]
    qfirst = qfirst_ref[pl.ds(q0, stretch), :]
    return (kpos <= qpos) & (kpos >= qfirst)


def attend_kernel(dims, scale, base_ref, see_ref, q_ref, kv_ref, qpos_ref, qfirst_ref, off_ref, out_ref, lse_ref, acc_ref, sum_ref):
    qh, kh, hd, stretch = dims
    group = qh // kh
    tile = pl.program_id(0)
    last = pl.num_programs(0) - 1

    @pl.when(tile == 0)
    def _():
        acc_ref[...] = jnp.zeros_like(acc_ref)
        sum_ref[...] = jnp.zeros_like(sum_ref)

    for e in range(2):
        q0 = e * stretch

        @pl.when(see_ref[e, tile] > 0)
        def _():
            mask = tile_masks(base_ref, tile, qpos_ref, qfirst_ref, off_ref, q0, stretch)
            for h in range(qh):
                k = kv_ref[:, (h // group) * hd : (h // group + 1) * hd]
                v = kv_ref[:, (kh + h // group) * hd : (kh + h // group + 1) * hd]
                q = q_ref[q0 : q0 + stretch, h * hd : (h + 1) * hd]
                s = dot(q, k, NT) * scale
                p = jnp.where(mask, jnp.exp(s), 0.0)
                sum_ref[h, q0 : q0 + stretch, :] += jnp.sum(p, axis=-1, keepdims=True)
                acc_ref[q0 : q0 + stretch, h * hd : (h + 1) * hd] += dot(p.astype(BF16), v, NN)

    @pl.when(tile == last)
    def _():
        for h in range(qh):
            total = sum_ref[h]
            out_ref[:, h * hd : (h + 1) * hd] = (acc_ref[:, h * hd : (h + 1) * hd] / total).astype(BF16)
            lse_ref[:, h : h + 1] = jnp.log(total)


def attend(base, see, q, kv, qpos, qfirst, off, qh, kh, hd, scale):
    t = q.shape[0]
    stretch = t // 2
    tiles = kv.shape[0] // stretch

    def whole(shape):
        return pl.BlockSpec(shape, lambda i, *_: (0,) * len(shape))

    return pl.pallas_call(
        partial(attend_kernel, (qh, kh, hd, stretch), scale),
        grid_spec=pltpu.PrefetchScalarGridSpec(
            num_scalar_prefetch=2,
            grid=(tiles,),
            in_specs=[
                whole((t, qh * hd)),
                pl.BlockSpec((stretch, 2 * kh * hd), lambda i, *_: (i, 0)),
                whole((t, 1)),
                whole((t, 1)),
                whole((1, stretch)),
            ],
            out_specs=[whole((t, qh * hd)), whole((t, qh))],
            scratch_shapes=[pltpu.VMEM((t, qh * hd), F32), pltpu.VMEM((qh, t, 1), F32)],
        ),
        out_shape=[
            jax.ShapeDtypeStruct((t, qh * hd), BF16),
            jax.ShapeDtypeStruct((t, qh), F32),
        ],
        cost_estimate=pl.CostEstimate(
            flops=4 * t * kv.shape[0] * hd * qh, bytes_accessed=2 * kv.size, transcendentals=t * kv.shape[0]
        ),
        name="attend",
    )(base, see, q, kv, qpos, qfirst, off)


def attend_back_kernel(
    dims, scale, base_ref, see_ref, q_ref, kv_ref, do_ref, o_ref, lse_ref, qpos_ref, qfirst_ref, off_ref, dq_ref, dkv_out, acc_ref, delta_ref, dkv_ref
):
    qh, kh, hd, stretch = dims
    group = qh // kh
    tile = pl.program_id(0)
    last = pl.num_programs(0) - 1

    @pl.when(tile == 0)
    def _():
        acc_ref[...] = jnp.zeros_like(acc_ref)
        for h in range(qh):
            at = slice(h * hd, (h + 1) * hd)
            delta_ref[h] = jnp.sum(do_ref[:, at].astype(F32) * o_ref[:, at].astype(F32), axis=-1, keepdims=True)

    sees = [see_ref[0, tile] > 0, see_ref[1, tile] > 0]

    @pl.when(jnp.logical_not(sees[0]))
    def _():
        dkv_ref[...] = jnp.zeros_like(dkv_ref)

    def half(e, add):
        q0 = e * stretch
        mask = tile_masks(base_ref, tile, qpos_ref, qfirst_ref, off_ref, q0, stretch)
        for c in range(kh):
            k = kv_ref[:, c * hd : (c + 1) * hd]
            v = kv_ref[:, (kh + c) * hd : (kh + c + 1) * hd]
            dk = dv = None
            for h in range(c * group, (c + 1) * group):
                at = slice(h * hd, (h + 1) * hd)
                q = q_ref[q0 : q0 + stretch, at]
                do = do_ref[q0 : q0 + stretch, at]
                s = dot(q, k, NT) * scale
                p = jnp.where(mask, jnp.exp(s - lse_ref[q0 : q0 + stretch, h : h + 1]), 0.0)
                dp = dot(do, v, NT)
                ds = (p * (dp - delta_ref[h, q0 : q0 + stretch, :])).astype(BF16)
                acc_ref[q0 : q0 + stretch, at] += dot(ds, k, NN)
                dk_h = dot(ds, q, TN)
                dv_h = dot(p.astype(BF16), do, TN)
                dk = dk_h if dk is None else dk + dk_h
                dv = dv_h if dv is None else dv + dv_h
            ck = slice(c * hd, (c + 1) * hd)
            cv = slice((kh + c) * hd, (kh + c + 1) * hd)
            if add:
                dkv_ref[:, ck] += dk * scale
                dkv_ref[:, cv] += dv
            else:
                dkv_ref[:, ck] = dk * scale
                dkv_ref[:, cv] = dv

    for e in range(2):

        @pl.when(sees[e])
        def _():
            half(e, e == 1)

    dkv_out[...] = dkv_ref[...].astype(BF16)

    @pl.when(tile == last)
    def _():
        dq_ref[...] = (acc_ref[...] * scale).astype(BF16)


def attend_back(base, see, q, kv, do, o, lse, qpos, qfirst, off, qh, kh, hd, scale):
    t = q.shape[0]
    stretch = t // 2
    tiles = kv.shape[0] // stretch

    def whole(shape):
        return pl.BlockSpec(shape, lambda i, *_: (0,) * len(shape))

    tile_spec = pl.BlockSpec((stretch, 2 * kh * hd), lambda i, *_: (i, 0))
    return pl.pallas_call(
        partial(attend_back_kernel, (qh, kh, hd, stretch), scale),
        grid_spec=pltpu.PrefetchScalarGridSpec(
            num_scalar_prefetch=2,
            grid=(tiles,),
            in_specs=[
                whole((t, qh * hd)),
                tile_spec,
                whole((t, qh * hd)),
                whole((t, qh * hd)),
                whole((t, qh)),
                whole((t, 1)),
                whole((t, 1)),
                whole((1, stretch)),
            ],
            out_specs=[whole((t, qh * hd)), tile_spec],
            scratch_shapes=[
                pltpu.VMEM((t, qh * hd), F32),
                pltpu.VMEM((qh, t, 1), F32),
                pltpu.VMEM((stretch, 2 * kh * hd), F32),
            ],
        ),
        out_shape=[
            jax.ShapeDtypeStruct((t, qh * hd), BF16),
            jax.ShapeDtypeStruct((kv.shape[0], 2 * kh * hd), BF16),
        ],
        cost_estimate=pl.CostEstimate(
            flops=10 * t * kv.shape[0] * hd * qh, bytes_accessed=6 * kv.size, transcendentals=t * kv.shape[0]
        ),
        name="attend_back",
    )(base, see, q, kv, do, o, lse, qpos, qfirst, off)


def after(value, *others):
    return lax.optimization_barrier((value,) + others)[0]


def shards(
    n,
    layer_input,
    w_query,
    w_key,
    w_value,
    w_output,
    w_gate,
    w_up,
    w_down,
    norm_attn,
    norm_mlp,
    norm_query,
    norm_key,
    out_grad,
    doc_lengths,
    stretch_order,
):
    t, d = layer_input.shape
    hd = norm_query.shape[0]
    qh, kh = w_query.shape[1] // hd, w_key.shape[1] // hd
    stretch = t // 2
    quarter = t // 4
    width = d // n
    ny = n // NZ
    scale = hd ** (-0.5)
    blk, tp = lax.axis_index("blk"), lax.axis_index("tp")
    z = blk // ny

    order = ring_order(n)
    place = jnp.array([order.index(b) for b in range(n)], jnp.int32)
    me = lax.dynamic_index_in_dim(place, blk, keepdims=False)
    cols = jnp.take(jnp.array(order + order, jnp.int32), me + jnp.arange(n, dtype=jnp.int32))

    gain_attn = norm_attn.astype(F32)[:, None]
    gain_mlp = norm_mlp.astype(F32)[:, None]

    starts = jnp.cumsum(doc_lengths) - doc_lengths

    def first_of(pos):
        return jnp.max(jnp.where(starts[None, :] <= pos[:, None], starts[None, :], 0), axis=1)

    inside = jnp.arange(stretch, dtype=jnp.int32)
    base = stretch_order * stretch
    base_own = lax.dynamic_slice_in_dim(base, 2 * blk, 2, 0)
    positions = (base_own[:, None] + inside[None, :]).reshape(-1)
    firsts = first_of(positions)
    base_first = first_of(base_own)
    see = ((base[None, :] <= base_own[:, None]) & (base[None, :] + (stretch - 1) >= base_first[:, None])).astype(jnp.int32)
    inverse = ROPE_BASE ** (-2.0 * jnp.arange(hd // 2, dtype=F32) / hd)
    angles = (positions - firsts).astype(F32)[:, None] * inverse[None, :]
    cosine, sine = jnp.cos(angles), jnp.sin(angles)
    cosine = jnp.concatenate([cosine, cosine], axis=1)
    sine = jnp.concatenate([-sine, sine], axis=1)
    qpos, qfirst, off = positions[:, None], firsts[:, None], inside[None, :]
    gains = jnp.stack([norm_query.astype(F32)[None, :], norm_key.astype(F32)[None, :]])

    raw_q, raw_k, q, kv, unit_attn, full_qkv, full_out, *packed = head(
        n, layer_input, w_query, w_key, w_value, gain_attn, w_output, w_gate, w_up, w_down, gain_mlp, cosine, sine, gains
    )
    x_low = lax.dynamic_slice_in_dim(layer_input, tp * quarter, quarter, 0)
    g_low = lax.dynamic_slice_in_dim(out_grad, tp * quarter, quarter, 0)
    g_one, g_two = z_swap(after(g_low, q), n, 1), z_swap(after(g_low, q), n, 2)
    attn_low, lse = attend(base, see, q, kv, qpos, qfirst, off, qh, kh, hd, scale)

    hidden, grad_hidden, grad_heads, hidden_low, _, _, acts, w_mlp, own_piece, norm_mlp_terms, *pieces = feed(
        n, attn_low, full_out, x_low.astype(F32), out_grad, g_one, g_two, packed
    )

    if n <= 8:
        attention = (base, off, qpos, qfirst, q, kv, grad_heads, lse)
    else:
        dq, dkv = attend_back(base, see, q, kv, grad_heads, attn_low, lse, qpos, qfirst, off, qh, kh, hd, scale)
        dkv = [lax.dynamic_slice_in_dim(dkv, cols[r] * t, t, 0).astype(F32) for r in range(n)]
        attention = (dq, ring_scatter(lambda r: dkv[r], n, t))
    layer_output, input_grad, grad_q, grad_k, grad_v, grad_out_w, small = tail(
        n, scale, attention, raw_q, raw_k, cosine, sine, gains, unit_attn, full_qkv, hidden_low, attn_low, grad_hidden,
        x_low, hidden, acts, w_mlp, w_query, w_key, w_value, gain_attn, norm_mlp_terms,
    )
    order = jnp.stack([z, z + 1 - 2 * (z % 2), (z + 2) % NZ, NZ - 1 - z]).astype(jnp.int32)
    pieces = [after(piece, small) for piece in [own_piece] + pieces]
    grad_gate, grad_up, grad_down = finish(order, pieces, gain_mlp)
    heads = small[2 * width :, :]
    part = hd // n
    return (
        layer_output,
        input_grad.astype(F32),
        grad_q,
        grad_k,
        grad_v,
        grad_out_w,
        grad_gate,
        grad_up,
        grad_down,
        small[:width, 0],
        small[width : 2 * width, 0] / gain_mlp[:, 0],
        lax.dynamic_slice(heads, (0, blk * part), (1, part))[0],
        lax.dynamic_slice(heads, (1, blk * part), (1, part))[0],
    )


def solution(mesh):
    return jax.shard_map(
        partial(shards, mesh.shape["blk"]),
        mesh=mesh,
        in_specs=(
            P("blk", None),
            P("blk", "tp"),
            P("blk", "tp"),
            P("blk", "tp"),
            P("tp", "blk"),
            P("blk", "tp"),
            P("blk", "tp"),
            P("tp", "blk"),
            P("blk"),
            P("blk"),
            P(),
            P(),
            P("blk", None),
            P(),
            P(),
        ),
        out_specs=(
            P("blk", None),
            P("blk", None),
            P("blk", "tp"),
            P("blk", "tp"),
            P("blk", "tp"),
            P("tp", "blk"),
            P("blk", "tp"),
            P("blk", "tp"),
            P("tp", "blk"),
            P("blk"),
            P("blk"),
            P("blk"),
            P("blk"),
        ),
        check_vma=False,
    )
```

```python
from functools import partial

import jax
import jax.numpy as jnp
from jax import lax
from jax.experimental import pallas as pl
from jax.experimental.pallas import tpu as pltpu
from jax.sharding import PartitionSpec as P

EPS = 1e-06
ROPE_BASE = 1000000.0
F32 = jnp.float32
BF16 = jnp.bfloat16


def dot(a, b, dims, out=F32):
    return lax.dot_general(a, b, (dims, ((), ())), preferred_element_type=out)


NN = ((1,), (0,))
NT = ((1,), (1,))
TN = ((0,), (0,))


def ring_order(n):
    return list(range(0, n, 2)) + list(range(n - 1, 0, -2))


def ring_perms(n):
    order = ring_order(n)
    right = [(order[i], order[(i + 1) % n]) for i in range(n)]
    return right, [(b, a) for a, b in right]


def ring_scatter(part, n, rows):
    right, left = ring_perms(n)
    half = n // 2
    cut = rows // 2
    far = part(half).astype(BF16)
    to_right = lax.ppermute(far[:cut], "blk", right).astype(F32)
    to_left = lax.ppermute(far[cut:], "blk", left).astype(F32)
    if half == 1:
        return part(0) + jnp.concatenate([to_right, to_left], axis=0)
    for k in range(half - 1, 0, -1):
        send_right, send_left = part(k), part(n - k)
        if k == half - 1:
            send_right = jnp.concatenate([send_right[:cut] + to_right, send_right[cut:]], axis=0)
            send_left = jnp.concatenate([send_left[:cut], send_left[cut:] + to_left], axis=0)
        else:
            send_right = send_right + to_right
            send_left = send_left + to_left
        to_right = lax.ppermute(send_right.astype(BF16), "blk", right).astype(F32)
        to_left = lax.ppermute(send_left.astype(BF16), "blk", left).astype(F32)
    return part(0) + to_right + to_left


NZ = 4


VMEM = pl.BlockSpec(memory_space=pltpu.VMEM)
SMEM = pl.BlockSpec(memory_space=pltpu.SMEM)
HBM = pl.BlockSpec(memory_space=pl.ANY)


def finish_kernel(zs_ref, *refs):
    pieces = refs[:NZ]
    gain_ref, d_gate, d_up, d_down = refs[NZ:]
    part = d_gate.shape[1] // NZ
    gain = gain_ref[...]
    for s in range(NZ):
        at = pl.ds(pl.multiple_of(zs_ref[s] * part, part), part)
        d_gate[:, at] = pieces[s][:, :part].astype(F32) * gain
        d_up[:, at] = pieces[s][:, part : 2 * part].astype(F32) * gain
        d_down[at, :] = pieces[s][:, 2 * part :].astype(F32).T


def finish(zs, pieces, gain):
    rows, cols = pieces[0].shape[0], NZ * pieces[0].shape[1] // 3
    return pl.pallas_call(
        finish_kernel,
        in_specs=[SMEM] + [VMEM] * (NZ + 1),
        out_specs=[VMEM] * 3,
        out_shape=[
            jax.ShapeDtypeStruct((rows, cols), F32),
            jax.ShapeDtypeStruct((rows, cols), F32),
            jax.ShapeDtypeStruct((cols, rows), F32),
        ],
        name="finish",
    )(zs, *pieces, gain)


MESH = pl.DeviceIdType.MESH


class Wires:
    def __init__(self, send, recv):
        self.send, self.recv, self.sent, self.done = send, recv, [], []

    def go(self, src, dst, device):
        i = len(self.sent)
        copy = pltpu.make_async_remote_copy(
            src_ref=src,
            dst_ref=dst,
            send_sem=self.send.at[i],
            recv_sem=self.recv.at[i],
            device_id=device,
            device_id_type=MESH,
        )
        copy.start()
        self.sent.append(copy)
        return copy

    def drain(self, copies):
        for copy in copies:
            copy.wait_send()
            self.done.append(copy)

    def pass_on(self, buf, me, plane, q):
        at = rows_at(plane * 4 + me.tp, q)
        return self.go(buf.at[at], buf.at[at], me.far_dev), self.go(buf.at[at], buf.at[at], me.core_dev)

    def pass_far(self, buf, me, plane, q, copies):
        copies[0].wait_recv()
        at = rows_at(plane * 4 + me.tp_far, q)
        return copies[1], self.go(buf.at[at], buf.at[at], me.core_dev)

    def close(self):
        self.drain([copy for copy in self.sent if not any(copy is other for other in self.done)])


def greet(devices):
    barrier = pltpu.get_barrier_semaphore()
    for device in devices:
        pl.semaphore_signal(barrier, inc=1, device_id=device, device_id_type=MESH)
    pl.semaphore_wait(barrier, len(devices))


class Spot:
    def __init__(self, n):
        self.n, self.ny = n, n // NZ
        self.blk, self.tp = lax.axis_index("blk"), lax.axis_index("tp")
        self.z, self.y = self.blk // self.ny, self.blk % self.ny
        self.x, self.core = self.tp // 2, self.tp % 2
        self.tp_core = self.x * 2 + (1 - self.core)
        self.tp_far = (1 - self.x) * 2 + self.core
        self.core_dev = {"tp": self.tp_core}
        self.far_dev = {"tp": self.tp_far}
        self.place = jnp.where(self.blk % 2 == 0, self.blk // 2, n - 1 - self.blk // 2)
        self.right_dev = {"blk": self.at_place(1)}
        self.left_dev = {"blk": self.at_place(n - 1)}

    def at_place(self, r):
        p = (self.place + r) % self.n
        return jnp.where(p < self.n // 2, 2 * p, 2 * (self.n - 1 - p) + 1)

    def plane(self, s):
        return (self.z + s) % NZ

    def z_dev(self, s):
        return {"blk": self.plane(s) * self.ny + self.y}

    def plane_x(self, k):
        return (self.z + 1 - 2 * (self.z % 2), (self.z + 2) % NZ, NZ - 1 - self.z)[k - 1]

    def x_dev(self, k):
        return {"blk": self.plane_x(k) * self.ny + self.y}

    def y_dev(self, j):
        return {"blk": self.z * self.ny + (self.y + j) % self.ny}

    def peers(self):
        return (
            [self.core_dev, self.far_dev]
            + [self.z_dev(s) for s in range(1, NZ)]
            + [self.y_dev(j) for j in range(1, self.ny)]
        )


def rows_at(index, count):
    return pl.ds(pl.multiple_of(index * count, count), count)


def feed_copies(n):
    return 64 + 8 * (n // NZ - 1)


def feed_kernel(n, attn, wo, x_own, g_in, *refs):
    packed = refs[:NZ]
    hidden_o, gh_o, heads_o, hl_o, dw_o, y_o, act_o, w_o, own_o, norm_o, *owned = refs[NZ : NZ + 13]
    (u_all, g_all, dgu, o_part, o_core, o_x, part, near, core_in, x_in, z_in, dw_tile, dw_sum, dw_in, send, recv, dw_sem, in_sem, g_sem) = refs[NZ + 13 :]
    q, d = x_own.shape
    p = packed[0].shape[1] // 3
    bw = packed[0].shape[0]
    me = Spot(n)
    wires = Wires(send, recv)
    greet(me.peers())

    def quarter(plane, peer):
        return rows_at(plane * 4 + peer, q)

    def arrived(copies):
        for copy in copies:
            copy.wait_recv()

    mine = rows_at(me.blk, bw)
    two = rows_at(me.plane(2) * me.ny + me.y, bw)
    w_z = {1: wires.go(packed[1], w_o.at[mine], me.z_dev(1)), 3: wires.go(packed[2], w_o.at[mine], me.z_dev(3))}
    near_plane, over_plane, last_plane = me.plane_x(1), me.plane_x(2), me.plane_x(3)
    near_dev, over_dev = me.x_dev(1), me.x_dev(2)
    g_load = pltpu.make_async_copy(g_in, g_all, g_sem)
    g_load.start()
    w_y = [wires.go(packed[0], w_o.at[mine], me.y_dev(j)) for j in range(1, me.ny)]
    w_y += [wires.go(packed[3], w_o.at[two], me.y_dev(j)) for j in range(1, me.ny)]

    def project(peer):
        return dot(attn[rows_at(peer, q), :], wo[...], NT)

    for i, x in enumerate((1 - me.x, me.x)):
        o_part[i] = project(x * 2 + 1 - me.core).astype(BF16)
    far_in = wires.go(o_part.at[0], o_core.at[0], me.core_dev)
    near_in = wires.go(o_part.at[1], o_core.at[1], me.core_dev)
    own_far = project(me.tp_far)
    far_in.wait_recv()
    o_core[0] = (own_far + o_core[0].astype(F32)).astype(BF16)
    x_sum = wires.go(o_core.at[0], o_x, me.far_dev)
    own_sum = project(me.tp) + x_own[...].astype(F32)
    w_o[mine, :] = packed[0][...]
    w_o[two, :] = packed[3][...]
    near_in.wait_recv()
    own_sum = own_sum + o_core[1].astype(F32)
    x_sum.wait_recv()
    hidden = own_sum + o_x[...].astype(F32)
    hidden_o[...] = hidden
    rs = lax.rsqrt(jnp.mean(hidden * hidden, axis=-1, keepdims=True) + EPS)
    own_q = quarter(me.z, me.tp)
    u_all[own_q, :] = (hidden * rs).astype(BF16)

    own_pass = wires.pass_on(u_all, me, me.z, q)
    u_one = wires.go(u_all.at[own_q], u_all.at[own_q], near_dev)
    u_two = wires.go(u_all.at[own_q], u_all.at[own_q], over_dev)
    for s in (1, 3):
        w_z[s].wait_recv()
        at = rows_at(me.plane(-s) * me.ny + me.y, bw)
        w_y += [wires.go(w_o.at[at], w_o.at[at], me.y_dev(j)) for j in range(1, me.ny)]
    own_pass = wires.pass_far(u_all, me, me.z, q, own_pass)
    g_load.wait()
    arrived(w_y)
    arrived(own_pass)

    def compute(i, plane):
        @pl.loop(0, 2)
        def _(k):
            at = pl.ds(pl.multiple_of(plane * (4 * q) + k * (2 * q), 2 * q), 2 * q)
            gate_up = dot(u_all[at, :], w_o[:, : 2 * p], NN)
            grad_act = dot(g_all[at, :], w_o[:, 2 * p :], NN)
            gate, up = gate_up[:, :p], gate_up[:, p:]
            sig = 1.0 / (1.0 + jnp.exp(-gate))
            silu = gate * sig
            act_o[at, :] = (silu * up).astype(BF16)
            dgu[at, p:] = (grad_act * silu).astype(BF16)
            dgu[at, :p] = (grad_act * up * (sig * (1.0 + gate * (1.0 - sig)))).astype(BF16)

        rows = rows_at(plane, 4 * q)
        tile = 512

        @pl.loop(0, d // tile)
        def _(c):
            at = pl.ds(pl.multiple_of(c * tile, tile), tile)
            part[i % 2, :, at] = dot(dgu[rows, :], w_o[at, : 2 * p], NT).astype(BF16)

    cores, fars = {}, {}

    def reduce_core(i):
        cores[i] = []
        for k, x in enumerate((1 - me.x, me.x)):
            src = part.at[i % 2, rows_at(x * 2 + 1 - me.core, q)]
            cores[i].append(wires.go(src, core_in.at[i, k], me.core_dev))

    def reduce_prep(i):
        for k, peer in enumerate((me.tp_far, me.tp)):
            cores[i][k].wait_recv()
            core_in[i, k] = (part[i % 2, rows_at(peer, q), :].astype(F32) + core_in[i, k].astype(F32)).astype(BF16)
        wires.drain(cores[i])

    def reduce_far(i):
        fars[i] = wires.go(core_in.at[i, 0], x_in.at[i], me.far_dev)

    def reduce_near(i):
        fars[i].wait_recv()
        return core_in[i, 1].astype(F32) + x_in[i].astype(F32)

    tiles = d // (256 * NZ)

    def planes(k):
        return me.plane_x(k) if k else me.z

    def dw_copy(plane, c):
        rows = rows_at(plane * tiles + c, 256)
        return pltpu.make_async_copy(dw_tile.at[c % 2], dw_o.at[rows], dw_sem.at[c % 2])

    y_copies = {}

    def grads(k):
        plane = planes(k)

        @pl.loop(0, tiles)
        def _(c):
            @pl.when(c >= 2)
            def _():
                dw_copy(plane, c - 2).wait()

            at = rows_at(plane * tiles + c, 256)
            dw_tile[c % 2, :, : 2 * p] = dot(u_all[:, at], dgu[...], TN).astype(BF16)
            dw_tile[c % 2, :, 2 * p :] = dot(g_all[:, at], act_o[...], TN).astype(BF16)
            dw_copy(plane, c).start()

        for c in range(max(0, tiles - 2), tiles):
            dw_copy(plane, c).wait()
        y_copies[k] = [
            wires.go(dw_o.at[rows_at(plane * me.ny + (me.y + j) % me.ny, bw)], y_o.at[(j - 1) * NZ + k], me.y_dev(j))
            for j in range(1, me.ny)
        ]

    z_copies = []

    def to_owner(k):
        plane = planes(k)
        at = rows_at(plane * me.ny + me.y, bw)
        loads = [pltpu.make_async_copy(dw_o.at[at], dw_in.at[0], in_sem.at[0])]
        loads[0].start()
        for j in range(1, me.ny):
            y_copies[k][j - 1].wait_recv()
            loads.append(pltpu.make_async_copy(y_o.at[(j - 1) * NZ + k], dw_in.at[j], in_sem.at[j]))
            loads[j].start()
        total = None
        for j, load in enumerate(loads):
            load.wait()
            term = dw_in[j].astype(F32)
            total = term if total is None else total + term
        norm = jnp.sum(total[:, : 2 * p] * w_o[at, : 2 * p].astype(F32), axis=1, keepdims=True)
        norm_o[k] = jnp.broadcast_to(norm, norm_o.shape[1:])
        if k == 0:
            own_o[...] = total.astype(BF16)
        else:
            dw_sum[k - 1] = total.astype(BF16)
            z_copies.append(wires.go(dw_sum.at[k - 1], owned[k - 1], me.x_dev(k)))

    compute(0, me.z)
    reduce_core(0)
    u_one.wait_recv()
    u_one_pass = wires.pass_on(u_all, me, near_plane, q)
    u_two.wait_recv()
    u_three = wires.go(u_all.at[quarter(over_plane, me.tp)], u_all.at[quarter(over_plane, me.tp)], near_dev)
    u_two_pass = wires.pass_on(u_all, me, over_plane, q)
    reduce_prep(0)
    u_one_pass = wires.pass_far(u_all, me, near_plane, q, u_one_pass)
    arrived(u_one_pass)
    compute(1, near_plane)
    reduce_core(1)
    u_three.wait_recv()
    u_three_pass = wires.pass_on(u_all, me, last_plane, q)
    u_two_pass = wires.pass_far(u_all, me, over_plane, q, u_two_pass)
    reduce_prep(1)
    arrived(u_two_pass)
    compute(2, over_plane)
    reduce_core(2)
    u_three_pass = wires.pass_far(u_all, me, last_plane, q, u_three_pass)
    reduce_prep(2)
    reduce_far(2)
    arrived(u_three_pass)
    compute(3, last_plane)
    reduce_core(3)
    reduce_prep(3)
    reduce_far(3)
    grads(3)
    grads(2)
    near[1] = reduce_near(2).astype(BF16)
    near[2] = reduce_near(3).astype(BF16)
    z_three = wires.go(near.at[2], z_in.at[1], near_dev)
    reduce_far(1)
    reduce_far(0)
    grads(1)
    to_owner(3)
    z_three.wait_recv()
    near[1] = (near[1].astype(F32) + z_in[1].astype(F32)).astype(BF16)
    z_two = wires.go(near.at[1], z_in.at[2], over_dev)
    near[0] = reduce_near(1).astype(BF16)
    z_one = wires.go(near.at[0], z_in.at[0], near_dev)
    grads(0)
    m = reduce_near(0)
    z_one.wait_recv()
    m = m + z_in[0].astype(F32)
    z_two.wait_recv()
    m = m + z_in[2].astype(F32)

    hidden = hidden_o[...]
    rs = lax.rsqrt(jnp.mean(hidden * hidden, axis=-1, keepdims=True) + EPS)
    unit = hidden * rs
    grad = g_all[own_q, :].astype(F32) + (m - unit * jnp.mean(m * unit, axis=-1, keepdims=True)) * rs
    gh_o[...] = grad
    own = rows_at(me.tp, q)
    hl_o[own, :] = grad.astype(BF16)
    x_copy = wires.go(hl_o.at[own], hl_o.at[own], me.far_dev)
    c_copy = wires.go(hl_o.at[own], hl_o.at[own], me.core_dev)

    def heads(peer):
        heads_o[rows_at(peer, q), :] = dot(hl_o[rows_at(peer, q), :], wo[...], NN).astype(BF16)

    to_owner(2)
    heads(me.tp)
    c_copy.wait_recv()
    heads(me.tp_core)
    x_copy.wait_recv()
    at = rows_at(me.tp_far, q)
    last = wires.go(hl_o.at[at], hl_o.at[at], me.core_dev)
    heads(me.tp_far)
    to_owner(1)
    last.wait_recv()
    heads((1 - me.x) * 2 + 1 - me.core)
    to_owner(0)
    arrived(z_copies)
    wires.close()


def feed(n, attn, wo, x_own, g_in, packed):
    q, d = x_own.shape
    t, a = attn.shape
    bw, w3 = packed[0].shape
    p = w3 // 3
    tokens = NZ * t
    copies = feed_copies(n)
    vm = pltpu.VMEM
    return pl.pallas_call(
        partial(feed_kernel, n),
        in_specs=[VMEM] * 3 + [HBM] + [VMEM] * NZ,
        out_specs=[VMEM] * 4 + [HBM] * 2 + [VMEM] * 4 + [HBM] * 3,
        out_shape=[
            jax.ShapeDtypeStruct((q, d), F32),
            jax.ShapeDtypeStruct((q, d), F32),
            jax.ShapeDtypeStruct((t, a), BF16),
            jax.ShapeDtypeStruct((t, d), BF16),
            jax.ShapeDtypeStruct((d, w3), BF16),
            jax.ShapeDtypeStruct((NZ * (n // NZ - 1), bw, w3), BF16),
            jax.ShapeDtypeStruct((tokens, p), BF16),
            jax.ShapeDtypeStruct((d, w3), BF16),
            jax.ShapeDtypeStruct((bw, w3), BF16),
            jax.ShapeDtypeStruct((NZ, bw, 128), F32),
        ]
        + [jax.ShapeDtypeStruct((bw, w3), BF16)] * 3,
        scratch_shapes=[
            vm((tokens, d), BF16),
            vm((tokens, d), BF16),
            vm((tokens, 2 * p), BF16),
            vm((2, q, d), BF16),
            vm((2, q, d), BF16),
            vm((q, d), BF16),
            vm((2, t, d), BF16),
            vm((NZ - 1, q, d), BF16),
            vm((NZ, 2, q, d), BF16),
            vm((NZ, q, d), BF16),
            vm((NZ - 1, q, d), BF16),
            vm((2, 256, w3), BF16),
            vm((3, bw, w3), BF16),
            vm((n // NZ, bw, w3), BF16),
            pltpu.SemaphoreType.DMA((copies,)),
            pltpu.SemaphoreType.DMA((copies,)),
            pltpu.SemaphoreType.DMA((2,)),
            pltpu.SemaphoreType.DMA((n // NZ,)),
            pltpu.SemaphoreType.DMA,
        ],
        compiler_params=pltpu.CompilerParams(
            collective_id=1, has_side_effects=True, vmem_limit_bytes=67000000
        ),
        name="feed",
    )(attn, wo, x_own, g_in, *packed)


class RingSum:
    def __init__(self, wires, me, land, stage, part):
        self.wires, self.me, self.land, self.stage, self.part = wires, me, land, stage, part
        self.half = me.n // 2
        self.cut = land.shape[2] // 2
        self.got = None

    def start(self):
        top, low, cut = pl.ds(0, self.cut), pl.ds(self.cut, self.cut), self.half - 1
        self.stage[...] = self.part(self.half).astype(BF16)
        self.got = (
            self.wires.go(self.stage.at[top], self.land.at[0, cut, top], self.me.right_dev),
            self.wires.go(self.stage.at[low], self.land.at[1, cut, low], self.me.left_dev),
        )
        self.first = self.got

    def step(self, k):
        cut = self.cut
        sent = []
        for side, place, dev in ((0, k, self.me.right_dev), (1, self.me.n - k, self.me.left_dev)):
            mine = self.part(place)
            self.got[side].wait_recv()
            if k == self.half - 1:
                keep, fresh = (slice(0, cut), slice(cut, None)) if side == 0 else (slice(cut, None), slice(0, cut))
                self.land[side, k, keep, :] = (self.land[side, k, keep, :].astype(F32) + mine[keep]).astype(BF16)
                self.land[side, k, fresh, :] = mine[fresh].astype(BF16)
            else:
                self.land[side, k] = (self.land[side, k].astype(F32) + mine).astype(BF16)
            sent.append(self.wires.go(self.land.at[side, k], self.land.at[side, k - 1], dev))
        self.got = tuple(sent)

    def total(self):
        mine = self.part(0)
        for copy in self.got:
            copy.wait_recv()
        return mine + self.land[0, 0].astype(F32) + self.land[1, 0].astype(F32)


def tail_copies(n):
    return 2 * 4 * (n // 2) + 16 + 3 + 3 + 3 + 3 + 3 + 2 + 8


def tail_kernel(n, ringed, scale, *refs):
    ins = 8 if ringed else 2
    (raw_q, raw_k, cos_ref, sin_ref, gain_ref, u1, wqkv, hl, attn, gh, x_own, hidden, act, w_mlp) = refs[ins : ins + 14]
    w_q, w_k, w_v, gain_attn, norm_in = refs[ins + 14 : ins + 19]
    lo, ig_low, gq_o, gk_o, gv_o, go_o, small_o = refs[ins + 19 : ins + 26]
    (d_qkv, gains, kv_land, kv_stage, o_land, o_stage, q_land, w_land, w_stage, m_part, m_core, m_x, part, core_in, x_in, z_in) = refs[ins + 26 : ins + 42]
    norm_land, small_core, small_x, o_whole, w_whole, w_down, dq_acc, kv_acc, delta, send, recv, load_sem = refs[ins + 42 :]
    q, d = hidden.shape
    t, qw = raw_q.shape
    hd = cos_ref.shape[1]
    kw = raw_k.shape[1]
    bw = w_q.shape[0]
    p = act.shape[1]
    load = pltpu.make_async_copy(w_mlp.at[:, pl.ds(2 * p, p)], w_down, load_sem)
    load.start()
    me = Spot(n)
    wires = Wires(send, recv)
    greet(me.peers() + [me.right_dev, me.left_dev])

    norm_copies = [
        wires.go(norm_in.at[k], norm_land.at[k - 1], me.x_dev(k)) for k in range(1, NZ)
    ]

    def head_back(src, raw, heads, kind, to):
        gains[kind] = jnp.zeros((1, hd), F32)

        @pl.loop(0, 4)
        def _(k):
            at = pl.ds(pl.multiple_of(k * q, q), q)
            cosine, sine = cos_ref[at, :], sin_ref[at, :]
            for h in range(heads):
                cols = slice(h * hd, (h + 1) * hd)
                grad = src[at, cols].astype(F32)
                grad = grad * cosine - turned(grad, sine)
                v = raw[at, cols].astype(F32)
                rs = lax.rsqrt(jnp.mean(v * v, axis=-1, keepdims=True) + EPS)
                unit = v * rs
                gains[kind] += jnp.sum(grad * unit, axis=0, keepdims=True)
                m = grad * gain_ref[kind]
                back = (m - unit * jnp.mean(m * unit, axis=-1, keepdims=True)) * rs
                d_qkv[at, to + h * hd : to + (h + 1) * hd] = back.astype(BF16)

    slots = (3, 1, 2, 0)
    cores, fars, backs = {}, {}, {}

    def slot_plane(i):
        return me.plane_x(slots[i]) if slots[i] else me.z

    def down(i):
        rows = rows_at(slot_plane(i), 4 * q)
        tile = 512

        @pl.loop(0, d // tile)
        def _(c):
            at = pl.ds(pl.multiple_of(c * tile, tile), tile)
            part[i % 2, :, at] = dot(act[rows, :], w_down[at, :], NT).astype(BF16)

        cores[i] = [
            wires.go(part.at[i % 2, rows_at(x * 2 + 1 - me.core, q)], core_in.at[i, k], me.core_dev)
            for k, x in enumerate((1 - me.x, me.x))
        ]

    def down_far(i):
        cores[i][0].wait_recv()
        core_in[i, 0] = (part[i % 2, rows_at(me.tp_far, q), :].astype(F32) + core_in[i, 0].astype(F32)).astype(BF16)
        fars[i] = wires.go(core_in.at[i, 0], x_in.at[i], me.far_dev)

    def down_near(i):
        cores[i][1].wait_recv()
        fars[i].wait_recv()
        value = part[i % 2, rows_at(me.tp, q), :].astype(F32) + core_in[i, 1].astype(F32) + x_in[i].astype(F32)
        wires.drain(cores[i])
        if slots[i] == 0:
            return value
        if slots[i] == 2:
            backs[0].wait_recv()
            value = value + z_in[0].astype(F32)
        x_in[i] = value.astype(BF16)
        backs[i] = wires.go(x_in.at[i], z_in.at[i], me.x_dev(2 if slots[i] == 2 else 1))

    def term(left, right, whole):
        if bw % 128 == 0:
            return lambda r: dot(left[:, rows_at(me.at_place(r), bw)], right[...], TN)

        @pl.loop(0, d // 256)
        def _(c):
            at = rows_at(c, 256)
            whole[at, :] = dot(left[:, at], right[...], TN).astype(BF16)

        return lambda r: whole[rows_at(me.at_place(r), bw), :].astype(F32)

    o_part = term(hl, attn, o_whole)

    o_ring = RingSum(wires, me, o_land, o_stage, o_part)

    half = n // 2
    if ringed:
        base_ref, off_ref, qpos_ref, qfirst_ref, q_ref, kv_ref, do_ref, lse_ref = refs[:8]
        stretch, kh = t // 2, kw // hd
        group = qw // kw
        dq = dq_acc
        dq_acc[...] = jnp.zeros_like(dq_acc)
        for h in range(qw // hd):
            cols = slice(h * hd, (h + 1) * hd)
            delta[:, h : h + 1] = jnp.sum(do_ref[:, cols].astype(F32) * attn[:, cols].astype(F32), axis=-1, keepdims=True)

        def kv_terms(r):
            block = me.at_place(r)
            @pl.loop(0, 2)
            def _(e):
                keys = rows_at(2 * block + e, stretch)
                to = rows_at(e, stretch)
                kpos = off_ref[...] + base_ref[2 * block + e]
                mask = (kpos <= qpos_ref[...]) & (kpos >= qfirst_ref[...])
                for c in range(kh):
                    ck = slice(c * hd, (c + 1) * hd)
                    cv = slice((kh + c) * hd, (kh + c + 1) * hd)
                    k, v = kv_ref[keys, ck], kv_ref[keys, cv]
                    dk = dv = None
                    for h in range(c * group, (c + 1) * group):
                        cols = slice(h * hd, (h + 1) * hd)
                        qh, do = q_ref[:, cols], do_ref[:, cols]
                        prob = jnp.where(mask, jnp.exp(dot(qh, k, NT) * scale - lse_ref[:, h : h + 1]), 0.0)
                        ds = (prob * (dot(do, v, NT) - delta[:, h : h + 1])).astype(BF16)
                        dq_acc[:, cols] += dot(ds, k, NN)
                        dk_h, dv_h = dot(ds, qh, TN), dot(prob.astype(BF16), do, TN)
                        dk = dk_h if dk is None else dk + dk_h
                        dv = dv_h if dv is None else dv + dv_h
                    kv_acc[to, ck] = dk * scale
                    kv_acc[to, cv] = dv

            return kv_acc[...]

        kv_ring = RingSum(wires, me, kv_land, kv_stage, kv_terms)
        kv_ring.start()
    else:
        dq, dkv = refs[:2]
    load.wait()
    fill = [
        lambda: (o_ring.start(), down(0)),
        lambda: (down_far(0), down(1)),
        lambda: (down_near(0), down_far(1), down(2)),
        lambda: (down_near(1), down_far(2), down(3)),
    ]
    for k in range(half - 1, 0, -1):
        if ringed:
            kv_ring.step(k)
        if fill:
            fill.pop(0)()
        if k < half - 1:
            o_ring.step(k + 1)
    for job in fill:
        job()
    if half > 1:
        o_ring.step(1)
    if ringed:
        kv_total = kv_ring.total().astype(BF16)
        wires.drain(kv_ring.first)
        kv_stage[...] = kv_total
        kv_sum = kv_stage
        dq_acc[...] = dq_acc[...] * scale
    else:
        kv_sum = dkv
    head_back(dq, raw_q, qw // hd, 0, 0)
    head_back(kv_sum, raw_k, kw // hd, 1, qw)
    d_qkv[:, qw + kw :] = kv_sum[:, kw:].astype(BF16)

    def m_term(peer):
        return dot(d_qkv[rows_at(peer, q), :], wqkv[...], NT)

    q_cols, kv_cols = pl.ds(0, qw), pl.ds(qw, 2 * kw)
    split = bw % 128 != 0
    q_term = term(u1, d_qkv.at[:, q_cols], w_whole.at[:, q_cols] if split else None)
    kv_w_term = term(u1, d_qkv.at[:, kv_cols], w_whole.at[:, kv_cols] if split else None)

    def kv_part(r):
        body = kv_w_term(r)
        extra = w_land.shape[2] - bw
        rest = jnp.concatenate([gains[0], gains[1], jnp.zeros((extra - 2, hd), F32)], axis=0)
        rest = jnp.concatenate([rest, jnp.zeros((extra, body.shape[1] - hd), F32)], axis=1)
        return jnp.concatenate([body, rest], axis=0)

    rings = (RingSum(wires, me, q_land, o_stage, q_term), RingSum(wires, me, w_land, w_stage, kv_part))
    for i, x in enumerate((1 - me.x, me.x)):
        m_part[i] = m_term(x * 2 + 1 - me.core).astype(BF16)
    m_far = wires.go(m_part.at[0], m_core.at[0], me.core_dev)
    m_near = wires.go(m_part.at[1], m_core.at[1], me.core_dev)
    wires.drain(o_ring.first)
    for ring in rings:
        ring.start()
    own_far = m_term(me.tp_far)
    m_far.wait_recv()
    m_core[0] = (own_far + m_core[0].astype(F32)).astype(BF16)
    m_sum = wires.go(m_core.at[0], m_x, me.far_dev)
    own = m_term(me.tp)
    m_near.wait_recv()
    own = own + m_core[1].astype(F32)
    steps = list(range(half - 1, 0, -1))

    def tick():
        k = steps.pop(0)
        for ring in rings:
            ring.step(k)

    if steps:
        tick()
    m_sum.wait_recv()
    m = own + m_x[...].astype(F32)
    x = x_own[...].astype(F32)
    rs = lax.rsqrt(jnp.mean(x * x, axis=-1, keepdims=True) + EPS)
    unit = x * rs
    grad = gh[...] + (m - unit * jnp.mean(m * unit, axis=-1, keepdims=True)) * rs
    mine = rows_at(me.tp, q)
    ig_low[mine, :] = grad.astype(BF16)

    def spread(buf):
        far = wires.go(buf.at[mine], buf.at[mine], me.far_dev)
        core = wires.go(buf.at[mine], buf.at[mine], me.core_dev)
        return far, core

    def spread_far(buf, copies):
        copies[0].wait_recv()
        at = rows_at(me.tp_far, q)
        return wires.go(buf.at[at], buf.at[at], me.core_dev)

    ig_copies = spread(ig_low)
    if steps:
        tick()

    down_near(2)
    down_far(3)
    out = hidden[...] + down_near(3)
    for i in (1, 2):
        backs[i].wait_recv()
        out = out + z_in[i].astype(F32)
    lo[mine, :] = out.astype(BF16)
    lo_copies = spread(lo)
    ig_last = spread_far(ig_low, ig_copies)
    while steps:
        tick()
    go_o[...] = o_ring.total().T

    lo_last = spread_far(lo, lo_copies)
    ig_copies[1].wait_recv()
    ig_last.wait_recv()
    grad_q = rings[0].total()
    total = rings[1].total()
    grad = total[:bw]
    gain = gain_attn[...]
    norm = jnp.sum(grad_q * w_q[...].astype(F32), axis=1, keepdims=True)
    norm = norm + jnp.sum(grad[:, :kw] * w_k[...].astype(F32), axis=1, keepdims=True)
    norm = norm + jnp.sum(grad[:, kw:] * w_v[...].astype(F32), axis=1, keepdims=True)
    small_o[:bw, :] = jnp.broadcast_to(norm, (bw, hd))
    mlp = norm_in[0]
    for s in range(1, NZ):
        norm_copies[s - 1].wait_recv()
        mlp = mlp + norm_land[s - 1]
    small_o[bw : 2 * bw, :] = mlp
    small_o[2 * bw :, :] = total[bw : bw + 16, :hd]
    copy = wires.go(small_o, small_core, me.core_dev)
    gq_o[...] = grad_q * gain
    gk_o[...] = grad[:, :kw] * gain
    gv_o[...] = grad[:, kw:] * gain
    copy.wait_recv()
    small_core[...] += small_o[...]
    copy = wires.go(small_core, small_x, me.far_dev)
    lo_copies[1].wait_recv()
    lo_last.wait_recv()
    copy.wait_recv()
    wires.close()
    small_o[...] = small_core[...] + small_x[...]


def tail(n, scale, attention, raw_q, raw_k, cosine, sine, gains, u1, wqkv, hl, attn, gh, x_own, hidden, act, w_mlp, w_q, w_k, w_v, gain_attn, norm_in):
    ringed = len(attention) > 2
    q, d = hidden.shape
    t, qw = raw_q.shape
    hd = cosine.shape[1]
    kw = raw_k.shape[1]
    wide = qw + 2 * kw
    bw = d // n
    p = act.shape[1]
    half = n // 2
    copies = tail_copies(n)
    vm = pltpu.VMEM
    small = 2 * bw + 16
    shape = jax.ShapeDtypeStruct
    none = (16, 128)
    return pl.pallas_call(
        partial(tail_kernel, n, ringed, scale),
        in_specs=([SMEM] + [VMEM] * 7 if ringed else [VMEM] * 2) + [VMEM] * 13 + [HBM] + [VMEM] * 5,
        out_specs=[VMEM] * 7,
        out_shape=[
            shape((t, d), BF16),
            shape((t, d), BF16),
            shape((bw, qw), F32),
            shape((bw, kw), F32),
            shape((bw, kw), F32),
            shape((attn.shape[1], bw), F32),
            shape((small, hd), F32),
        ],
        scratch_shapes=[
            vm((t, wide), BF16),
            vm((2, 1, hd), F32),
            vm((2, half, t, 2 * kw) if ringed else (2, 1) + none, BF16),
            vm((t, 2 * kw) if ringed else none, BF16),
            vm((2, half, bw, attn.shape[1]), BF16),
            vm((bw, attn.shape[1]), BF16),
            vm((2, half, bw, qw), BF16),
            vm((2, half, bw + 32, 2 * kw), BF16),
            vm((bw + 32, 2 * kw), BF16),
            vm((2, q, d), BF16),
            vm((2, q, d), BF16),
            vm((q, d), BF16),
            vm((2, t, d), BF16),
            vm((NZ, 2, q, d), BF16),
            vm((NZ, q, d), BF16),
            vm((NZ - 1, q, d), BF16),
            vm((NZ - 1, bw, hd), F32),
            vm((small, hd), F32),
            vm((small, hd), F32),
            vm((d, attn.shape[1]) if bw % 128 else none, BF16),
            vm((d, wide) if bw % 128 else none, BF16),
            vm((d, p), BF16),
            vm((t, qw) if ringed else none, F32),
            vm((t, 2 * kw) if ringed else none, F32),
            vm((t, qw // hd) if ringed else none, F32),
            pltpu.SemaphoreType.DMA((copies,)),
            pltpu.SemaphoreType.DMA((copies,)),
            pltpu.SemaphoreType.DMA,
        ],
        compiler_params=pltpu.CompilerParams(
            collective_id=2, has_side_effects=True, vmem_limit_bytes=67000000
        ),
        name="tail",
    )(*attention, raw_q, raw_k, cosine, sine, gains, u1, wqkv, hl, attn, gh, x_own, hidden, act, w_mlp, w_q, w_k, w_v, gain_attn, norm_in)


def turned(v, sine):
    return pltpu.roll(v, v.shape[1] // 2, 1) * sine


class RingGather:
    def __init__(self, wires, me, buf, rows, part=(0, 1)):
        self.wires, self.me, self.buf, self.rows, self.part = wires, me, buf, rows, part
        self.half = me.n // 2
        self.got = None

    def send(self, right, left):
        buf = self.buf
        self.got = (
            self.wires.go(buf.at[right], buf.at[right], self.me.right_dev),
            self.wires.go(buf.at[left], buf.at[left], self.me.left_dev),
        )

    def wait(self):
        for copy in self.got:
            copy.wait_recv()

    def step(self, k):
        if k > 1:
            self.wait()
        which, parts = self.part
        size = self.rows // parts
        right = self.me.at_place(self.me.n - k + 1) * self.rows + which * size
        left = self.me.at_place(k - 1) * self.rows + which * size
        if k == self.half:
            size = size // 2
            left = left + size
        self.send(pl.ds(pl.multiple_of(right, size), size), pl.ds(pl.multiple_of(left, size), size))


def head_copies(n):
    return 4 * n + 16


def head_kernel(n, scale, x, w_q, w_k, w_v, gain_attn, w_out, w_gate, w_up, w_down, gain_mlp, cos_ref, sin_ref, gain_ref, g_rows, *refs):
    ins = 0 if scale is None else 4
    outs = ins + (0 if scale is None else 2)
    raw_q, raw_k, q_o, kv_o, u1, wqkv, wo, x_own, g_all = refs[ins : ins + 9]
    packed, w_far = refs[ins + 9 : ins + 12], refs[ins + 12]
    own_far, acc, tot, send, recv, g_sem = refs[outs + 13 :]
    t, d = x.shape
    hd = cos_ref.shape[1]
    qw, kw = w_q.shape[1], w_k.shape[1]
    bw = w_q.shape[0]
    p = w_gate.shape[1] // NZ
    me = Spot(n)
    wires = Wires(send, recv)
    greet([me.right_dev, me.left_dev, me.x_dev(1), me.x_dev(2), me.core_dev, me.far_dev])
    g_own = pltpu.make_async_copy(g_rows, g_all.at[rows_at(me.z, t)], g_sem)
    g_own.start()
    half = n // 2
    mine = rows_at(me.blk, bw)

    gain = gain_attn[...]
    wqkv[mine, :qw] = (w_q[...].astype(F32) * gain).astype(BF16)
    wqkv[mine, qw : qw + kw] = (w_k[...].astype(F32) * gain).astype(BF16)
    wqkv[mine, qw + kw :] = (w_v[...].astype(F32) * gain).astype(BF16)
    parts = 2 if bw % 64 == 0 else 1
    w_rings = [RingGather(wires, me, wqkv, bw, (i, parts)) for i in range(parts)]
    for ring in w_rings:
        ring.step(1)

    def unit():
        @pl.loop(0, 4)
        def _(k):
            at = rows_at(k, t // 4)
            v = x[at, :].astype(F32)
            u1[at, :] = (v * lax.rsqrt(jnp.mean(v * v, axis=-1, keepdims=True) + EPS)).astype(BF16)

    def pack(s, to):
        at = rows_at(me.plane(s), p)
        gain = gain_mlp[...]
        to[:, :p] = (w_gate[:, at].astype(F32) * gain).astype(BF16)
        to[:, p : 2 * p] = (w_up[:, at].astype(F32) * gain).astype(BF16)
        to[:, 2 * p :] = w_down[at, :].astype(F32).T.astype(BF16)

    x_own[...] = x[rows_at(me.tp, t // 4), :]

    def output_block():
        wo[mine, :] = w_out[...].astype(F32).T.astype(BF16)

    jobs = [
        lambda: (unit(), output_block()),
        lambda: (pack(2, own_far), pack(0, packed[0])),
        lambda: (pack(1, packed[1]), pack(3, packed[2])),
    ]
    for k in range(2, half + 1):
        if jobs:
            jobs.pop(0)()
        for ring in w_rings:
            ring.step(k)
    for job in jobs:
        job()
    far = wires.go(own_far, w_far, me.z_dev(2))
    q = t // 4
    g_src, g_dst = g_rows.at[rows_at(me.tp, q)], g_all.at[rows_at(me.z * 4 + me.tp, q)]
    near_plane, over_plane, last_plane = me.plane_x(1), me.plane_x(2), me.plane_x(3)
    g_one = wires.go(g_src, g_dst, me.x_dev(1))
    g_two = wires.go(g_src, g_dst, me.x_dev(2))
    g_copies = {}

    def g_near():
        g_one.wait_recv()
        g_copies[1] = wires.pass_on(g_all, me, near_plane, q)

    def g_over():
        g_two.wait_recv()
        at = rows_at(over_plane * 4 + me.tp, q)
        g_copies[0] = wires.go(g_all.at[at], g_all.at[at], me.x_dev(1))
        g_copies[2] = wires.pass_on(g_all, me, over_plane, q)

    def g_far():
        g_copies[1] = wires.pass_far(g_all, me, near_plane, q, g_copies[1])
        g_copies[2] = wires.pass_far(g_all, me, over_plane, q, g_copies[2])

    def g_last():
        g_copies[0].wait_recv()
        g_copies[3] = wires.pass_on(g_all, me, last_plane, q)

    g_jobs = [g_near, g_over, g_far, g_last]
    for ring in w_rings:
        ring.wait()

    rows = t // 2

    @pl.loop(0, 2)
    def _(k):
        at = rows_at(k, rows)
        own = pl.ds(pl.multiple_of(me.blk * t + k * rows, rows), rows)
        y = dot(u1[at, :], wqkv[...], NN)
        raw_q[at, :] = y[:, :qw].astype(BF16)
        raw_k[at, :] = y[:, qw : qw + kw].astype(BF16)
        cosine, sine = cos_ref[at, :], sin_ref[at, :]
        for h in range((qw + kw) // hd):
            v = y[:, h * hd : (h + 1) * hd]
            rs = lax.rsqrt(jnp.mean(v * v, axis=-1, keepdims=True) + EPS)
            v = v * rs * gain_ref[0 if h * hd < qw else 1]
            v = (v * cosine + turned(v, sine)).astype(BF16)
            if h * hd < qw:
                q_o[at, h * hd : (h + 1) * hd] = v
            else:
                kv_o[own, h * hd - qw : (h + 1) * hd - qw] = v
        kv_o[own, kw:] = y[:, qw + kw :].astype(BF16)

    def attend_block(r):
        if scale is None:
            return
        base_ref, off_ref, qpos_ref, qfirst_ref = refs[:ins]
        block = me.at_place(r)
        stretch = t // 2
        kh = kw // hd
        group = qw // kw

        @pl.loop(0, 2)
        def _(e):
            keys = rows_at(2 * block + e, stretch)
            kpos = off_ref[...] + base_ref[2 * block + e]
            mask = (kpos <= qpos_ref[...]) & (kpos >= qfirst_ref[...])
            for h in range(qw // hd):
                c = h // group
                cols = slice(h * hd, (h + 1) * hd)
                k, v = kv_o[keys, c * hd : (c + 1) * hd], kv_o[keys, (kh + c) * hd : (kh + c + 1) * hd]
                prob = jnp.where(mask, jnp.exp(dot(q_o[:, cols], k, NT) * scale), 0.0)
                tot[:, h : h + 1] += jnp.sum(prob, axis=-1, keepdims=True)
                acc[:, cols] += dot(prob.astype(BF16), v, NN)

    kv_ring = RingGather(wires, me, kv_o, t)
    o_ring = RingGather(wires, me, wo, bw)
    acc[...] = jnp.zeros_like(acc)
    tot[...] = jnp.zeros_like(tot)
    for k in range(1, half + 1):
        kv_ring.step(k)
        o_ring.step(k)
        if k > 1:
            attend_block(n - k + 1)
        attend_block(k - 1)
        if g_jobs:
            g_jobs.pop(0)()
    for job in g_jobs:
        job()
    kv_ring.wait()
    attend_block(half)
    if scale is not None:
        attn_o, lse_o = refs[outs + 11 : outs + 13]
        for h in range(qw // hd):
            cols = slice(h * hd, (h + 1) * hd)
            attn_o[:, cols] = (acc[:, cols] / tot[:, h : h + 1]).astype(BF16)
        lse_o[...] = jnp.log(tot[...])
    o_ring.wait()
    g_copies[3] = wires.pass_far(g_all, me, last_plane, q, g_copies[3])
    for k in (1, 2, 3):
        for copy in g_copies[k]:
            copy.wait_recv()
    g_own.wait()
    far.wait_recv()
    wires.close()


def head(n, scale, seen, x, w_q, w_k, w_v, gain_attn, w_out, w_gate, w_up, w_down, gain_mlp, cosine, sine, gains, g_rows):
    t, d = x.shape
    bw, qw = w_q.shape
    kw = w_k.shape[1]
    w3 = 3 * w_gate.shape[1] // NZ
    heads = qw // cosine.shape[1]
    shape = jax.ShapeDtypeStruct
    copies = head_copies(n)
    return pl.pallas_call(
        partial(head_kernel, n, scale),
        in_specs=[VMEM] * 14 + ([] if scale is None else [SMEM] + [VMEM] * 3),
        out_specs=[VMEM] * 8 + [HBM] + [VMEM] * (4 if scale is None else 6),
        out_shape=[
            shape((t, qw), BF16),
            shape((t, kw), BF16),
            shape((t, qw), BF16),
            shape((n * t, 2 * kw), BF16),
            shape((t, d), BF16),
            shape((d, qw + 2 * kw), BF16),
            shape((d, qw), BF16),
            shape((t // 4, d), BF16),
            shape((NZ * t, d), BF16),
        ]
        + [shape((bw, w3), BF16)] * 4
        + ([] if scale is None else [shape((t, qw), BF16), shape((t, heads), F32)]),
        scratch_shapes=[
            pltpu.VMEM((bw, w3), BF16),
            pltpu.VMEM((t, qw), F32),
            pltpu.VMEM((t, heads), F32),
            pltpu.SemaphoreType.DMA((copies,)),
            pltpu.SemaphoreType.DMA((copies,)),
            pltpu.SemaphoreType.DMA,
        ],
        compiler_params=pltpu.CompilerParams(
            collective_id=3, has_side_effects=True, vmem_limit_bytes=67000000
        ),
        name="head",
    )(x, w_q, w_k, w_v, gain_attn, w_out, w_gate, w_up, w_down, gain_mlp, cosine, sine, gains, g_rows, *seen)


def tile_masks(base_ref, tile, qpos_ref, qfirst_ref, off_ref, q0, stretch):
    kpos = off_ref[...] + base_ref[tile]
    qpos = qpos_ref[pl.ds(q0, stretch), :]
    qfirst = qfirst_ref[pl.ds(q0, stretch), :]
    return (kpos <= qpos) & (kpos >= qfirst)


def attend_kernel(dims, scale, base_ref, see_ref, q_ref, kv_ref, qpos_ref, qfirst_ref, off_ref, out_ref, lse_ref, acc_ref, sum_ref):
    qh, kh, hd, stretch = dims
    group = qh // kh
    tile = pl.program_id(0)
    last = pl.num_programs(0) - 1

    @pl.when(tile == 0)
    def _():
        acc_ref[...] = jnp.zeros_like(acc_ref)
        sum_ref[...] = jnp.zeros_like(sum_ref)

    for e in range(2):
        q0 = e * stretch

        @pl.when(see_ref[e, tile] > 0)
        def _():
            mask = tile_masks(base_ref, tile, qpos_ref, qfirst_ref, off_ref, q0, stretch)
            for h in range(qh):
                k = kv_ref[:, (h // group) * hd : (h // group + 1) * hd]
                v = kv_ref[:, (kh + h // group) * hd : (kh + h // group + 1) * hd]
                q = q_ref[q0 : q0 + stretch, h * hd : (h + 1) * hd]
                s = dot(q, k, NT) * scale
                p = jnp.where(mask, jnp.exp(s), 0.0)
                sum_ref[h, q0 : q0 + stretch, :] += jnp.sum(p, axis=-1, keepdims=True)
                acc_ref[q0 : q0 + stretch, h * hd : (h + 1) * hd] += dot(p.astype(BF16), v, NN)

    @pl.when(tile == last)
    def _():
        for h in range(qh):
            total = sum_ref[h]
            out_ref[:, h * hd : (h + 1) * hd] = (acc_ref[:, h * hd : (h + 1) * hd] / total).astype(BF16)
            lse_ref[:, h : h + 1] = jnp.log(total)


def attend(base, see, q, kv, qpos, qfirst, off, qh, kh, hd, scale):
    t = q.shape[0]
    stretch = t // 2
    tiles = kv.shape[0] // stretch

    def whole(shape):
        return pl.BlockSpec(shape, lambda i, *_: (0,) * len(shape))

    return pl.pallas_call(
        partial(attend_kernel, (qh, kh, hd, stretch), scale),
        grid_spec=pltpu.PrefetchScalarGridSpec(
            num_scalar_prefetch=2,
            grid=(tiles,),
            in_specs=[
                whole((t, qh * hd)),
                pl.BlockSpec((stretch, 2 * kh * hd), lambda i, *_: (i, 0)),
                whole((t, 1)),
                whole((t, 1)),
                whole((1, stretch)),
            ],
            out_specs=[whole((t, qh * hd)), whole((t, qh))],
            scratch_shapes=[pltpu.VMEM((t, qh * hd), F32), pltpu.VMEM((qh, t, 1), F32)],
        ),
        out_shape=[
            jax.ShapeDtypeStruct((t, qh * hd), BF16),
            jax.ShapeDtypeStruct((t, qh), F32),
        ],
        cost_estimate=pl.CostEstimate(
            flops=4 * t * kv.shape[0] * hd * qh, bytes_accessed=2 * kv.size, transcendentals=t * kv.shape[0]
        ),
        name="attend",
    )(base, see, q, kv, qpos, qfirst, off)


def attend_back_kernel(
    dims, scale, base_ref, see_ref, q_ref, kv_ref, do_ref, o_ref, lse_ref, qpos_ref, qfirst_ref, off_ref, dq_ref, dkv_out, acc_ref, delta_ref, dkv_ref
):
    qh, kh, hd, stretch = dims
    group = qh // kh
    tile = pl.program_id(0)
    last = pl.num_programs(0) - 1

    @pl.when(tile == 0)
    def _():
        acc_ref[...] = jnp.zeros_like(acc_ref)
        for h in range(qh):
            at = slice(h * hd, (h + 1) * hd)
            delta_ref[h] = jnp.sum(do_ref[:, at].astype(F32) * o_ref[:, at].astype(F32), axis=-1, keepdims=True)

    sees = [see_ref[0, tile] > 0, see_ref[1, tile] > 0]

    @pl.when(jnp.logical_not(sees[0]))
    def _():
        dkv_ref[...] = jnp.zeros_like(dkv_ref)

    def half(e, add):
        q0 = e * stretch
        mask = tile_masks(base_ref, tile, qpos_ref, qfirst_ref, off_ref, q0, stretch)
        for c in range(kh):
            k = kv_ref[:, c * hd : (c + 1) * hd]
            v = kv_ref[:, (kh + c) * hd : (kh + c + 1) * hd]
            dk = dv = None
            for h in range(c * group, (c + 1) * group):
                at = slice(h * hd, (h + 1) * hd)
                q = q_ref[q0 : q0 + stretch, at]
                do = do_ref[q0 : q0 + stretch, at]
                s = dot(q, k, NT) * scale
                p = jnp.where(mask, jnp.exp(s - lse_ref[q0 : q0 + stretch, h : h + 1]), 0.0)
                dp = dot(do, v, NT)
                ds = (p * (dp - delta_ref[h, q0 : q0 + stretch, :])).astype(BF16)
                acc_ref[q0 : q0 + stretch, at] += dot(ds, k, NN)
                dk_h = dot(ds, q, TN)
                dv_h = dot(p.astype(BF16), do, TN)
                dk = dk_h if dk is None else dk + dk_h
                dv = dv_h if dv is None else dv + dv_h
            ck = slice(c * hd, (c + 1) * hd)
            cv = slice((kh + c) * hd, (kh + c + 1) * hd)
            if add:
                dkv_ref[:, ck] += dk * scale
                dkv_ref[:, cv] += dv
            else:
                dkv_ref[:, ck] = dk * scale
                dkv_ref[:, cv] = dv

    for e in range(2):

        @pl.when(sees[e])
        def _():
            half(e, e == 1)

    dkv_out[...] = dkv_ref[...].astype(BF16)

    @pl.when(tile == last)
    def _():
        dq_ref[...] = (acc_ref[...] * scale).astype(BF16)


def attend_back(base, see, q, kv, do, o, lse, qpos, qfirst, off, qh, kh, hd, scale):
    t = q.shape[0]
    stretch = t // 2
    tiles = kv.shape[0] // stretch

    def whole(shape):
        return pl.BlockSpec(shape, lambda i, *_: (0,) * len(shape))

    tile_spec = pl.BlockSpec((stretch, 2 * kh * hd), lambda i, *_: (i, 0))
    return pl.pallas_call(
        partial(attend_back_kernel, (qh, kh, hd, stretch), scale),
        grid_spec=pltpu.PrefetchScalarGridSpec(
            num_scalar_prefetch=2,
            grid=(tiles,),
            in_specs=[
                whole((t, qh * hd)),
                tile_spec,
                whole((t, qh * hd)),
                whole((t, qh * hd)),
                whole((t, qh)),
                whole((t, 1)),
                whole((t, 1)),
                whole((1, stretch)),
            ],
            out_specs=[whole((t, qh * hd)), tile_spec],
            scratch_shapes=[
                pltpu.VMEM((t, qh * hd), F32),
                pltpu.VMEM((qh, t, 1), F32),
                pltpu.VMEM((stretch, 2 * kh * hd), F32),
            ],
        ),
        out_shape=[
            jax.ShapeDtypeStruct((t, qh * hd), BF16),
            jax.ShapeDtypeStruct((kv.shape[0], 2 * kh * hd), BF16),
        ],
        cost_estimate=pl.CostEstimate(
            flops=10 * t * kv.shape[0] * hd * qh, bytes_accessed=6 * kv.size, transcendentals=t * kv.shape[0]
        ),
        name="attend_back",
    )(base, see, q, kv, do, o, lse, qpos, qfirst, off)


def after(value, *others):
    return lax.optimization_barrier((value,) + others)[0]


def shards(
    n,
    layer_input,
    w_query,
    w_key,
    w_value,
    w_output,
    w_gate,
    w_up,
    w_down,
    norm_attn,
    norm_mlp,
    norm_query,
    norm_key,
    out_grad,
    doc_lengths,
    stretch_order,
):
    t, d = layer_input.shape
    hd = norm_query.shape[0]
    qh, kh = w_query.shape[1] // hd, w_key.shape[1] // hd
    stretch = t // 2
    quarter = t // 4
    width = d // n
    ny = n // NZ
    scale = hd ** (-0.5)
    blk, tp = lax.axis_index("blk"), lax.axis_index("tp")
    z = blk // ny

    order = ring_order(n)
    place = jnp.array([order.index(b) for b in range(n)], jnp.int32)
    me = lax.dynamic_index_in_dim(place, blk, keepdims=False)
    cols = jnp.take(jnp.array(order + order, jnp.int32), me + jnp.arange(n, dtype=jnp.int32))

    gain_attn = norm_attn.astype(F32)[:, None]
    gain_mlp = norm_mlp.astype(F32)[:, None]

    starts = jnp.cumsum(doc_lengths) - doc_lengths

    def first_of(pos):
        return jnp.max(jnp.where(starts[None, :] <= pos[:, None], starts[None, :], 0), axis=1)

    inside = jnp.arange(stretch, dtype=jnp.int32)
    base = stretch_order * stretch
    base_own = lax.dynamic_slice_in_dim(base, 2 * blk, 2, 0)
    positions = (base_own[:, None] + inside[None, :]).reshape(-1)
    firsts = first_of(positions)
    base_first = first_of(base_own)
    see = ((base[None, :] <= base_own[:, None]) & (base[None, :] + (stretch - 1) >= base_first[:, None])).astype(jnp.int32)
    inverse = ROPE_BASE ** (-2.0 * jnp.arange(hd // 2, dtype=F32) / hd)
    angles = (positions - firsts).astype(F32)[:, None] * inverse[None, :]
    cosine, sine = jnp.cos(angles), jnp.sin(angles)
    cosine = jnp.concatenate([cosine, cosine], axis=1)
    sine = jnp.concatenate([-sine, sine], axis=1)
    qpos, qfirst, off = positions[:, None], firsts[:, None], inside[None, :]
    gains = jnp.stack([norm_query.astype(F32)[None, :], norm_key.astype(F32)[None, :]])

    fused = n <= 8
    raw_q, raw_k, q, kv, unit_attn, full_qkv, full_out, x_low, g_all, *rest = head(
        n, scale if fused else None, (base, off, qpos, qfirst) if fused else (), layer_input, w_query, w_key, w_value,
        gain_attn, w_output, w_gate, w_up, w_down, gain_mlp, cosine, sine, gains, out_grad,
    )
    packed = rest[:4]
    attn_low, lse = rest[4:] if fused else attend(base, see, q, kv, qpos, qfirst, off, qh, kh, hd, scale)

    hidden, grad_hidden, grad_heads, hidden_low, _, _, acts, w_mlp, own_piece, norm_mlp_terms, *pieces = feed(
        n, attn_low, full_out, x_low, g_all, packed
    )

    if fused:
        attention = (base, off, qpos, qfirst, q, kv, grad_heads, lse)
    else:
        dq, dkv = attend_back(base, see, q, kv, grad_heads, attn_low, lse, qpos, qfirst, off, qh, kh, hd, scale)
        dkv = [lax.dynamic_slice_in_dim(dkv, cols[r] * t, t, 0).astype(F32) for r in range(n)]
        attention = (dq, ring_scatter(lambda r: dkv[r], n, t))
    layer_output, input_grad, grad_q, grad_k, grad_v, grad_out_w, small = tail(
        n, scale, attention, raw_q, raw_k, cosine, sine, gains, unit_attn, full_qkv, hidden_low, attn_low, grad_hidden,
        x_low, hidden, acts, w_mlp, w_query, w_key, w_value, gain_attn, norm_mlp_terms,
    )
    order = jnp.stack([z, z + 1 - 2 * (z % 2), (z + 2) % NZ, NZ - 1 - z]).astype(jnp.int32)
    pieces = [after(piece, small) for piece in [own_piece] + pieces]
    grad_gate, grad_up, grad_down = finish(order, pieces, gain_mlp)
    heads = small[2 * width :, :]
    part = hd // n
    return (
        layer_output,
        input_grad.astype(F32),
        grad_q,
        grad_k,
        grad_v,
        grad_out_w,
        grad_gate,
        grad_up,
        grad_down,
        small[:width, 0],
        small[width : 2 * width, 0] / gain_mlp[:, 0],
        lax.dynamic_slice(heads, (0, blk * part), (1, part))[0],
        lax.dynamic_slice(heads, (1, blk * part), (1, part))[0],
    )


def solution(mesh):
    return jax.shard_map(
        partial(shards, mesh.shape["blk"]),
        mesh=mesh,
        in_specs=(
            P("blk", None),
            P("blk", "tp"),
            P("blk", "tp"),
            P("blk", "tp"),
            P("tp", "blk"),
            P("blk", "tp"),
            P("blk", "tp"),
            P("tp", "blk"),
            P("blk"),
            P("blk"),
            P(),
            P(),
            P("blk", None),
            P(),
            P(),
        ),
        out_specs=(
            P("blk", None),
            P("blk", None),
            P("blk", "tp"),
            P("blk", "tp"),
            P("blk", "tp"),
            P("tp", "blk"),
            P("blk", "tp"),
            P("blk", "tp"),
            P("tp", "blk"),
            P("blk"),
            P("blk"),
            P("blk"),
            P("blk"),
        ),
        check_vma=False,
    )
```

```python
from functools import partial

import jax
import jax.numpy as jnp
from jax import lax
from jax.experimental import pallas as pl
from jax.experimental.pallas import tpu as pltpu
from jax.sharding import PartitionSpec as P

EPS = 1e-06
ROPE_BASE = 1000000.0
F32 = jnp.float32
BF16 = jnp.bfloat16


def dot(a, b, dims, out=F32):
    return lax.dot_general(a, b, (dims, ((), ())), preferred_element_type=out)


NN = ((1,), (0,))
NT = ((1,), (1,))
TN = ((0,), (0,))


def ring_order(n):
    return list(range(0, n, 2)) + list(range(n - 1, 0, -2))


def ring_perms(n):
    order = ring_order(n)
    right = [(order[i], order[(i + 1) % n]) for i in range(n)]
    return right, [(b, a) for a, b in right]


def ring_scatter(part, n, rows):
    right, left = ring_perms(n)
    half = n // 2
    cut = rows // 2
    far = part(half).astype(BF16)
    to_right = lax.ppermute(far[:cut], "blk", right).astype(F32)
    to_left = lax.ppermute(far[cut:], "blk", left).astype(F32)
    if half == 1:
        return part(0) + jnp.concatenate([to_right, to_left], axis=0)
    for k in range(half - 1, 0, -1):
        send_right, send_left = part(k), part(n - k)
        if k == half - 1:
            send_right = jnp.concatenate([send_right[:cut] + to_right, send_right[cut:]], axis=0)
            send_left = jnp.concatenate([send_left[:cut], send_left[cut:] + to_left], axis=0)
        else:
            send_right = send_right + to_right
            send_left = send_left + to_left
        to_right = lax.ppermute(send_right.astype(BF16), "blk", right).astype(F32)
        to_left = lax.ppermute(send_left.astype(BF16), "blk", left).astype(F32)
    return part(0) + to_right + to_left


NZ = 4


VMEM = pl.BlockSpec(memory_space=pltpu.VMEM)
SMEM = pl.BlockSpec(memory_space=pltpu.SMEM)
HBM = pl.BlockSpec(memory_space=pl.ANY)


def finish_kernel(zs_ref, *refs):
    pieces, (gain_ref, *ins), (d_gate, d_up, d_down, *outs) = refs[:NZ], refs[NZ : NZ + 7], refs[NZ + 7 :]
    part = d_gate.shape[1]
    step = pl.program_id(0)
    gain = gain_ref[...]
    for s in range(NZ):

        @pl.when(step == s)
        def _():
            d_gate[...] = pieces[s][:, :part].astype(F32) * gain
            d_up[...] = pieces[s][:, part : 2 * part].astype(F32) * gain
            d_down[...] = pieces[s][:, 2 * part :].astype(F32).T

    for src, dst in zip(ins, outs):
        dst[...] = src[...].astype(dst.dtype)


def finish(zs, pieces, gain, layer_output, input_grad, others):
    rows, w3 = pieces[0].shape
    part = w3 // 3
    whole = pl.BlockSpec((rows, w3), lambda i, z: (0, 0))
    moved = [layer_output, input_grad, *others]
    specs = [pl.BlockSpec((v.shape[0] // NZ, v.shape[1]), lambda i, z: (i, 0)) for v in moved]
    types = [layer_output.dtype, F32] + [v.dtype for v in others]
    shape = jax.ShapeDtypeStruct
    return pl.pallas_call(
        finish_kernel,
        grid_spec=pltpu.PrefetchScalarGridSpec(
            num_scalar_prefetch=1,
            grid=(NZ,),
            in_specs=[whole] * NZ + [pl.BlockSpec((rows, 1), lambda i, z: (0, 0))] + specs,
            out_specs=[
                pl.BlockSpec((rows, part), lambda i, z: (0, z[i])),
                pl.BlockSpec((rows, part), lambda i, z: (0, z[i])),
                pl.BlockSpec((part, rows), lambda i, z: (z[i], 0)),
            ]
            + specs,
        ),
        out_shape=[shape((rows, NZ * part), F32), shape((rows, NZ * part), F32), shape((NZ * part, rows), F32)]
        + [shape(v.shape, dtype) for v, dtype in zip(moved, types)],
        name="finish",
    )(zs, *pieces, gain, *moved)


MESH = pl.DeviceIdType.MESH


class Wires:
    def __init__(self, send, recv):
        self.send, self.recv, self.sent, self.done = send, recv, [], []

    def go(self, src, dst, device):
        i = len(self.sent)
        copy = pltpu.make_async_remote_copy(
            src_ref=src,
            dst_ref=dst,
            send_sem=self.send.at[i],
            recv_sem=self.recv.at[i],
            device_id=device,
            device_id_type=MESH,
        )
        copy.start()
        self.sent.append(copy)
        return copy

    def drain(self, copies):
        for copy in copies:
            copy.wait_send()
            self.done.append(copy)

    def pass_on(self, buf, me, plane, q):
        at = rows_at(plane * 4 + me.tp, q)
        return self.go(buf.at[at], buf.at[at], me.far_dev), self.go(buf.at[at], buf.at[at], me.core_dev)

    def pass_far(self, buf, me, plane, q, copies):
        copies[0].wait_recv()
        at = rows_at(plane * 4 + me.tp_far, q)
        return copies[1], self.go(buf.at[at], buf.at[at], me.core_dev)

    def close(self):
        self.drain([copy for copy in self.sent if not any(copy is other for other in self.done)])


def greet(devices):
    barrier = pltpu.get_barrier_semaphore()
    for device in devices:
        pl.semaphore_signal(barrier, inc=1, device_id=device, device_id_type=MESH)
    pl.semaphore_wait(barrier, len(devices))


class Spot:
    def __init__(self, n):
        self.n, self.ny = n, n // NZ
        self.blk, self.tp = lax.axis_index("blk"), lax.axis_index("tp")
        self.z, self.y = self.blk // self.ny, self.blk % self.ny
        self.x, self.core = self.tp // 2, self.tp % 2
        self.tp_core = self.x * 2 + (1 - self.core)
        self.tp_far = (1 - self.x) * 2 + self.core
        self.core_dev = {"tp": self.tp_core}
        self.far_dev = {"tp": self.tp_far}
        self.place = jnp.where(self.blk % 2 == 0, self.blk // 2, n - 1 - self.blk // 2)
        self.right_dev = {"blk": self.at_place(1)}
        self.left_dev = {"blk": self.at_place(n - 1)}

    def at_place(self, r):
        p = (self.place + r) % self.n
        return jnp.where(p < self.n // 2, 2 * p, 2 * (self.n - 1 - p) + 1)

    def plane(self, s):
        return (self.z + s) % NZ

    def z_dev(self, s):
        return {"blk": self.plane(s) * self.ny + self.y}

    def plane_x(self, k):
        return (self.z + 1 - 2 * (self.z % 2), (self.z + 2) % NZ, NZ - 1 - self.z)[k - 1]

    def x_dev(self, k):
        return {"blk": self.plane_x(k) * self.ny + self.y}

    def y_dev(self, j):
        return {"blk": self.z * self.ny + (self.y + j) % self.ny}

    def peers(self):
        return (
            [self.core_dev, self.far_dev]
            + [self.z_dev(s) for s in range(1, NZ)]
            + [self.y_dev(j) for j in range(1, self.ny)]
        )


def rows_at(index, count):
    return pl.ds(pl.multiple_of(index * count, count), count)


def feed_copies(n):
    return 64 + 8 * (n // NZ - 1)


def feed_kernel(n, attn, wo, x_own, g_in, *refs):
    packed = refs[:NZ]
    hidden_o, gh_o, heads_o, hl_o, dw_o, y_o, act_o, w_o, own_o, norm_o, *owned = refs[NZ : NZ + 13]
    (u_all, g_all, dgu, o_part, o_core, o_x, part, near, core_in, x_in, z_in, dw_tile, dw_sum, dw_in, send, recv, dw_sem, in_sem, g_sem) = refs[NZ + 13 :]
    q, d = x_own.shape
    p = packed[0].shape[1] // 3
    bw = packed[0].shape[0]
    me = Spot(n)
    wires = Wires(send, recv)
    greet(me.peers())

    def quarter(plane, peer):
        return rows_at(plane * 4 + peer, q)

    def arrived(copies):
        for copy in copies:
            copy.wait_recv()

    mine = rows_at(me.blk, bw)
    two = rows_at(me.plane(2) * me.ny + me.y, bw)
    w_z = {1: wires.go(packed[1], w_o.at[mine], me.z_dev(1)), 3: wires.go(packed[2], w_o.at[mine], me.z_dev(3))}
    near_plane, over_plane, last_plane = me.plane_x(1), me.plane_x(2), me.plane_x(3)
    near_dev, over_dev = me.x_dev(1), me.x_dev(2)
    g_load = pltpu.make_async_copy(g_in, g_all, g_sem)
    g_load.start()
    w_y = [wires.go(packed[0], w_o.at[mine], me.y_dev(j)) for j in range(1, me.ny)]
    w_y += [wires.go(packed[3], w_o.at[two], me.y_dev(j)) for j in range(1, me.ny)]

    def project(peer):
        return dot(attn[rows_at(peer, q), :], wo[...], NT)

    for i, x in enumerate((1 - me.x, me.x)):
        o_part[i] = project(x * 2 + 1 - me.core).astype(BF16)
    far_in = wires.go(o_part.at[0], o_core.at[0], me.core_dev)
    near_in = wires.go(o_part.at[1], o_core.at[1], me.core_dev)
    own_far = project(me.tp_far)
    far_in.wait_recv()
    o_core[0] = (own_far + o_core[0].astype(F32)).astype(BF16)
    x_sum = wires.go(o_core.at[0], o_x, me.far_dev)
    own_sum = project(me.tp) + x_own[...].astype(F32)
    w_o[mine, :] = packed[0][...]
    w_o[two, :] = packed[3][...]
    near_in.wait_recv()
    own_sum = own_sum + o_core[1].astype(F32)
    x_sum.wait_recv()
    hidden = own_sum + o_x[...].astype(F32)
    hidden_o[...] = hidden
    rs = lax.rsqrt(jnp.mean(hidden * hidden, axis=-1, keepdims=True) + EPS)
    own_q = quarter(me.z, me.tp)
    u_all[own_q, :] = (hidden * rs).astype(BF16)

    own_pass = wires.pass_on(u_all, me, me.z, q)
    u_one = wires.go(u_all.at[own_q], u_all.at[own_q], near_dev)
    u_two = wires.go(u_all.at[own_q], u_all.at[own_q], over_dev)
    for s in (1, 3):
        w_z[s].wait_recv()
        at = rows_at(me.plane(-s) * me.ny + me.y, bw)
        w_y += [wires.go(w_o.at[at], w_o.at[at], me.y_dev(j)) for j in range(1, me.ny)]
    own_pass = wires.pass_far(u_all, me, me.z, q, own_pass)
    g_load.wait()
    arrived(w_y)
    arrived(own_pass)

    def compute(i, plane):
        @pl.loop(0, 2)
        def _(k):
            at = pl.ds(pl.multiple_of(plane * (4 * q) + k * (2 * q), 2 * q), 2 * q)
            gate_up = dot(u_all[at, :], w_o[:, : 2 * p], NN)
            grad_act = dot(g_all[at, :], w_o[:, 2 * p :], NN)
            gate, up = gate_up[:, :p], gate_up[:, p:]
            sig = 1.0 / (1.0 + jnp.exp(-gate))
            silu = gate * sig
            act_o[at, :] = (silu * up).astype(BF16)
            dgu[at, p:] = (grad_act * silu).astype(BF16)
            dgu[at, :p] = (grad_act * up * (sig * (1.0 + gate * (1.0 - sig)))).astype(BF16)

        rows = rows_at(plane, 4 * q)
        tile = 512

        @pl.loop(0, d // tile)
        def _(c):
            at = pl.ds(pl.multiple_of(c * tile, tile), tile)
            part[i % 2, :, at] = dot(dgu[rows, :], w_o[at, : 2 * p], NT).astype(BF16)

    cores, fars = {}, {}

    def reduce_core(i):
        cores[i] = []
        for k, x in enumerate((1 - me.x, me.x)):
            src = part.at[i % 2, rows_at(x * 2 + 1 - me.core, q)]
            cores[i].append(wires.go(src, core_in.at[i, k], me.core_dev))

    def reduce_prep(i):
        for k, peer in enumerate((me.tp_far, me.tp)):
            cores[i][k].wait_recv()
            core_in[i, k] = (part[i % 2, rows_at(peer, q), :].astype(F32) + core_in[i, k].astype(F32)).astype(BF16)
        wires.drain(cores[i])

    def reduce_far(i):
        fars[i] = wires.go(core_in.at[i, 0], x_in.at[i], me.far_dev)

    def reduce_near(i):
        fars[i].wait_recv()
        return core_in[i, 1].astype(F32) + x_in[i].astype(F32)

    tiles = d // (256 * NZ)

    def planes(k):
        return me.plane_x(k) if k else me.z

    def dw_copy(plane, c):
        rows = rows_at(plane * tiles + c, 256)
        return pltpu.make_async_copy(dw_tile.at[c % 2], dw_o.at[rows], dw_sem.at[c % 2])

    y_copies = {}

    def grads(k):
        plane = planes(k)

        @pl.loop(0, tiles)
        def _(c):
            @pl.when(c >= 2)
            def _():
                dw_copy(plane, c - 2).wait()

            at = rows_at(plane * tiles + c, 256)
            dw_tile[c % 2, :, : 2 * p] = dot(u_all[:, at], dgu[...], TN).astype(BF16)
            dw_tile[c % 2, :, 2 * p :] = dot(g_all[:, at], act_o[...], TN).astype(BF16)
            dw_copy(plane, c).start()

        for c in range(max(0, tiles - 2), tiles):
            dw_copy(plane, c).wait()
        y_copies[k] = [
            wires.go(dw_o.at[rows_at(plane * me.ny + (me.y + j) % me.ny, bw)], y_o.at[(j - 1) * NZ + k], me.y_dev(j))
            for j in range(1, me.ny)
        ]

    z_copies = []

    def to_owner(k):
        plane = planes(k)
        at = rows_at(plane * me.ny + me.y, bw)
        loads = [pltpu.make_async_copy(dw_o.at[at], dw_in.at[0], in_sem.at[0])]
        loads[0].start()
        for j in range(1, me.ny):
            y_copies[k][j - 1].wait_recv()
            loads.append(pltpu.make_async_copy(y_o.at[(j - 1) * NZ + k], dw_in.at[j], in_sem.at[j]))
            loads[j].start()
        total = None
        for j, load in enumerate(loads):
            load.wait()
            term = dw_in[j].astype(F32)
            total = term if total is None else total + term
        norm = jnp.sum(total[:, : 2 * p] * w_o[at, : 2 * p].astype(F32), axis=1, keepdims=True)
        norm_o[k] = jnp.broadcast_to(norm, norm_o.shape[1:])
        if k == 0:
            own_o[...] = total.astype(BF16)
        else:
            dw_sum[k - 1] = total.astype(BF16)
            z_copies.append(wires.go(dw_sum.at[k - 1], owned[k - 1], me.x_dev(k)))

    compute(0, me.z)
    reduce_core(0)
    u_one.wait_recv()
    u_one_pass = wires.pass_on(u_all, me, near_plane, q)
    u_two.wait_recv()
    u_three = wires.go(u_all.at[quarter(over_plane, me.tp)], u_all.at[quarter(over_plane, me.tp)], near_dev)
    u_two_pass = wires.pass_on(u_all, me, over_plane, q)
    reduce_prep(0)
    u_one_pass = wires.pass_far(u_all, me, near_plane, q, u_one_pass)
    arrived(u_one_pass)
    compute(1, near_plane)
    reduce_core(1)
    u_three.wait_recv()
    u_three_pass = wires.pass_on(u_all, me, last_plane, q)
    u_two_pass = wires.pass_far(u_all, me, over_plane, q, u_two_pass)
    reduce_prep(1)
    arrived(u_two_pass)
    compute(2, over_plane)
    reduce_core(2)
    u_three_pass = wires.pass_far(u_all, me, last_plane, q, u_three_pass)
    reduce_prep(2)
    reduce_far(2)
    arrived(u_three_pass)
    compute(3, last_plane)
    reduce_core(3)
    reduce_prep(3)
    reduce_far(3)
    grads(3)
    grads(2)
    near[1] = reduce_near(2).astype(BF16)
    near[2] = reduce_near(3).astype(BF16)
    z_three = wires.go(near.at[2], z_in.at[1], near_dev)
    reduce_far(1)
    reduce_far(0)
    grads(1)
    to_owner(3)
    z_three.wait_recv()
    near[1] = (near[1].astype(F32) + z_in[1].astype(F32)).astype(BF16)
    z_two = wires.go(near.at[1], z_in.at[2], over_dev)
    near[0] = reduce_near(1).astype(BF16)
    z_one = wires.go(near.at[0], z_in.at[0], near_dev)
    grads(0)
    m = reduce_near(0)
    z_one.wait_recv()
    m = m + z_in[0].astype(F32)
    z_two.wait_recv()
    m = m + z_in[2].astype(F32)

    hidden = hidden_o[...]
    rs = lax.rsqrt(jnp.mean(hidden * hidden, axis=-1, keepdims=True) + EPS)
    unit = hidden * rs
    grad = g_all[own_q, :].astype(F32) + (m - unit * jnp.mean(m * unit, axis=-1, keepdims=True)) * rs
    gh_o[...] = grad
    own = rows_at(me.tp, q)
    hl_o[own, :] = grad.astype(BF16)
    x_copy = wires.go(hl_o.at[own], hl_o.at[own], me.far_dev)
    c_copy = wires.go(hl_o.at[own], hl_o.at[own], me.core_dev)

    def heads(peer):
        heads_o[rows_at(peer, q), :] = dot(hl_o[rows_at(peer, q), :], wo[...], NN).astype(BF16)

    to_owner(2)
    heads(me.tp)
    c_copy.wait_recv()
    heads(me.tp_core)
    x_copy.wait_recv()
    at = rows_at(me.tp_far, q)
    last = wires.go(hl_o.at[at], hl_o.at[at], me.core_dev)
    heads(me.tp_far)
    to_owner(1)
    last.wait_recv()
    heads((1 - me.x) * 2 + 1 - me.core)
    to_owner(0)
    arrived(z_copies)
    wires.close()


def feed(n, attn, wo, x_own, g_in, packed):
    q, d = x_own.shape
    t, a = attn.shape
    bw, w3 = packed[0].shape
    p = w3 // 3
    tokens = NZ * t
    copies = feed_copies(n)
    vm = pltpu.VMEM
    return pl.pallas_call(
        partial(feed_kernel, n),
        in_specs=[VMEM] * 3 + [HBM] + [VMEM] * NZ,
        out_specs=[VMEM] * 4 + [HBM] * 2 + [VMEM] * 4 + [HBM] * 3,
        out_shape=[
            jax.ShapeDtypeStruct((q, d), F32),
            jax.ShapeDtypeStruct((q, d), F32),
            jax.ShapeDtypeStruct((t, a), BF16),
            jax.ShapeDtypeStruct((t, d), BF16),
            jax.ShapeDtypeStruct((d, w3), BF16),
            jax.ShapeDtypeStruct((NZ * (n // NZ - 1), bw, w3), BF16),
            jax.ShapeDtypeStruct((tokens, p), BF16),
            jax.ShapeDtypeStruct((d, w3), BF16),
            jax.ShapeDtypeStruct((bw, w3), BF16),
            jax.ShapeDtypeStruct((NZ, bw, 128), F32),
        ]
        + [jax.ShapeDtypeStruct((bw, w3), BF16)] * 3,
        scratch_shapes=[
            vm((tokens, d), BF16),
            vm((tokens, d), BF16),
            vm((tokens, 2 * p), BF16),
            vm((2, q, d), BF16),
            vm((2, q, d), BF16),
            vm((q, d), BF16),
            vm((2, t, d), BF16),
            vm((NZ - 1, q, d), BF16),
            vm((NZ, 2, q, d), BF16),
            vm((NZ, q, d), BF16),
            vm((NZ - 1, q, d), BF16),
            vm((2, 256, w3), BF16),
            vm((3, bw, w3), BF16),
            vm((n // NZ, bw, w3), BF16),
            pltpu.SemaphoreType.DMA((copies,)),
            pltpu.SemaphoreType.DMA((copies,)),
            pltpu.SemaphoreType.DMA((2,)),
            pltpu.SemaphoreType.DMA((n // NZ,)),
            pltpu.SemaphoreType.DMA,
        ],
        compiler_params=pltpu.CompilerParams(
            collective_id=1, has_side_effects=True, vmem_limit_bytes=67000000
        ),
        name="feed",
    )(attn, wo, x_own, g_in, *packed)


class RingSum:
    def __init__(self, wires, me, land, stage, part):
        self.wires, self.me, self.land, self.stage, self.part = wires, me, land, stage, part
        self.half = me.n // 2
        self.cut = land.shape[2] // 2
        self.got = None

    def start(self):
        top, low, cut = pl.ds(0, self.cut), pl.ds(self.cut, self.cut), self.half - 1
        self.stage[...] = self.part(self.half).astype(BF16)
        self.got = (
            self.wires.go(self.stage.at[top], self.land.at[0, cut, top], self.me.right_dev),
            self.wires.go(self.stage.at[low], self.land.at[1, cut, low], self.me.left_dev),
        )
        self.first = self.got

    def step(self, k):
        cut = self.cut
        sent = []
        for side, place, dev in ((0, k, self.me.right_dev), (1, self.me.n - k, self.me.left_dev)):
            mine = self.part(place)
            self.got[side].wait_recv()
            if k == self.half - 1:
                keep, fresh = (slice(0, cut), slice(cut, None)) if side == 0 else (slice(cut, None), slice(0, cut))
                self.land[side, k, keep, :] = (self.land[side, k, keep, :].astype(F32) + mine[keep]).astype(BF16)
                self.land[side, k, fresh, :] = mine[fresh].astype(BF16)
            else:
                self.land[side, k] = (self.land[side, k].astype(F32) + mine).astype(BF16)
            sent.append(self.wires.go(self.land.at[side, k], self.land.at[side, k - 1], dev))
        self.got = tuple(sent)

    def total(self):
        mine = self.part(0)
        for copy in self.got:
            copy.wait_recv()
        return mine + self.land[0, 0].astype(F32) + self.land[1, 0].astype(F32)


def tail_copies(n):
    return 2 * 4 * (n // 2) + 16 + 3 + 3 + 3 + 3 + 3 + 2 + 8


def tail_kernel(n, ringed, scale, *refs):
    ins = 8 if ringed else 2
    (raw_q, raw_k, cos_ref, sin_ref, gain_ref, u1, wqkv, hl, attn, gh, x_own, hidden, act, w_mlp) = refs[ins : ins + 14]
    w_q, w_k, w_v, gain_attn, norm_in = refs[ins + 14 : ins + 19]
    lo, ig_low, gq_o, gk_o, gv_o, go_o, small_o = refs[ins + 19 : ins + 26]
    (d_qkv, gains, kv_land, kv_stage, o_land, o_stage, q_land, w_land, w_stage, m_part, m_core, m_x, part, core_in, x_in, z_in) = refs[ins + 26 : ins + 42]
    norm_land, small_core, small_x, o_whole, w_whole, w_down, dq_acc, kv_acc, delta, send, recv, load_sem = refs[ins + 42 :]
    q, d = hidden.shape
    t, qw = raw_q.shape
    hd = cos_ref.shape[1]
    kw = raw_k.shape[1]
    bw = w_q.shape[0]
    p = act.shape[1]
    load = pltpu.make_async_copy(w_mlp.at[:, pl.ds(2 * p, p)], w_down, load_sem)
    load.start()
    me = Spot(n)
    wires = Wires(send, recv)
    greet(me.peers() + [me.right_dev, me.left_dev])

    norm_copies = [
        wires.go(norm_in.at[k], norm_land.at[k - 1], me.x_dev(k)) for k in range(1, NZ)
    ]

    def head_back(src, raw, heads, kind, to):
        gains[kind] = jnp.zeros((1, hd), F32)

        @pl.loop(0, 4)
        def _(k):
            at = pl.ds(pl.multiple_of(k * q, q), q)
            cosine, sine = cos_ref[at, :], sin_ref[at, :]
            for h in range(heads):
                cols = slice(h * hd, (h + 1) * hd)
                grad = src[at, cols].astype(F32)
                grad = grad * cosine - turned(grad, sine)
                v = raw[at, cols].astype(F32)
                rs = lax.rsqrt(jnp.mean(v * v, axis=-1, keepdims=True) + EPS)
                unit = v * rs
                gains[kind] += jnp.sum(grad * unit, axis=0, keepdims=True)
                m = grad * gain_ref[kind]
                back = (m - unit * jnp.mean(m * unit, axis=-1, keepdims=True)) * rs
                d_qkv[at, to + h * hd : to + (h + 1) * hd] = back.astype(BF16)

    slots = (3, 1, 2, 0)
    cores, fars, backs = {}, {}, {}

    def slot_plane(i):
        return me.plane_x(slots[i]) if slots[i] else me.z

    def down(i):
        rows = rows_at(slot_plane(i), 4 * q)
        tile = 512

        @pl.loop(0, d // tile)
        def _(c):
            at = pl.ds(pl.multiple_of(c * tile, tile), tile)
            part[i % 2, :, at] = dot(act[rows, :], w_down[at, :], NT).astype(BF16)

        cores[i] = [
            wires.go(part.at[i % 2, rows_at(x * 2 + 1 - me.core, q)], core_in.at[i, k], me.core_dev)
            for k, x in enumerate((1 - me.x, me.x))
        ]

    def down_far(i):
        cores[i][0].wait_recv()
        core_in[i, 0] = (part[i % 2, rows_at(me.tp_far, q), :].astype(F32) + core_in[i, 0].astype(F32)).astype(BF16)
        fars[i] = wires.go(core_in.at[i, 0], x_in.at[i], me.far_dev)

    def down_near(i):
        cores[i][1].wait_recv()
        fars[i].wait_recv()
        value = part[i % 2, rows_at(me.tp, q), :].astype(F32) + core_in[i, 1].astype(F32) + x_in[i].astype(F32)
        wires.drain(cores[i])
        if slots[i] == 0:
            return value
        if slots[i] == 2:
            backs[0].wait_recv()
            value = value + z_in[0].astype(F32)
        x_in[i] = value.astype(BF16)
        backs[i] = wires.go(x_in.at[i], z_in.at[i], me.x_dev(2 if slots[i] == 2 else 1))

    def term(left, right, whole):
        if bw % 128 == 0:
            return lambda r: dot(left[:, rows_at(me.at_place(r), bw)], right[...], TN)

        @pl.loop(0, d // 256)
        def _(c):
            at = rows_at(c, 256)
            whole[at, :] = dot(left[:, at], right[...], TN).astype(BF16)

        return lambda r: whole[rows_at(me.at_place(r), bw), :].astype(F32)

    o_part = term(hl, attn, o_whole)

    o_ring = RingSum(wires, me, o_land, o_stage, o_part)

    half = n // 2
    if ringed:
        base_ref, off_ref, qpos_ref, qfirst_ref, q_ref, kv_ref, do_ref, lse_ref = refs[:8]
        stretch, kh = t // 2, kw // hd
        group = qw // kw
        dq = dq_acc
        dq_acc[...] = jnp.zeros_like(dq_acc)
        for h in range(qw // hd):
            cols = slice(h * hd, (h + 1) * hd)
            delta[:, h : h + 1] = jnp.sum(do_ref[:, cols].astype(F32) * attn[:, cols].astype(F32), axis=-1, keepdims=True)

        def kv_terms(r):
            block = me.at_place(r)
            @pl.loop(0, 2)
            def _(e):
                keys = rows_at(2 * block + e, stretch)
                to = rows_at(e, stretch)
                kpos = off_ref[...] + base_ref[2 * block + e]
                mask = (kpos <= qpos_ref[...]) & (kpos >= qfirst_ref[...])
                for c in range(kh):
                    ck = slice(c * hd, (c + 1) * hd)
                    cv = slice((kh + c) * hd, (kh + c + 1) * hd)
                    k, v = kv_ref[keys, ck], kv_ref[keys, cv]
                    dk = dv = None
                    for h in range(c * group, (c + 1) * group):
                        cols = slice(h * hd, (h + 1) * hd)
                        qh, do = q_ref[:, cols], do_ref[:, cols]
                        prob = jnp.where(mask, jnp.exp(dot(qh, k, NT) * scale - lse_ref[:, h : h + 1]), 0.0)
                        ds = (prob * (dot(do, v, NT) - delta[:, h : h + 1])).astype(BF16)
                        dq_acc[:, cols] += dot(ds, k, NN)
                        dk_h, dv_h = dot(ds, qh, TN), dot(prob.astype(BF16), do, TN)
                        dk = dk_h if dk is None else dk + dk_h
                        dv = dv_h if dv is None else dv + dv_h
                    kv_acc[to, ck] = dk * scale
                    kv_acc[to, cv] = dv

            return kv_acc[...]

        kv_ring = RingSum(wires, me, kv_land, kv_stage, kv_terms)
        kv_ring.start()
    else:
        dq, dkv = refs[:2]
    load.wait()
    fill = [
        lambda: (o_ring.start(),),
        lambda: (down(0),),
        lambda: (down_far(0), down(1)),
        lambda: (down_near(0), down_far(1), down(2)),
    ]
    for k in range(half - 1, 0, -1):
        if ringed:
            kv_ring.step(k)
        if fill:
            fill.pop(0)()
        if k < half - 1:
            o_ring.step(k + 1)
    for job in fill:
        job()
    if half > 1:
        o_ring.step(1)
    if ringed:
        kv_total = kv_ring.total().astype(BF16)
        wires.drain(kv_ring.first)
        kv_stage[...] = kv_total
        kv_sum = kv_stage
        dq_acc[...] = dq_acc[...] * scale
    else:
        kv_sum = dkv
    head_back(dq, raw_q, qw // hd, 0, 0)
    head_back(kv_sum, raw_k, kw // hd, 1, qw)
    d_qkv[:, qw + kw :] = kv_sum[:, kw:].astype(BF16)

    def m_term(peer):
        return dot(d_qkv[rows_at(peer, q), :], wqkv[...], NT)

    q_cols, kv_cols = pl.ds(0, qw), pl.ds(qw, 2 * kw)
    split = bw % 128 != 0
    q_term = term(u1, d_qkv.at[:, q_cols], w_whole.at[:, q_cols] if split else None)
    kv_w_term = term(u1, d_qkv.at[:, kv_cols], w_whole.at[:, kv_cols] if split else None)

    def kv_part(r):
        body = kv_w_term(r)
        extra = w_land.shape[2] - bw
        rest = jnp.concatenate([gains[0], gains[1], jnp.zeros((extra - 2, hd), F32)], axis=0)
        rest = jnp.concatenate([rest, jnp.zeros((extra, body.shape[1] - hd), F32)], axis=1)
        return jnp.concatenate([body, rest], axis=0)

    rings = (RingSum(wires, me, q_land, o_stage, q_term), RingSum(wires, me, w_land, w_stage, kv_part))
    for i, x in enumerate((1 - me.x, me.x)):
        m_part[i] = m_term(x * 2 + 1 - me.core).astype(BF16)
    m_far = wires.go(m_part.at[0], m_core.at[0], me.core_dev)
    m_near = wires.go(m_part.at[1], m_core.at[1], me.core_dev)
    wires.drain(o_ring.first)
    for ring in rings:
        ring.start()
    down_near(1)
    down_far(2)
    down(3)
    own_far = m_term(me.tp_far)
    m_far.wait_recv()
    m_core[0] = (own_far + m_core[0].astype(F32)).astype(BF16)
    m_sum = wires.go(m_core.at[0], m_x, me.far_dev)
    own = m_term(me.tp)
    m_near.wait_recv()
    own = own + m_core[1].astype(F32)
    steps = list(range(half - 1, 0, -1))

    def tick():
        k = steps.pop(0)
        for ring in rings:
            ring.step(k)

    if steps:
        tick()
    m_sum.wait_recv()
    m = own + m_x[...].astype(F32)
    x = x_own[...].astype(F32)
    rs = lax.rsqrt(jnp.mean(x * x, axis=-1, keepdims=True) + EPS)
    unit = x * rs
    grad = gh[...] + (m - unit * jnp.mean(m * unit, axis=-1, keepdims=True)) * rs
    mine = rows_at(me.tp, q)
    ig_low[mine, :] = grad.astype(BF16)

    def spread(buf):
        far = wires.go(buf.at[mine], buf.at[mine], me.far_dev)
        core = wires.go(buf.at[mine], buf.at[mine], me.core_dev)
        return far, core

    def spread_far(buf, copies):
        copies[0].wait_recv()
        at = rows_at(me.tp_far, q)
        return wires.go(buf.at[at], buf.at[at], me.core_dev)

    ig_copies = spread(ig_low)
    if steps:
        tick()

    down_near(2)
    down_far(3)
    out = hidden[...] + down_near(3)
    for i in (1, 2):
        backs[i].wait_recv()
        out = out + z_in[i].astype(F32)
    lo[mine, :] = out.astype(BF16)
    lo_copies = spread(lo)
    ig_last = spread_far(ig_low, ig_copies)
    while steps:
        tick()
    go_o[...] = o_ring.total().T

    lo_last = spread_far(lo, lo_copies)
    ig_copies[1].wait_recv()
    ig_last.wait_recv()
    grad_q = rings[0].total()
    total = rings[1].total()
    grad = total[:bw]
    gain = gain_attn[...]
    norm = jnp.sum(grad_q * w_q[...].astype(F32), axis=1, keepdims=True)
    norm = norm + jnp.sum(grad[:, :kw] * w_k[...].astype(F32), axis=1, keepdims=True)
    norm = norm + jnp.sum(grad[:, kw:] * w_v[...].astype(F32), axis=1, keepdims=True)
    small_o[:bw, :] = jnp.broadcast_to(norm, (bw, hd))
    mlp = norm_in[0]
    for s in range(1, NZ):
        norm_copies[s - 1].wait_recv()
        mlp = mlp + norm_land[s - 1]
    small_o[bw : 2 * bw, :] = mlp
    small_o[2 * bw :, :] = total[bw : bw + 16, :hd]
    copy = wires.go(small_o, small_core, me.core_dev)
    gq_o[...] = grad_q * gain
    gk_o[...] = grad[:, :kw] * gain
    gv_o[...] = grad[:, kw:] * gain
    copy.wait_recv()
    small_core[...] += small_o[...]
    copy = wires.go(small_core, small_x, me.far_dev)
    lo_copies[1].wait_recv()
    lo_last.wait_recv()
    copy.wait_recv()
    wires.close()
    small_o[...] = small_core[...] + small_x[...]


def tail(n, scale, attention, raw_q, raw_k, cosine, sine, gains, u1, wqkv, hl, attn, gh, x_own, hidden, act, w_mlp, w_q, w_k, w_v, gain_attn, norm_in):
    ringed = len(attention) > 2
    q, d = hidden.shape
    t, qw = raw_q.shape
    hd = cosine.shape[1]
    kw = raw_k.shape[1]
    wide = qw + 2 * kw
    bw = d // n
    p = act.shape[1]
    half = n // 2
    copies = tail_copies(n)
    vm = pltpu.VMEM
    small = 2 * bw + 16
    shape = jax.ShapeDtypeStruct
    none = (16, 128)
    return pl.pallas_call(
        partial(tail_kernel, n, ringed, scale),
        in_specs=([SMEM] + [VMEM] * 7 if ringed else [VMEM] * 2) + [VMEM] * 13 + [HBM] + [VMEM] * 5,
        out_specs=[VMEM] * 7,
        out_shape=[
            shape((t, d), BF16),
            shape((t, d), BF16),
            shape((bw, qw), F32),
            shape((bw, kw), F32),
            shape((bw, kw), F32),
            shape((attn.shape[1], bw), F32),
            shape((small, hd), F32),
        ],
        scratch_shapes=[
            vm((t, wide), BF16),
            vm((2, 1, hd), F32),
            vm((2, half, t, 2 * kw) if ringed else (2, 1) + none, BF16),
            vm((t, 2 * kw) if ringed else none, BF16),
            vm((2, half, bw, attn.shape[1]), BF16),
            vm((bw, attn.shape[1]), BF16),
            vm((2, half, bw, qw), BF16),
            vm((2, half, bw + 32, 2 * kw), BF16),
            vm((bw + 32, 2 * kw), BF16),
            vm((2, q, d), BF16),
            vm((2, q, d), BF16),
            vm((q, d), BF16),
            vm((2, t, d), BF16),
            vm((NZ, 2, q, d), BF16),
            vm((NZ, q, d), BF16),
            vm((NZ - 1, q, d), BF16),
            vm((NZ - 1, bw, hd), F32),
            vm((small, hd), F32),
            vm((small, hd), F32),
            vm((d, attn.shape[1]) if bw % 128 else none, BF16),
            vm((d, wide) if bw % 128 else none, BF16),
            vm((d, p), BF16),
            vm((t, qw) if ringed else none, F32),
            vm((t, 2 * kw) if ringed else none, F32),
            vm((t, qw // hd) if ringed else none, F32),
            pltpu.SemaphoreType.DMA((copies,)),
            pltpu.SemaphoreType.DMA((copies,)),
            pltpu.SemaphoreType.DMA,
        ],
        compiler_params=pltpu.CompilerParams(
            collective_id=2, has_side_effects=True, vmem_limit_bytes=67000000
        ),
        name="tail",
    )(*attention, raw_q, raw_k, cosine, sine, gains, u1, wqkv, hl, attn, gh, x_own, hidden, act, w_mlp, w_q, w_k, w_v, gain_attn, norm_in)


def turned(v, sine):
    return pltpu.roll(v, v.shape[1] // 2, 1) * sine


class RingGather:
    def __init__(self, wires, me, buf, rows, part=(0, 1)):
        self.wires, self.me, self.buf, self.rows, self.part = wires, me, buf, rows, part
        self.half = me.n // 2
        self.got = None

    def send(self, right, left):
        buf = self.buf
        self.got = (
            self.wires.go(buf.at[right], buf.at[right], self.me.right_dev),
            self.wires.go(buf.at[left], buf.at[left], self.me.left_dev),
        )

    def wait(self):
        for copy in self.got:
            copy.wait_recv()

    def step(self, k):
        if k > 1:
            self.wait()
        which, parts = self.part
        size = self.rows // parts
        right = self.me.at_place(self.me.n - k + 1) * self.rows + which * size
        left = self.me.at_place(k - 1) * self.rows + which * size
        if k == self.half:
            size = size // 2
            left = left + size
        self.send(pl.ds(pl.multiple_of(right, size), size), pl.ds(pl.multiple_of(left, size), size))


def head_copies(n):
    return 4 * n + 16


def head_kernel(n, scale, x, w_q, w_k, w_v, gain_attn, w_out, w_gate, w_up, w_down, gain_mlp, cos_ref, sin_ref, gain_ref, g_rows, *refs):
    ins = 0 if scale is None else 4
    outs = ins + (0 if scale is None else 2)
    raw_q, raw_k, q_o, kv_o, u1, wqkv, wo, x_own, g_all = refs[ins : ins + 9]
    packed, w_far = refs[ins + 9 : ins + 12], refs[ins + 12]
    own_far, acc, tot, send, recv, g_sem = refs[outs + 13 :]
    t, d = x.shape
    hd = cos_ref.shape[1]
    qw, kw = w_q.shape[1], w_k.shape[1]
    bw = w_q.shape[0]
    p = w_gate.shape[1] // NZ
    me = Spot(n)
    wires = Wires(send, recv)
    greet([me.right_dev, me.left_dev, me.x_dev(1), me.x_dev(2), me.core_dev, me.far_dev])
    g_own = pltpu.make_async_copy(g_rows, g_all.at[rows_at(me.z, t)], g_sem)
    g_own.start()
    half = n // 2
    mine = rows_at(me.blk, bw)

    gain = gain_attn[...]
    wqkv[mine, :qw] = (w_q[...].astype(F32) * gain).astype(BF16)
    wqkv[mine, qw : qw + kw] = (w_k[...].astype(F32) * gain).astype(BF16)
    wqkv[mine, qw + kw :] = (w_v[...].astype(F32) * gain).astype(BF16)
    parts = 2 if bw % 64 == 0 else 1
    w_rings = [RingGather(wires, me, wqkv, bw, (i, parts)) for i in range(parts)]
    for ring in w_rings:
        ring.step(1)

    def unit():
        @pl.loop(0, 4)
        def _(k):
            at = rows_at(k, t // 4)
            v = x[at, :].astype(F32)
            u1[at, :] = (v * lax.rsqrt(jnp.mean(v * v, axis=-1, keepdims=True) + EPS)).astype(BF16)

    def pack(s, to):
        at = rows_at(me.plane(s), p)
        gain = gain_mlp[...]
        to[:, :p] = (w_gate[:, at].astype(F32) * gain).astype(BF16)
        to[:, p : 2 * p] = (w_up[:, at].astype(F32) * gain).astype(BF16)
        to[:, 2 * p :] = w_down[at, :].astype(F32).T.astype(BF16)

    x_own[...] = x[rows_at(me.tp, t // 4), :]

    def output_block():
        wo[mine, :] = w_out[...].astype(F32).T.astype(BF16)

    jobs = [
        lambda: (unit(), output_block()),
        lambda: (pack(2, own_far), pack(0, packed[0])),
        lambda: (pack(1, packed[1]), pack(3, packed[2])),
    ]
    for k in range(2, half + 1):
        if jobs:
            jobs.pop(0)()
        for ring in w_rings:
            ring.step(k)
    for job in jobs:
        job()
    far = wires.go(own_far, w_far, me.z_dev(2))
    q = t // 4
    g_src, g_dst = g_rows.at[rows_at(me.tp, q)], g_all.at[rows_at(me.z * 4 + me.tp, q)]
    near_plane, over_plane, last_plane = me.plane_x(1), me.plane_x(2), me.plane_x(3)
    g_one = wires.go(g_src, g_dst, me.x_dev(1))
    g_two = wires.go(g_src, g_dst, me.x_dev(2))
    g_copies = {}

    def g_near():
        g_one.wait_recv()
        g_copies[1] = wires.pass_on(g_all, me, near_plane, q)

    def g_over():
        g_two.wait_recv()
        at = rows_at(over_plane * 4 + me.tp, q)
        g_copies[0] = wires.go(g_all.at[at], g_all.at[at], me.x_dev(1))
        g_copies[2] = wires.pass_on(g_all, me, over_plane, q)

    def g_far():
        g_copies[1] = wires.pass_far(g_all, me, near_plane, q, g_copies[1])
        g_copies[2] = wires.pass_far(g_all, me, over_plane, q, g_copies[2])

    def g_last():
        g_copies[0].wait_recv()
        g_copies[3] = wires.pass_on(g_all, me, last_plane, q)

    g_jobs = [g_near, g_over, g_far, g_last]
    for ring in w_rings:
        ring.wait()

    rows = t // 2

    @pl.loop(0, 2)
    def _(k):
        at = rows_at(k, rows)
        own = pl.ds(pl.multiple_of(me.blk * t + k * rows, rows), rows)
        y = dot(u1[at, :], wqkv[...], NN)
        raw_q[at, :] = y[:, :qw].astype(BF16)
        raw_k[at, :] = y[:, qw : qw + kw].astype(BF16)
        cosine, sine = cos_ref[at, :], sin_ref[at, :]
        for h in range((qw + kw) // hd):
            v = y[:, h * hd : (h + 1) * hd]
            rs = lax.rsqrt(jnp.mean(v * v, axis=-1, keepdims=True) + EPS)
            v = v * rs * gain_ref[0 if h * hd < qw else 1]
            v = (v * cosine + turned(v, sine)).astype(BF16)
            if h * hd < qw:
                q_o[at, h * hd : (h + 1) * hd] = v
            else:
                kv_o[own, h * hd - qw : (h + 1) * hd - qw] = v
        kv_o[own, kw:] = y[:, qw + kw :].astype(BF16)

    def attend_block(r):
        if scale is None:
            return
        base_ref, off_ref, qpos_ref, qfirst_ref = refs[:ins]
        block = me.at_place(r)
        stretch = t // 2
        kh = kw // hd
        group = qw // kw

        @pl.loop(0, 2)
        def _(e):
            keys = rows_at(2 * block + e, stretch)
            kpos = off_ref[...] + base_ref[2 * block + e]
            mask = (kpos <= qpos_ref[...]) & (kpos >= qfirst_ref[...])
            for h in range(qw // hd):
                c = h // group
                cols = slice(h * hd, (h + 1) * hd)
                k, v = kv_o[keys, c * hd : (c + 1) * hd], kv_o[keys, (kh + c) * hd : (kh + c + 1) * hd]
                prob = jnp.where(mask, jnp.exp(dot(q_o[:, cols], k, NT) * scale), 0.0)
                tot[:, h : h + 1] += jnp.sum(prob, axis=-1, keepdims=True)
                acc[:, cols] += dot(prob.astype(BF16), v, NN)

    kv_ring = RingGather(wires, me, kv_o, t)
    o_ring = RingGather(wires, me, wo, bw)
    acc[...] = jnp.zeros_like(acc)
    tot[...] = jnp.zeros_like(tot)
    for k in range(1, half + 1):
        kv_ring.step(k)
        o_ring.step(k)
        if k > 1:
            attend_block(n - k + 1)
        attend_block(k - 1)
        if g_jobs:
            g_jobs.pop(0)()
    for job in g_jobs:
        job()
    kv_ring.wait()
    attend_block(half)
    if scale is not None:
        attn_o, lse_o = refs[outs + 11 : outs + 13]
        for h in range(qw // hd):
            cols = slice(h * hd, (h + 1) * hd)
            attn_o[:, cols] = (acc[:, cols] / tot[:, h : h + 1]).astype(BF16)
        lse_o[...] = jnp.log(tot[...])
    o_ring.wait()
    g_copies[3] = wires.pass_far(g_all, me, last_plane, q, g_copies[3])
    for k in (1, 2, 3):
        for copy in g_copies[k]:
            copy.wait_recv()
    g_own.wait()
    far.wait_recv()
    wires.close()


def head(n, scale, seen, x, w_q, w_k, w_v, gain_attn, w_out, w_gate, w_up, w_down, gain_mlp, cosine, sine, gains, g_rows):
    t, d = x.shape
    bw, qw = w_q.shape
    kw = w_k.shape[1]
    w3 = 3 * w_gate.shape[1] // NZ
    heads = qw // cosine.shape[1]
    shape = jax.ShapeDtypeStruct
    copies = head_copies(n)
    return pl.pallas_call(
        partial(head_kernel, n, scale),
        in_specs=[VMEM] * 14 + ([] if scale is None else [SMEM] + [VMEM] * 3),
        out_specs=[VMEM] * 8 + [HBM] + [VMEM] * (4 if scale is None else 6),
        out_shape=[
            shape((t, qw), BF16),
            shape((t, kw), BF16),
            shape((t, qw), BF16),
            shape((n * t, 2 * kw), BF16),
            shape((t, d), BF16),
            shape((d, qw + 2 * kw), BF16),
            shape((d, qw), BF16),
            shape((t // 4, d), BF16),
            shape((NZ * t, d), BF16),
        ]
        + [shape((bw, w3), BF16)] * 4
        + ([] if scale is None else [shape((t, qw), BF16), shape((t, heads), F32)]),
        scratch_shapes=[
            pltpu.VMEM((bw, w3), BF16),
            pltpu.VMEM((t, qw), F32),
            pltpu.VMEM((t, heads), F32),
            pltpu.SemaphoreType.DMA((copies,)),
            pltpu.SemaphoreType.DMA((copies,)),
            pltpu.SemaphoreType.DMA,
        ],
        compiler_params=pltpu.CompilerParams(
            collective_id=3, has_side_effects=True, vmem_limit_bytes=67000000
        ),
        name="head",
    )(x, w_q, w_k, w_v, gain_attn, w_out, w_gate, w_up, w_down, gain_mlp, cosine, sine, gains, g_rows, *seen)


def tile_masks(base_ref, tile, qpos_ref, qfirst_ref, off_ref, q0, stretch):
    kpos = off_ref[...] + base_ref[tile]
    qpos = qpos_ref[pl.ds(q0, stretch), :]
    qfirst = qfirst_ref[pl.ds(q0, stretch), :]
    return (kpos <= qpos) & (kpos >= qfirst)


def attend_kernel(dims, scale, base_ref, see_ref, q_ref, kv_ref, qpos_ref, qfirst_ref, off_ref, out_ref, lse_ref, acc_ref, sum_ref):
    qh, kh, hd, stretch = dims
    group = qh // kh
    tile = pl.program_id(0)
    last = pl.num_programs(0) - 1

    @pl.when(tile == 0)
    def _():
        acc_ref[...] = jnp.zeros_like(acc_ref)
        sum_ref[...] = jnp.zeros_like(sum_ref)

    for e in range(2):
        q0 = e * stretch

        @pl.when(see_ref[e, tile] > 0)
        def _():
            mask = tile_masks(base_ref, tile, qpos_ref, qfirst_ref, off_ref, q0, stretch)
            for h in range(qh):
                k = kv_ref[:, (h // group) * hd : (h // group + 1) * hd]
                v = kv_ref[:, (kh + h // group) * hd : (kh + h // group + 1) * hd]
                q = q_ref[q0 : q0 + stretch, h * hd : (h + 1) * hd]
                s = dot(q, k, NT) * scale
                p = jnp.where(mask, jnp.exp(s), 0.0)
                sum_ref[h, q0 : q0 + stretch, :] += jnp.sum(p, axis=-1, keepdims=True)
                acc_ref[q0 : q0 + stretch, h * hd : (h + 1) * hd] += dot(p.astype(BF16), v, NN)

    @pl.when(tile == last)
    def _():
        for h in range(qh):
            total = sum_ref[h]
            out_ref[:, h * hd : (h + 1) * hd] = (acc_ref[:, h * hd : (h + 1) * hd] / total).astype(BF16)
            lse_ref[:, h : h + 1] = jnp.log(total)


def attend(base, see, q, kv, qpos, qfirst, off, qh, kh, hd, scale):
    t = q.shape[0]
    stretch = t // 2
    tiles = kv.shape[0] // stretch

    def whole(shape):
        return pl.BlockSpec(shape, lambda i, *_: (0,) * len(shape))

    return pl.pallas_call(
        partial(attend_kernel, (qh, kh, hd, stretch), scale),
        grid_spec=pltpu.PrefetchScalarGridSpec(
            num_scalar_prefetch=2,
            grid=(tiles,),
            in_specs=[
                whole((t, qh * hd)),
                pl.BlockSpec((stretch, 2 * kh * hd), lambda i, *_: (i, 0)),
                whole((t, 1)),
                whole((t, 1)),
                whole((1, stretch)),
            ],
            out_specs=[whole((t, qh * hd)), whole((t, qh))],
            scratch_shapes=[pltpu.VMEM((t, qh * hd), F32), pltpu.VMEM((qh, t, 1), F32)],
        ),
        out_shape=[
            jax.ShapeDtypeStruct((t, qh * hd), BF16),
            jax.ShapeDtypeStruct((t, qh), F32),
        ],
        cost_estimate=pl.CostEstimate(
            flops=4 * t * kv.shape[0] * hd * qh, bytes_accessed=2 * kv.size, transcendentals=t * kv.shape[0]
        ),
        name="attend",
    )(base, see, q, kv, qpos, qfirst, off)


def attend_back_kernel(
    dims, scale, base_ref, see_ref, q_ref, kv_ref, do_ref, o_ref, lse_ref, qpos_ref, qfirst_ref, off_ref, dq_ref, dkv_out, acc_ref, delta_ref, dkv_ref
):
    qh, kh, hd, stretch = dims
    group = qh // kh
    tile = pl.program_id(0)
    last = pl.num_programs(0) - 1

    @pl.when(tile == 0)
    def _():
        acc_ref[...] = jnp.zeros_like(acc_ref)
        for h in range(qh):
            at = slice(h * hd, (h + 1) * hd)
            delta_ref[h] = jnp.sum(do_ref[:, at].astype(F32) * o_ref[:, at].astype(F32), axis=-1, keepdims=True)

    sees = [see_ref[0, tile] > 0, see_ref[1, tile] > 0]

    @pl.when(jnp.logical_not(sees[0]))
    def _():
        dkv_ref[...] = jnp.zeros_like(dkv_ref)

    def half(e, add):
        q0 = e * stretch
        mask = tile_masks(base_ref, tile, qpos_ref, qfirst_ref, off_ref, q0, stretch)
        for c in range(kh):
            k = kv_ref[:, c * hd : (c + 1) * hd]
            v = kv_ref[:, (kh + c) * hd : (kh + c + 1) * hd]
            dk = dv = None
            for h in range(c * group, (c + 1) * group):
                at = slice(h * hd, (h + 1) * hd)
                q = q_ref[q0 : q0 + stretch, at]
                do = do_ref[q0 : q0 + stretch, at]
                s = dot(q, k, NT) * scale
                p = jnp.where(mask, jnp.exp(s - lse_ref[q0 : q0 + stretch, h : h + 1]), 0.0)
                dp = dot(do, v, NT)
                ds = (p * (dp - delta_ref[h, q0 : q0 + stretch, :])).astype(BF16)
                acc_ref[q0 : q0 + stretch, at] += dot(ds, k, NN)
                dk_h = dot(ds, q, TN)
                dv_h = dot(p.astype(BF16), do, TN)
                dk = dk_h if dk is None else dk + dk_h
                dv = dv_h if dv is None else dv + dv_h
            ck = slice(c * hd, (c + 1) * hd)
            cv = slice((kh + c) * hd, (kh + c + 1) * hd)
            if add:
                dkv_ref[:, ck] += dk * scale
                dkv_ref[:, cv] += dv
            else:
                dkv_ref[:, ck] = dk * scale
                dkv_ref[:, cv] = dv

    for e in range(2):

        @pl.when(sees[e])
        def _():
            half(e, e == 1)

    dkv_out[...] = dkv_ref[...].astype(BF16)

    @pl.when(tile == last)
    def _():
        dq_ref[...] = (acc_ref[...] * scale).astype(BF16)


def attend_back(base, see, q, kv, do, o, lse, qpos, qfirst, off, qh, kh, hd, scale):
    t = q.shape[0]
    stretch = t // 2
    tiles = kv.shape[0] // stretch

    def whole(shape):
        return pl.BlockSpec(shape, lambda i, *_: (0,) * len(shape))

    tile_spec = pl.BlockSpec((stretch, 2 * kh * hd), lambda i, *_: (i, 0))
    return pl.pallas_call(
        partial(attend_back_kernel, (qh, kh, hd, stretch), scale),
        grid_spec=pltpu.PrefetchScalarGridSpec(
            num_scalar_prefetch=2,
            grid=(tiles,),
            in_specs=[
                whole((t, qh * hd)),
                tile_spec,
                whole((t, qh * hd)),
                whole((t, qh * hd)),
                whole((t, qh)),
                whole((t, 1)),
                whole((t, 1)),
                whole((1, stretch)),
            ],
            out_specs=[whole((t, qh * hd)), tile_spec],
            scratch_shapes=[
                pltpu.VMEM((t, qh * hd), F32),
                pltpu.VMEM((qh, t, 1), F32),
                pltpu.VMEM((stretch, 2 * kh * hd), F32),
            ],
        ),
        out_shape=[
            jax.ShapeDtypeStruct((t, qh * hd), BF16),
            jax.ShapeDtypeStruct((kv.shape[0], 2 * kh * hd), BF16),
        ],
        cost_estimate=pl.CostEstimate(
            flops=10 * t * kv.shape[0] * hd * qh, bytes_accessed=6 * kv.size, transcendentals=t * kv.shape[0]
        ),
        name="attend_back",
    )(base, see, q, kv, do, o, lse, qpos, qfirst, off)


def shards(
    n,
    layer_input,
    w_query,
    w_key,
    w_value,
    w_output,
    w_gate,
    w_up,
    w_down,
    norm_attn,
    norm_mlp,
    norm_query,
    norm_key,
    out_grad,
    doc_lengths,
    stretch_order,
):
    t, d = layer_input.shape
    hd = norm_query.shape[0]
    qh, kh = w_query.shape[1] // hd, w_key.shape[1] // hd
    stretch = t // 2
    quarter = t // 4
    width = d // n
    ny = n // NZ
    scale = hd ** (-0.5)
    blk, tp = lax.axis_index("blk"), lax.axis_index("tp")
    z = blk // ny

    order = ring_order(n)
    place = jnp.array([order.index(b) for b in range(n)], jnp.int32)
    me = lax.dynamic_index_in_dim(place, blk, keepdims=False)
    cols = jnp.take(jnp.array(order + order, jnp.int32), me + jnp.arange(n, dtype=jnp.int32))

    gain_attn = norm_attn.astype(F32)[:, None]
    gain_mlp = norm_mlp.astype(F32)[:, None]

    starts = jnp.cumsum(doc_lengths) - doc_lengths

    def first_of(pos):
        return jnp.max(jnp.where(starts[None, :] <= pos[:, None], starts[None, :], 0), axis=1)

    inside = jnp.arange(stretch, dtype=jnp.int32)
    base = stretch_order * stretch
    base_own = lax.dynamic_slice_in_dim(base, 2 * blk, 2, 0)
    positions = (base_own[:, None] + inside[None, :]).reshape(-1)
    firsts = first_of(positions)
    base_first = first_of(base_own)
    see = ((base[None, :] <= base_own[:, None]) & (base[None, :] + (stretch - 1) >= base_first[:, None])).astype(jnp.int32)
    inverse = ROPE_BASE ** (-2.0 * jnp.arange(hd // 2, dtype=F32) / hd)
    angles = (positions - firsts).astype(F32)[:, None] * inverse[None, :]
    cosine, sine = jnp.cos(angles), jnp.sin(angles)
    cosine = jnp.concatenate([cosine, cosine], axis=1)
    sine = jnp.concatenate([-sine, sine], axis=1)
    qpos, qfirst, off = positions[:, None], firsts[:, None], inside[None, :]
    gains = jnp.stack([norm_query.astype(F32)[None, :], norm_key.astype(F32)[None, :]])

    fused = n <= 8
    raw_q, raw_k, q, kv, unit_attn, full_qkv, full_out, x_low, g_all, *rest = head(
        n, scale if fused else None, (base, off, qpos, qfirst) if fused else (), layer_input, w_query, w_key, w_value,
        gain_attn, w_output, w_gate, w_up, w_down, gain_mlp, cosine, sine, gains, out_grad,
    )
    packed = rest[:4]
    attn_low, lse = rest[4:] if fused else attend(base, see, q, kv, qpos, qfirst, off, qh, kh, hd, scale)

    hidden, grad_hidden, grad_heads, hidden_low, _, _, acts, w_mlp, own_piece, norm_mlp_terms, *pieces = feed(
        n, attn_low, full_out, x_low, g_all, packed
    )

    if fused:
        attention = (base, off, qpos, qfirst, q, kv, grad_heads, lse)
    else:
        dq, dkv = attend_back(base, see, q, kv, grad_heads, attn_low, lse, qpos, qfirst, off, qh, kh, hd, scale)
        dkv = [lax.dynamic_slice_in_dim(dkv, cols[r] * t, t, 0).astype(F32) for r in range(n)]
        attention = (dq, ring_scatter(lambda r: dkv[r], n, t))
    layer_output, input_grad, grad_q, grad_k, grad_v, grad_out_w, small = tail(
        n, scale, attention, raw_q, raw_k, cosine, sine, gains, unit_attn, full_qkv, hidden_low, attn_low, grad_hidden,
        x_low, hidden, acts, w_mlp, w_query, w_key, w_value, gain_attn, norm_mlp_terms,
    )
    order = jnp.stack([z, z + 1 - 2 * (z % 2), (z + 2) % NZ, NZ - 1 - z]).astype(jnp.int32)
    grad_gate, grad_up, grad_down, layer_output, input_grad, *others = finish(
        order, [own_piece] + pieces, gain_mlp, layer_output, input_grad, [grad_q, grad_k, grad_v, grad_out_w]
    )
    heads = small[2 * width :, :]
    part = hd // n
    return (
        layer_output,
        input_grad,
        *others,
        grad_gate,
        grad_up,
        grad_down,
        small[:width, 0],
        small[width : 2 * width, 0] / gain_mlp[:, 0],
        lax.dynamic_slice(heads, (0, blk * part), (1, part))[0],
        lax.dynamic_slice(heads, (1, blk * part), (1, part))[0],
    )


def solution(mesh):
    return jax.shard_map(
        partial(shards, mesh.shape["blk"]),
        mesh=mesh,
        in_specs=(
            P("blk", None),
            P("blk", "tp"),
            P("blk", "tp"),
            P("blk", "tp"),
            P("tp", "blk"),
            P("blk", "tp"),
            P("blk", "tp"),
            P("tp", "blk"),
            P("blk"),
            P("blk"),
            P(),
            P(),
            P("blk", None),
            P(),
            P(),
        ),
        out_specs=(
            P("blk", None),
            P("blk", None),
            P("blk", "tp"),
            P("blk", "tp"),
            P("blk", "tp"),
            P("tp", "blk"),
            P("blk", "tp"),
            P("blk", "tp"),
            P("tp", "blk"),
            P("blk"),
            P("blk"),
            P("blk"),
            P("blk"),
        ),
        check_vma=False,
    )
```
